32 devices in a mesh: freq: 4 (over y, core), lat: 8 (over z, x).
Axes of the slice: x: 2, y: 2, z: 4, core: 2. Of those that a mesh axis runs over, the one named last changes fastest.
Arguments:
- spectra: float32 [2, 4, 32768], P(None, None, ('freq', 'lat')), may hold values from -6 to 6
- tile_route: int32 [32768, 1], P(('freq', 'lat')), may hold values from 0 to 255; in each aligned block of 1024 rows (0 to 1023, 1024 to 2047, ...) at most 8 rows name the same one
- bin_in_tile: int32 [32768], P(('freq', 'lat')), may hold values from 0 to 1023
- trace_offset: float32 [2, 32768], P(None, ('freq', 'lat')), may hold values from -0.5 to 0.5
- weights: float32 [32768], P(('freq', 'lat')), may hold values from 0.2 to 5
- frequency: float32 [4], P('freq'), may hold values from 0.5 to 1.5
- slowness: float32 [2, 8], replicated, may hold values from 0.6 to 1.6
- vel_index: int32 [2, 512, 512], P(None, 'lat'), may hold values from 0 to 7
Outputs:
- wavefield: float32 [2, 4, 512, 512], P(None, 'freq', 'lat')
- depth_image: float32 [2, 512, 512], P(None, 'lat', 'freq')
The draws below stay inside these ranges and needn't reach their ends.
Inputs may be any that keep to these rules, and one draw needn't show every extreme that they name: `tile_route`: tiles of 32 x 32 bins, numbered row by row over the grid; among the rows of one device no tile is named by more than 8 traces. `bin_in_tile`: row * 32 + column of the bin within the tile.
All inputs are finite; a program needn't handle non-finite values.
Results may differ from the reference program's by a relative error of at most 0.0003.
Values sent between devices are 32-bit elements; how exact they have to be, the bound alone decides.
A program may use at most 64 MiB of HBM per device.

```python
import math
import jax
import jax.numpy as jnp
import numpy as np
from jax import lax

NX = 512
NY = 512
TB = 32
MODES = 8
TR_DEV = 1024
NSTEPS = 2
NREF = 2
NVEL = 8
NF = 4
TRACES = 32768
TILES = 256
CAP = 8
N_LAT = 8
DEVICES = 32


def plant(values, rng, least, largest):
    shape = values.shape
    place = [jax.random.randint(jax.random.fold_in(rng, axis), (), 0, shape[axis]) for axis in range(len(shape))]
    values = values.at[tuple(place)].set(least)
    longest = shape.index(max(shape))
    place[longest] = (place[longest] + 1) % shape[longest]
    return values.at[tuple(place)].set(largest)


def block_scale(key, dims, shards, low, top_value):
    loudness, own = 1.0, jax.random.fold_in(key, 6)
    for dim, parts in shards:
        steps = jnp.exp(jax.random.uniform(jax.random.fold_in(own, dim), (parts,), jnp.float32, low / len(shards), top_value / len(shards)))
        loudness = loudness * jnp.repeat(steps, dims[dim] // parts).reshape([-1 if axis == dim else 1 for axis in range(len(dims))])
    return loudness


def shared_out(rng, own, number, rows, count, top, most, skew):
    order = jax.random.permutation(rng, count)
    heavy_load, common = load_shares(count, rows * top, most, skew, True), load_shares(count, rows * top, most, skew, False)
    places = jnp.arange(count)

    def named(sizes, turn):
        used = int((sizes > 0).sum())
        fixed = max(1, used // 4)
        moved = fixed + (places - fixed + turn * (used - fixed)) % max(1, count - fixed)
        return jnp.zeros((count,), jnp.int32).at[order[jnp.where(places < fixed, places, moved)]].set(jnp.asarray(sizes, jnp.int32))

    sizes = jnp.where(number % 4 == 0, named(heavy_load, number // 4), named(common, number - number // 4 - 1))
    mixed = jax.random.permutation(jax.random.fold_in(own, 3), count)
    donor, sink = mixed[0:count // 2 * 2:2], mixed[1:count // 2 * 2:2]
    room = jnp.minimum(sizes[donor] - 1, most - sizes[sink]) // 2
    room = jnp.where((donor == order[0]) | (sink == order[0]) | (sizes[sink] == 0), 0, jnp.maximum(room, 0))
    moved = jax.random.randint(jax.random.fold_in(own, 4), (count // 2,), 0, 1 << 20) % (room + 1)
    sizes = sizes.at[donor].add(-moved).at[sink].add(moved)
    labels = jnp.searchsorted(jnp.cumsum(sizes), jnp.arange(rows * top), side="right").astype(jnp.int32)
    table = labels.reshape(top, rows).T
    table = table[jax.random.permutation(jax.random.fold_in(own, 1), rows)]
    turn = jax.random.randint(jax.random.fold_in(own, 2), (rows, 1), 0, top)
    return jnp.take_along_axis(table, (jnp.arange(top)[None, :] + turn) % top, axis=1)


def load_shares(amount, total, reach, lean, full):
    portions = [(1 << 20) // math.isqrt(grade ** lean) + 1 for grade in range(1, amount + 1)]
    largest = reach if full else min(reach, max(-(-total // amount), total * portions[0] // sum(portions)))
    least = 1 if total - largest >= amount - 1 else 0
    given, spare = [largest] + [least] * (amount - 1), total - largest - least * (amount - 1)
    while spare > 0:
        candidates = [i for i in range(1, amount) if given[i] < largest] or [i for i in range(1, amount) if given[i] < reach]
        mass, budget = sum([portions[i] for i in candidates]), spare
        for i in candidates:
            more = min(reach - given[i], max(1, budget * portions[i] // mass), spare)
            given[i] = given[i] + more
            spare = spare - more
    return np.array(given)


def gaussian(key, dims, deviation, reach, pieces=(), kind=jnp.bfloat16):
    result = jax.random.normal(key, dims, jnp.float32) * deviation
    if len(pieces) > 0:
        result = block_scale(key, dims, pieces, -0.22, 0.18) * result
    return jnp.clip(result, min=-reach, max=reach).astype(kind)


def setup_inputs(seed: int = 0) -> dict:
    streams_of = jax.random.split(jax.random.key(seed), 9)
    spectra = gaussian(streams_of[0], (2, NF, TRACES), 1.0, 6.0, ((2, 32),), jnp.float32)
    tile_route_keys = jax.random.split(jax.random.fold_in(streams_of[1], 1), TRACES // TR_DEV)
    tile_route_turns = jax.random.permutation(jax.random.fold_in(streams_of[1], 3), TRACES // TR_DEV)
    tile_route = jax.vmap(lambda own, number: shared_out(jax.random.fold_in(streams_of[1], 2), own, number, TR_DEV, TILES, 1, CAP, 2))(tile_route_keys, tile_route_turns).reshape((TRACES, 1))
    bin_in_tile = plant(jax.random.randint(streams_of[2], (TRACES,), 0, TB * TB), jax.random.fold_in(streams_of[2], 1), 0, (TB * TB) - 1).astype(jnp.int32)
    trace_offset = jnp.clip(jax.random.uniform(streams_of[3], (2, TRACES), jnp.float32, -0.5, 0.5) * block_scale(streams_of[3], (2, TRACES), ((1, 32),), -0.4, 0.0), -0.5, 0.5)
    weights = jnp.clip(jnp.exp(math.log(5.0) - 3.218876 * jax.random.uniform(streams_of[4], (TRACES,), jnp.float32) ** block_scale(streams_of[4], (TRACES,), ((0, 32),), -0.2, 0.2)), 0.2, 5.0)
    frequency = jnp.clip(0.5 + 1.0 * jax.random.uniform(streams_of[5], (NF,), jnp.float32) ** block_scale(streams_of[5], (NF,), ((0, 4),), -0.2, 0.2), 0.5, 1.5)
    slowness = jnp.clip(jnp.exp(jax.random.uniform(streams_of[6], (NSTEPS, NVEL), jnp.float32, math.log(0.6), math.log(1.6))), 0.6, 1.6)
    vel_index = plant(jax.random.randint(streams_of[7], (NSTEPS, NX, NY), 0, NVEL), jax.random.fold_in(streams_of[7], 1), 0, NVEL - 1).astype(jnp.int32)
    return dict(spectra=spectra, tile_route=tile_route, bin_in_tile=bin_in_tile, trace_offset=trace_offset, weights=weights, frequency=frequency, slowness=slowness, vel_index=vel_index)


damping = 1.0
depth_step = 1.0

def basis_of(cell_x, cell_y):
    mode_ids = jnp.arange(MODES).astype(jnp.float32)
    along_x = jnp.cos(math.pi * mode_ids.reshape((MODES,) + (1,) * cell_x.ndim) * (cell_x[None] + 0.5) / TB)
    along_y = jnp.cos(math.pi * mode_ids.reshape((MODES,) + (1,) * cell_y.ndim) * (cell_y[None] + 0.5) / TB)
    return (along_x[:, None] * along_y[None, :]).reshape((MODES * MODES,) + cell_x.shape)

def fit_grid(normal, right_side, row_count):
    tile_count = normal.shape[0]
    system = normal + damping * jnp.eye(MODES * MODES, dtype=jnp.float32)
    factor = jnp.linalg.cholesky(system)
    flat_rhs = right_side.reshape(tile_count, MODES * MODES, -1)
    middle = jax.scipy.linalg.solve_triangular(factor, flat_rhs, lower=True)
    coeffs = jax.scipy.linalg.solve_triangular(factor, middle, lower=True, trans='T')
    coeffs = coeffs.reshape(row_count // TB, NY // TB, MODES, MODES, 2, -1)
    cell_pos = jnp.arange(TB).astype(jnp.float32)
    cos_table = jnp.cos(math.pi * jnp.arange(MODES).astype(jnp.float32)[:, None] * (cell_pos[None, :] + 0.5) / TB)
    viewed = jnp.einsum('xyabpq,ai,bj->pqxiyj', coeffs, cos_table, cos_table, precision=lax.Precision.HIGHEST)
    return viewed.reshape(2, viewed.shape[1], row_count, NY)

def reference(spectra, tile_route, bin_in_tile, trace_offset, weights, frequency, slowness, vel_index):
    tile_id = tile_route[:, 0].astype(jnp.int32)
    trace_count = tile_id.shape[0]
    per_tile = DEVICES * CAP
    ranking = jnp.argsort(tile_id, stable=True).astype(jnp.int32)
    sorted_tiles = tile_id[ranking]
    firsts = jnp.searchsorted(sorted_tiles, sorted_tiles, side='left').astype(jnp.int32)
    position = sorted_tiles * per_tile + jnp.arange(trace_count, dtype=jnp.int32) - firsts
    lookup = jnp.full((TILES * per_tile,), trace_count, jnp.int32).at[position].set(ranking)
    cell_x = (bin_in_tile // TB).astype(jnp.float32) + trace_offset[0]
    cell_y = (bin_in_tile % TB).astype(jnp.float32) + trace_offset[1]
    trace_meta = jnp.stack([weights, cell_x, cell_y], 0)
    padded_meta = jnp.concatenate([trace_meta, jnp.zeros((3, 1), jnp.float32)], 1)
    padded_spec = jnp.concatenate([spectra, jnp.zeros((2, NF, 1), jnp.float32)], 2)
    tile_dev = TILES // N_LAT
    row_count = NX // N_LAT

    def one_owner(owner_at):
        picks = lax.dynamic_slice_in_dim(lookup, owner_at * tile_dev * per_tile, tile_dev * per_tile)
        meta_here = padded_meta[:, picks].reshape(3, tile_dev, per_tile)
        spec_here = padded_spec[:, :, picks].reshape(2, NF, tile_dev, per_tile)
        basis_vals = basis_of(meta_here[1], meta_here[2])
        weighted = basis_vals * meta_here[0][None]
        normal = jnp.einsum('itc,jtc->tij', weighted, basis_vals, precision=lax.Precision.HIGHEST)
        right_side = jnp.einsum('itc,pqtc->tipq', weighted, spec_here, precision=lax.Precision.HIGHEST)
        return fit_grid(normal, right_side, row_count)
    slabs = lax.map(one_owner, jnp.arange(N_LAT, dtype=jnp.int32))
    gridded = jnp.moveaxis(slabs, 0, 2).reshape(2, NF, NX, NY)
    wave_field = gridded[0] + 1j * gridded[1]
    index_x = jnp.arange(NX)
    index_y = jnp.arange(NY)
    signed_x = jnp.where(index_x >= NX // 2, index_x - NX, index_x)
    signed_y = jnp.where(index_y >= NY // 2, index_y - NY, index_y)
    kx_vals = 2.0 * math.pi / NX * signed_x.astype(jnp.float32)
    ky_vals = 2.0 * math.pi / NY * signed_y.astype(jnp.float32)
    per_group = NVEL // NREF
    images = []
    for depth_at in range(NSTEPS):
        table_row = slowness[depth_at]
        references = table_row.reshape(NREF, per_group).mean(axis=1)
        spectrum = jnp.fft.fft2(wave_field)
        wave_num = frequency[None, :] * references[:, None]
        vertical = (wave_num * wave_num)[:, :, None, None] - (kx_vals * kx_vals)[None, None, :, None] - (ky_vals * ky_vals)[None, None, None, :]
        phase_angle = jnp.sqrt(jnp.maximum(vertical, 0.0)) * depth_step
        damped = jnp.exp(-jnp.sqrt(jnp.maximum(-vertical, 0.0)) * depth_step)
        returned = jnp.fft.ifft2(spectrum[None] * (damped * jnp.exp(1j * phase_angle)))
        velocity = vel_index[depth_at]
        local_slow = table_row[velocity]
        group_of = velocity // per_group
        split_phase = frequency[None, :, None, None] * (local_slow[None, None] - references[:, None, None, None]) * depth_step
        group_mask = group_of[None] == jnp.arange(NREF)[:, None, None]
        wave_field = lax.optimization_barrier(jnp.sum(jnp.where(group_mask[:, None], returned * jnp.exp(1j * split_phase), 0.0), 0))
        images.append(lax.optimization_barrier(jnp.sum(jnp.real(wave_field), 0)).astype(jnp.float32))
    wavefield = jnp.stack([jnp.real(wave_field), jnp.imag(wave_field)], 0).astype(jnp.float32)
    return (wavefield, jnp.stack(images, 0))
```

```python
import functools
import math

import jax
import jax.numpy as jnp
import numpy as np
from jax import lax
from jax.experimental import pallas as pl
from jax.experimental.pallas import tpu as pltpu
from jax.sharding import PartitionSpec as P

TB = 32
MODES = 8
CAP = 8
TERMS = MODES * MODES
REFS = 2

damping = 1.0
depth_step = 1.0

NN = (((1,), (0,)), ((), ()))
NT = (((1,), (1,)), ((), ()))
VMEM = pl.BlockSpec(memory_space=pltpu.VMEM)
SMEM = pl.BlockSpec(memory_space=pltpu.SMEM)
ANY = pl.BlockSpec(memory_space=pl.ANY)
MESH = pl.DeviceIdType.MESH


def two_parts(exact):
    high = exact.astype(jnp.bfloat16)
    low = (exact - high.astype(np.float64)).astype(jnp.bfloat16)
    return np.stack([high, low], 0)


def hartley(length):
    at = np.arange(length)
    angle = 2.0 * math.pi / length * (at[:, None] * at[None, :] % length)
    return (np.cos(angle) + np.sin(angle)) / math.sqrt(length)


def mode_table(length):
    cosines = np.cos(math.pi * np.arange(MODES)[:, None] * (np.arange(TB)[None, :] + 0.5) / TB)
    fold = np.zeros((length // TB, MODES, length))
    for tile in range(length // TB):
        fold[tile, :, tile * TB : (tile + 1) * TB] = cosines
    return fold.reshape(length // TB * MODES, length) @ hartley(length)


def split2(x):
    high = x.astype(jnp.bfloat16)
    return high, (x - high.astype(jnp.float32)).astype(jnp.bfloat16)


def dot(a, b, dims=NN):
    return lax.dot_general(a, b, dims, preferred_element_type=jnp.float32)


def dot3(a, b, dims=NN):
    return dot(a[0], b[0], dims) + (dot(a[0], b[1], dims) + dot(a[1], b[0], dims))


def series(value, first, count):
    total = jnp.full(value.shape, 1.0 / math.factorial(2 * (count - 1) + first), jnp.float32)
    for n in range(count - 2, -1, -1):
        total = 1.0 / math.factorial(2 * n + first) - value * total
    return total


def cosine_of(cell):
    angle = (0.5 * TB - (cell + 0.5)) * (math.pi / TB)
    return angle * series(angle * angle, 1, 9)


def propagator(wave_squared, kx, ky):
    vertical = wave_squared - kx * kx - ky * ky
    root = jnp.sqrt(jnp.abs(vertical)) * depth_step
    squared = root * root
    moving = vertical > 0.0
    even = jnp.where(moving, series(squared, 0, 10), jnp.exp(-root))
    odd = jnp.where(moving, root * series(squared, 1, 10), 0.0)
    return even, odd


def signed(index, length):
    return (
        2.0 * math.pi / length * jnp.where(index >= length // 2, index - length, index).astype(jnp.float32)
    )


def iota(shape, axis):
    return lax.broadcasted_iota(jnp.int32, shape, axis)


def program(
    cfg,
    spectra_ref,
    tile_ref,
    bin_ref,
    offset_ref,
    weight_ref,
    freq_ref,
    slow_ref,
    vel_hbm,
    hart_hbm,
    modes_hbm,
    modes_t_hbm,
    wave_ref,
    image_ref,
    hart,
    modes,
    modes_t,
    vel,
    route_out,
    route_in,
    system,
    coef_out,
    coef_in,
    wide_even,
    wide_odd,
    band_even,
    band_odd,
    along,
    across,
    fwd_out,
    fwd_in,
    back_out,
    back_in,
    image_out,
    image_in,
    table_sem,
    route_sent,
    route_got,
    coef_sent,
    coef_got,
    fwd_sent,
    fwd_got,
    back_sent,
    back_got,
    image_sent,
    image_got,
):
    F, L, tiles, nx, ny, rows, band, data_rows, padded, steps, nvel = cfg
    devices = F * L
    slots = tiles * CAP
    per_group = nvel // REFS
    lanes = 2 * band
    me_f = lax.axis_index("freq")
    me_l = lax.axis_index("lat")
    me = me_l * F + me_f

    loads = [
        pltpu.make_async_copy(src, dst, table_sem.at[at])
        for at, (src, dst) in enumerate(
            [(vel_hbm, vel), (modes_hbm, modes), (modes_t_hbm, modes_t), (hart_hbm, hart)]
        )
    ]
    for load in loads:
        load.start()

    barrier = pltpu.get_barrier_semaphore()

    def partner_of(step):
        other = lax.rem(me + step, devices)
        return other, {"freq": lax.rem(other, F), "lat": lax.div(other, F)}

    def greet(step, carry):
        _, device = partner_of(step)
        pl.semaphore_signal(barrier, inc=1, device_id=device, device_id_type=MESH)
        return carry

    lax.fori_loop(1, devices, greet, 0)

    count = tile_ref.shape[1]
    width = 128
    tile = tile_ref[...]
    columns = [
        jnp.transpose(jnp.broadcast_to(tile[:, at : at + width], (width, width)))
        for at in range(0, count, width)
    ]
    earlier = iota((width, width), 0) < iota((width, width), 1)
    ranks = []
    for at in range(count // width):
        row = jnp.broadcast_to(tile[:, at * width : (at + 1) * width], (width, width))
        same = jnp.where((columns[at] == row) & earlier, 1, 0)
        for before in range(at):
            same = same + jnp.where(columns[before] == row, 1, 0)
        ranks.append(jnp.sum(same, 0, keepdims=True))
    rank = jnp.concatenate(ranks, 1)
    turned = lax.rem(lax.rem(tile, tiles) + me, tiles)
    slot = lax.div(tile, tiles) * slots + turned * CAP + rank

    cell = bin_ref[...]
    root_weight = jnp.sqrt(weight_ref[...])
    cell_x = lax.div(cell, TB).astype(jnp.float32) + offset_ref[0:1, :]
    cell_y = lax.rem(cell, TB).astype(jnp.float32) + offset_ref[1:2, :]
    feats = jnp.concatenate(
        [spectra_ref[0] * root_weight, spectra_ref[1] * root_weight]
        + [root_weight, cosine_of(cell_x), cosine_of(cell_y)]
        + [jnp.zeros((padded - data_rows - 3, count), jnp.float32)],
        0,
    )
    high = feats.astype(jnp.bfloat16)
    rest = feats - high.astype(jnp.float32)
    middle = rest.astype(jnp.bfloat16)
    low = (rest - middle.astype(jnp.float32)).astype(jnp.bfloat16)
    parts = jnp.concatenate([high, middle, low], 0)
    wide = 256
    for at in range(0, devices * slots, wide):
        places = iota((wide, count), 0) + at
        chosen = jnp.where(places == slot, 1.0, 0.0).astype(jnp.bfloat16)
        got = dot(parts, chosen, NT)
        got = got[:padded] + got[padded : 2 * padded] + got[2 * padded :]
        for piece in range(wide // slots):
            route_out[at // slots + piece] = got[:, piece * slots : (piece + 1) * slots]

    pl.semaphore_wait(barrier, devices - 1)

    def spread(out, into, sent, landed):
        def copy_of(step):
            other, device = partner_of(step)
            return pltpu.make_async_remote_copy(
                src_ref=out.at[other] if out.shape[0] == devices else out.at[lax.rem(other, F)],
                dst_ref=into.at[me],
                send_sem=sent.at[step],
                recv_sem=landed.at[step],
                device_id=device,
                device_id_type=MESH,
            )

        def start(step, carry):
            copy_of(step).start()
            return carry

        def arrive(step, carry):
            copy_of(step).wait_recv()
            return carry

        def leave(step, carry):
            copy_of(step).wait_send()
            return carry

        lax.fori_loop(1, devices, start, 0)
        return (
            lambda: lax.fori_loop(1, devices, arrive, 0),
            lambda: lax.fori_loop(1, devices, leave, 0),
        )

    arrive, leave_route = spread(route_out, route_in, route_sent, route_got)
    route_in[pl.ds(me, 1)] = route_out[pl.ds(me, 1)]

    frequency = freq_ref[0]
    waves = []
    for depth_at in range(steps):
        squares = []
        for g in range(REFS):
            total = slow_ref[depth_at, g * per_group]
            for i in range(1, per_group):
                total = total + slow_ref[depth_at, g * per_group + i]
            reference = total * (1.0 / per_group)
            squares.append((reference, (frequency * reference) * (frequency * reference)))
        waves.append(squares)

    chunk = 8

    def wide_tables(at, carry):
        first = pl.multiple_of(at * chunk, chunk)
        kx = signed(iota((chunk, ny), 0) + first, nx)
        ky = signed(iota((chunk, ny), 1), ny)
        for g in range(REFS):
            even, odd = propagator(waves[0][g][1], kx, ky)
            wide_even[g, pl.ds(first, chunk), :] = even
            wide_odd[g, pl.ds(first, chunk), :] = odd
        return carry

    lax.fori_loop(0, nx // chunk, wide_tables, 0)
    arrive()

    group_at = lax.div(iota((padded, slots), 1), CAP)
    eye = jnp.where(iota((TERMS, TERMS + data_rows), 0) == iota((TERMS, TERMS + data_rows), 1), damping, 0.0)

    def chebyshev(cosine):
        terms = [jnp.ones_like(cosine), cosine]
        for _ in range(MODES - 2):
            terms.append(2.0 * cosine * terms[-1] - terms[-2])
        return terms

    for t in range(tiles):
        pieces = []
        for first in range(0, devices, tiles):
            picked = route_in[first]
            for i in range(1, tiles):
                picked = jnp.where(group_at == (t + i) % tiles, route_in[first + i], picked)
            pieces.append(picked)
        got = jnp.concatenate(pieces, 1)
        scale = got[data_rows : data_rows + 1]
        along_x = chebyshev(got[data_rows + 1 : data_rows + 2])
        along_y = jnp.concatenate(chebyshev(got[data_rows + 2 : data_rows + 3]), 0)
        basis = jnp.concatenate([(term * scale) * along_y for term in along_x], 0)
        right = jnp.concatenate([basis, got[:data_rows]], 0)
        system[t] = eye + lax.dot_general(
            basis, right, NT, preferred_element_type=jnp.float32, precision=lax.Precision.HIGHEST
        )
    for k in range(TERMS):
        row = system[:, k : k + 1, :]
        scaled = row * (1.0 / row[:, :, k : k + 1])
        whole = system[...]
        system[...] = whole - whole[:, :, k : k + 1] * scaled
        system[:, k : k + 1, :] = scaled
    solved = [jnp.transpose(system[t])[TERMS:] for t in range(tiles)]
    for a in range(MODES):
        line = jnp.concatenate([one[:, a * MODES : (a + 1) * MODES] for one in solved], 1)
        for part in range(2):
            for f in range(F):
                at = part * F + f
                coef_out[f, part, a : a + 1, :] = line[at : at + 1]

    arrive, leave_coef = spread(coef_out, coef_in, coef_sent, coef_got)
    coef_in[pl.ds(me, 1)] = coef_out[pl.ds(me_f, 1)]

    line = iota((chunk, lanes), 1)
    ky = signed(me_l * band + lax.rem(line, band), ny)
    sign = jnp.where(line < band, -1.0, 1.0)

    def band_tables(at, carry):
        first = pl.multiple_of(at * chunk, chunk)
        kx = signed(iota((chunk, lanes), 0) + first, nx)
        for depth_at in range(1, steps):
            for g in range(REFS):
                even, odd = propagator(waves[depth_at][g][1], kx, ky)
                band_even[depth_at - 1, g, pl.ds(first, chunk), :] = even
                band_odd[depth_at - 1, g, pl.ds(first, chunk), :] = odd * sign
        return carry

    lax.fori_loop(0, nx // chunk, band_tables, 0)
    for load in loads:
        load.wait()
    for depth_at in range(steps):
        velocity = vel[depth_at]
        cosine = jnp.zeros(velocity.shape, jnp.float32)
        sine = jnp.zeros(velocity.shape, jnp.float32)
        for i in range(nvel):
            shift = slow_ref[depth_at, i] - waves[depth_at][i // per_group][0]
            angle = jnp.full((8, 128), frequency * shift * depth_step, jnp.float32)
            squared = angle * angle
            cosine_i = series(squared, 0, 9)[0:1, 0:1]
            sine_i = (angle * series(squared, 1, 9))[0:1, 0:1]
            cosine = jnp.where(velocity == i, cosine_i, cosine)
            sine = jnp.where(velocity == i, sine_i, sine)
        along[depth_at] = cosine
        across[depth_at] = sine
    arrive()

    per_row = (ny // TB) // tiles
    lines = []
    for part in range(2):
        for tile_row in range(nx // TB):
            lines.append(
                jnp.concatenate([coef_in[tile_row * per_row + j, part] for j in range(per_row)], 1)
            )
    spread_y = dot3(split2(jnp.concatenate(lines, 0)), (modes[0], modes[1]))
    mode_rows = nx // TB * MODES
    spread_y = split2(jnp.concatenate([spread_y[:mode_rows], spread_y[mode_rows:]], 1))
    own = pl.ds(pl.multiple_of(me_l * rows, rows), rows)
    own_high, own_low = hart[0, own, :], hart[1, own, :]
    both = jnp.concatenate([own_high, own_low], 0)
    half = nx // 2
    backs = [None] * REFS
    for first in range(0, nx, half):
        part = slice(first, first + half)
        spectrum = dot3((modes_t[0, part, :], modes_t[1, part, :]), spread_y)
        real, imag = spectrum[:, :ny], spectrum[:, ny:]
        for g in range(REFS):
            even, odd = wide_even[g, part, :], wide_odd[g, part, :]
            moved = split2(jnp.concatenate([real * even - imag * odd, real * odd + imag * even], 1))
            made = dot(both[:, part], moved[0])
            made = made[:rows] + (made[rows:] + dot(own_high[:, part], moved[1]))
            backs[g] = made if backs[g] is None else backs[g] + made
    lines = [back[:, p * ny : (p + 1) * ny] for back in backs for p in range(2)]

    def to_field(depth_at, lines):
        made = dot3(split2(jnp.concatenate(lines, 0)), (hart[0], hart[1]))
        velocity = vel[depth_at]
        real, imag = made[:rows], made[rows : 2 * rows]
        for g in range(1, REFS):
            chosen = velocity >= g * per_group
            real = jnp.where(chosen, made[2 * g * rows : (2 * g + 1) * rows], real)
            imag = jnp.where(chosen, made[(2 * g + 1) * rows : (2 * g + 2) * rows], imag)
        cosine, sine = along[depth_at], across[depth_at]
        return real * cosine - imag * sine, real * sine + imag * cosine

    def swap(x):
        return jnp.concatenate([x[:, band:], x[:, :band]], 1)

    def send_image(depth_at, real):
        piece = ny // F
        for f in range(F):
            image_out[depth_at, f] = real[:, f * piece : (f + 1) * piece]
        copies = []
        for step in range(1, F):
            other = lax.rem(me_f + step, F)
            copies.append(
                pltpu.make_async_remote_copy(
                    src_ref=image_out.at[depth_at, other],
                    dst_ref=image_in.at[depth_at, me_f],
                    send_sem=image_sent.at[depth_at, step],
                    recv_sem=image_got.at[depth_at, step],
                    device_id={"freq": other},
                    device_id_type=MESH,
                )
            )
        for copy in copies:
            copy.start()
        image_in[depth_at, pl.ds(me_f, 1)] = image_out[depth_at, pl.ds(me_f, 1)]
        return copies

    def exchange(at, out, into, sent, landed):
        copies = []
        for step in range(1, L):
            other = lax.rem(me_l + step, L)
            copies.append(
                pltpu.make_async_remote_copy(
                    src_ref=out.at[at, other],
                    dst_ref=into.at[at, me_l],
                    send_sem=sent.at[at, step],
                    recv_sem=landed.at[at, step],
                    device_id={"lat": other},
                    device_id_type=MESH,
                )
            )
        for copy in copies:
            copy.start()
        into[at, pl.ds(me_l, 1)] = out[at, pl.ds(me_l, 1)]
        return copies

    pending = []
    images = []
    for depth_at in range(steps):
        real, imag = to_field(depth_at, lines)
        images.append(send_image(depth_at, real))
        if depth_at == steps - 1:
            wave_ref[0] = real
            wave_ref[1] = imag
            break
        made = dot3(split2(jnp.concatenate([real, imag], 0)), (hart[0], hart[1]))
        for dst in range(L):
            part = slice(dst * band, (dst + 1) * band)
            fwd_out[depth_at, dst] = jnp.concatenate([made[:rows, part], made[rows:, part]], 1)
        copies = exchange(depth_at, fwd_out, fwd_in, fwd_sent, fwd_got)
        pending += copies
        for copy in copies:
            copy.wait_recv()
        got = split2(fwd_in[depth_at].reshape(nx, lanes))
        made = dot(hart[0], jnp.concatenate([got[0], got[1]], 1))
        spectrum = made[:, :lanes] + (made[:, lanes:] + dot(hart[1], got[0]))
        swapped = swap(spectrum)
        moved = jnp.concatenate(
            [
                spectrum * band_even[depth_at, g] + swapped * band_odd[depth_at, g]
                for g in range(REFS)
            ],
            1,
        )
        back = dot3((hart[0], hart[1]), split2(moved))
        back_out[depth_at] = back.reshape(L, rows, REFS * lanes)
        copies = exchange(depth_at, back_out, back_in, back_sent, back_got)
        pending += copies
        for copy in copies:
            copy.wait_recv()
        lines = [
            jnp.concatenate(
                [back_in[depth_at, src, :, q * band : (q + 1) * band] for src in range(L)], 1
            )
            for q in range(2 * REFS)
        ]

    leave_route()
    leave_coef()
    for copy in pending:
        copy.wait_send()
    for depth_at in range(steps):
        for copy in images[depth_at]:
            copy.wait()
        total = image_in[depth_at, 0]
        for f in range(1, F):
            total = total + image_in[depth_at, f]
        image_ref[depth_at] = total


def local(spectra, tile_route, bin_in_tile, trace_offset, weights, frequency, slowness, vel_index):
    F = lax.axis_size("freq")
    L = lax.axis_size("lat")
    devices = F * L
    steps, rows, ny = vel_index.shape
    nx = rows * L
    tiles = (nx // TB) * (ny // TB) // devices
    slots = tiles * CAP
    count = spectra.shape[2]
    data_rows = 2 * spectra.shape[1]
    padded = -(-(data_rows + 3) // 16) * 16
    band = ny // L
    lanes = 2 * band
    nvel = slowness.shape[1]
    mode_rows = nx // TB * MODES
    cfg = (F, L, tiles, nx, ny, rows, band, data_rows, padded, steps, nvel)

    hart = jnp.asarray(two_parts(hartley(nx)))
    modes = two_parts(mode_table(nx))
    modes_t = jnp.asarray(np.ascontiguousarray(modes.transpose(0, 2, 1)))
    modes = jnp.asarray(modes)

    f32, bf16 = jnp.float32, jnp.bfloat16
    between = max(steps - 1, 1)
    dma = pltpu.SemaphoreType.DMA
    wave, image = pl.pallas_call(
        functools.partial(program, cfg),
        out_shape=[
            jax.ShapeDtypeStruct((2, rows, ny), f32),
            jax.ShapeDtypeStruct((steps, rows, ny // F), f32),
        ],
        in_specs=[VMEM, VMEM, VMEM, VMEM, VMEM, SMEM, SMEM, ANY, ANY, ANY, ANY],
        out_specs=[VMEM, VMEM],
        scratch_shapes=[
            pltpu.VMEM((2, nx, nx), bf16),
            pltpu.VMEM((2, mode_rows, nx), bf16),
            pltpu.VMEM((2, nx, mode_rows), bf16),
            pltpu.VMEM((steps, rows, ny), jnp.int32),
            pltpu.VMEM((devices, padded, slots), f32),
            pltpu.VMEM((devices, padded, slots), f32),
            pltpu.VMEM((tiles, TERMS, TERMS + data_rows), f32),
            pltpu.VMEM((F, 2, MODES, tiles * MODES), f32),
            pltpu.VMEM((devices, 2, MODES, tiles * MODES), f32),
            pltpu.VMEM((REFS, nx, ny), f32),
            pltpu.VMEM((REFS, nx, ny), f32),
            pltpu.VMEM((between, REFS, nx, lanes), f32),
            pltpu.VMEM((between, REFS, nx, lanes), f32),
            pltpu.VMEM((steps, rows, ny), f32),
            pltpu.VMEM((steps, rows, ny), f32),
            pltpu.VMEM((between, L, rows, lanes), f32),
            pltpu.VMEM((between, L, rows, lanes), f32),
            pltpu.VMEM((between, L, rows, REFS * lanes), f32),
            pltpu.VMEM((between, L, rows, REFS * lanes), f32),
            pltpu.VMEM((steps, F, rows, ny // F), f32),
            pltpu.VMEM((steps, F, rows, ny // F), f32),
            dma((4,)),
            dma((devices,)),
            dma((devices,)),
            dma((devices,)),
            dma((devices,)),
            dma((between, L)),
            dma((between, L)),
            dma((between, L)),
            dma((between, L)),
            dma((steps, F)),
            dma((steps, F)),
        ],
        compiler_params=pltpu.CompilerParams(
            collective_id=0, has_side_effects=True, vmem_limit_bytes=56 << 20
        ),
    )(
        spectra,
        tile_route.reshape(1, count),
        bin_in_tile.reshape(1, count),
        trace_offset,
        weights.reshape(1, count),
        frequency,
        slowness,
        vel_index,
        hart,
        modes,
        modes_t,
    )
    return wave[:, None], image


def solution(mesh):
    return jax.shard_map(
        local,
        mesh=mesh,
        in_specs=(
            P(None, None, ("freq", "lat")),
            P(("freq", "lat"), None),
            P(("freq", "lat")),
            P(None, ("freq", "lat")),
            P(("freq", "lat")),
            P("freq"),
            P(),
            P(None, "lat", None),
        ),
        out_specs=(P(None, "freq", "lat", None), P(None, "lat", "freq")),
        check_vma=False,
    )
```

```python
import functools
import math

import jax
import jax.numpy as jnp
import numpy as np
from jax import lax
from jax.experimental import pallas as pl
from jax.experimental.pallas import tpu as pltpu
from jax.sharding import PartitionSpec as P

TB = 32
MODES = 8
CAP = 8
TERMS = MODES * MODES
REFS = 2

damping = 1.0
depth_step = 1.0

NN = (((1,), (0,)), ((), ()))
NT = (((1,), (1,)), ((), ()))
VMEM = pl.BlockSpec(memory_space=pltpu.VMEM)
SMEM = pl.BlockSpec(memory_space=pltpu.SMEM)
HBM = pl.BlockSpec(memory_space=pltpu.HBM)
MESH = pl.DeviceIdType.MESH


def two_parts(exact):
    high = exact.astype(jnp.bfloat16)
    low = (exact - high.astype(np.float64)).astype(jnp.bfloat16)
    return high, low


def hartley(length):
    at = np.arange(length)
    angle = 2.0 * math.pi / length * (at[:, None] * at[None, :] % length)
    return (np.cos(angle) + np.sin(angle)) / math.sqrt(length)


def half_tables(length):
    whole = hartley(length)[:, : length // 2]
    even, odd = whole[0::2], whole[1::2]
    return np.stack([np.stack(two_parts(one), 0) for one in (even, odd, odd.T)], 0)


def mode_tables(length):
    cosines = np.cos(math.pi * np.arange(MODES)[:, None] * (np.arange(TB)[None, :] + 0.5) / TB)
    count = length // TB // 2
    fold = np.zeros((count, MODES, length))
    for tile in range(count):
        fold[tile, :, tile * TB : (tile + 1) * TB] = cosines
    whole = fold.reshape(count * MODES, length) @ hartley(length)
    left, right = [], []
    for parity in range(2):
        high, low = two_parts(whole[:, parity::2])
        right.append(np.concatenate([high, high, low], 0))
        left.append(np.concatenate([high.T, low.T, high.T], 1))
    return np.stack(left, 0), np.stack(right, 0)


def split2(x):
    high = x.astype(jnp.bfloat16)
    return high, (x - high.astype(jnp.float32)).astype(jnp.bfloat16)


def dot(a, b, dims=NN):
    return lax.dot_general(a, b, dims, preferred_element_type=jnp.float32)


def dot3(a, b, dims=NN):
    return dot(a[0], b[0], dims) + (dot(a[0], b[1], dims) + dot(a[1], b[0], dims))


def series(value, first, count):
    total = jnp.full(value.shape, 1.0 / math.factorial(2 * (count - 1) + first), jnp.float32)
    for n in range(count - 2, -1, -1):
        total = 1.0 / math.factorial(2 * n + first) - value * total
    return total


def cosine_of(cell):
    angle = (0.5 * TB - (cell + 0.5)) * (math.pi / TB)
    return angle * series(angle * angle, 1, 9)


def propagator(wave_squared, kx, ky):
    vertical = wave_squared - kx * kx - ky * ky
    root = jnp.sqrt(jnp.abs(vertical)) * depth_step
    squared = root * root
    moving = vertical > 0.0
    even = jnp.where(moving, series(squared, 0, 10), jnp.exp(-root))
    odd = jnp.where(moving, root * series(squared, 1, 10), 0.0)
    return even, odd


def signed(place, length):
    half = length // 2
    index = 2 * lax.rem(place, half) + lax.div(place, half)
    return 2.0 * math.pi / length * jnp.where(index >= half, index - length, index).astype(jnp.float32)


def iota(shape, axis):
    return lax.broadcasted_iota(jnp.int32, shape, axis)


def program(
    cfg,
    spectra_hbm,
    tile_hbm,
    bin_hbm,
    offset_hbm,
    weight_hbm,
    freq_ref,
    slow_ref,
    vel_hbm,
    hart_hbm,
    modes_x_hbm,
    modes_y_hbm,
    wave_ref,
    image_ref,
    spectra_ref,
    tile_ref,
    bin_ref,
    offset_ref,
    weight_ref,
    hart,
    modes_x,
    modes_y,
    vel_first,
    vel_last,
    route_out,
    route_in,
    system,
    coef_out,
    coef_in,
    wide_even,
    wide_odd,
    band_even,
    band_odd,
    along_first,
    across_first,
    along_last,
    across_last,
    fwd_out,
    fwd_in,
    back_out,
    back_in,
    image_out,
    image_in,
    trace_sem,
    table_sem,
    route_sent,
    route_got,
    coef_sent,
    coef_got,
    vel_sem,
    fwd_sent,
    fwd_got,
    back_sent,
    back_got,
    image_sent,
    image_got,
):
    F, L, tiles, nx, ny, rows, data_rows, padded, nvel = cfg
    devices = F * L
    group = L // 2
    half_x, half_y = nx // 2, ny // 2
    band = ny // group
    slots = tiles * CAP
    per_group = nvel // REFS
    me_f = lax.axis_index("freq")
    me_l = lax.axis_index("lat")
    me = me_l * F + me_f
    side = lax.div(me_l, group)
    seat = lax.rem(me_l, group)

    barrier = pltpu.get_barrier_semaphore()

    def partner_of(at):
        step = devices // 2 + (1 - 2 * lax.rem(at, 2)) * lax.div(at, 2)
        other = lax.rem(me + step, devices)
        return other, {"freq": lax.rem(other, F), "lat": lax.div(other, F)}

    def greet(at, carry):
        _, device = partner_of(at)
        pl.semaphore_signal(barrier, inc=1, device_id=device, device_id_type=MESH)
        return carry

    inputs = [
        pltpu.make_async_copy(src, dst, trace_sem.at[at])
        for at, (src, dst) in enumerate(
            [
                (tile_hbm, tile_ref),
                (bin_hbm, bin_ref),
                (offset_hbm, offset_ref),
                (weight_hbm, weight_ref),
                (spectra_hbm, spectra_ref),
            ]
        )
    ]
    for load in inputs:
        load.start()
    lax.fori_loop(1, devices, greet, 0)
    loads = [
        pltpu.make_async_copy(src, dst, table_sem.at[at])
        for at, (src, dst) in enumerate(
            [
                (vel_hbm.at[0], vel_first.at[side]),
                (vel_hbm.at[1], vel_last),
                (modes_x_hbm, modes_x),
                (modes_y_hbm, modes_y),
                (hart_hbm, hart),
            ]
        )
    ]
    for load in loads:
        load.start()
    for load in inputs:
        load.wait()

    count = tile_ref.shape[1]
    width = 128
    tile = tile_ref[...]
    columns = [
        jnp.transpose(jnp.broadcast_to(tile[:, at : at + width], (width, width)))
        for at in range(0, count, width)
    ]
    earlier = iota((width, width), 0) < iota((width, width), 1)
    ranks = []
    for at in range(count // width):
        row = jnp.broadcast_to(tile[:, at * width : (at + 1) * width], (width, width))
        same = jnp.where((columns[at] == row) & earlier, 1, 0)
        for before in range(at):
            same = same + jnp.where(columns[before] == row, 1, 0)
        ranks.append(jnp.sum(same, 0, keepdims=True))
    rank = jnp.concatenate(ranks, 1)
    turned = lax.rem(lax.rem(tile, tiles) + me, tiles)
    slot = lax.div(tile, tiles) * slots + turned * CAP + rank

    cell = bin_ref[...]
    root_weight = jnp.sqrt(weight_ref[...])
    cell_x = lax.div(cell, TB).astype(jnp.float32) + offset_ref[0:1, :]
    cell_y = lax.rem(cell, TB).astype(jnp.float32) + offset_ref[1:2, :]
    feats = jnp.concatenate(
        [spectra_ref[0] * root_weight, spectra_ref[1] * root_weight]
        + [root_weight, cosine_of(cell_x), cosine_of(cell_y)]
        + [jnp.zeros((padded - data_rows - 3, count), jnp.float32)],
        0,
    )
    high = feats.astype(jnp.bfloat16)
    rest = feats - high.astype(jnp.float32)
    middle = rest.astype(jnp.bfloat16)
    low = (rest - middle.astype(jnp.float32)).astype(jnp.bfloat16)
    parts = jnp.concatenate([high, middle, low], 0)
    wide = 256
    for at in range(0, devices * slots, wide):
        places = iota((wide, count), 0) + at
        chosen = jnp.where(places == slot, 1.0, 0.0).astype(jnp.bfloat16)
        got = dot(parts, chosen, NT)
        got = got[:padded] + got[padded : 2 * padded] + got[2 * padded :]
        for piece in range(wide // slots):
            route_out[at // slots + piece] = got[:, piece * slots : (piece + 1) * slots]

    pl.semaphore_wait(barrier, devices - 1)

    def spread(out, into, sent, landed):
        def copy_of(at):
            other, device = partner_of(at)
            return pltpu.make_async_remote_copy(
                src_ref=out.at[other] if out.shape[0] == devices else out.at[lax.rem(other, F)],
                dst_ref=into.at[me],
                send_sem=sent.at[at],
                recv_sem=landed.at[at],
                device_id=device,
                device_id_type=MESH,
            )

        def start(at, carry):
            copy_of(at).start()
            return carry

        def arrive(at, carry):
            copy_of(at).wait_recv()
            return carry

        def leave(at, carry):
            copy_of(at).wait_send()
            return carry

        lax.fori_loop(1, devices, start, 0)
        return (
            lambda: lax.fori_loop(1, devices, arrive, 0),
            lambda: lax.fori_loop(1, devices, leave, 0),
        )

    arrive, leave_route = spread(route_out, route_in, route_sent, route_got)
    route_in[pl.ds(me, 1)] = route_out[pl.ds(me, 1)]

    frequency = freq_ref[0]
    waves = []
    for depth_at in range(2):
        squares = []
        for g in range(REFS):
            total = slow_ref[depth_at, g * per_group]
            for i in range(1, per_group):
                total = total + slow_ref[depth_at, g * per_group + i]
            reference = total * (1.0 / per_group)
            squares.append((reference, (frequency * reference) * (frequency * reference)))
        waves.append(squares)

    chunk = 8

    def wide_tables(at, carry):
        first = pl.multiple_of(at * chunk, chunk)
        kx = signed(iota((chunk, ny), 0) + first, nx)
        ky = signed(iota((chunk, ny), 1), ny)
        for g in range(REFS):
            even, odd = propagator(waves[0][g][1], kx, ky)
            wide_even[g, pl.ds(first, chunk), :] = even
            wide_odd[g, pl.ds(first, chunk), :] = odd
        return carry

    lax.fori_loop(0, nx // chunk, wide_tables, 0)
    for load in loads:
        load.wait()
    arrive()

    mirror = pltpu.make_async_remote_copy(
        src_ref=vel_first.at[side],
        dst_ref=vel_first.at[side],
        send_sem=vel_sem.at[0],
        recv_sem=vel_sem.at[1],
        device_id={"lat": lax.rem(me_l + group, L)},
        device_id_type=MESH,
    )
    mirror.start()

    group_at = lax.div(iota((padded, slots), 1), CAP)
    eye = jnp.where(iota((TERMS, TERMS + data_rows), 0) == iota((TERMS, TERMS + data_rows), 1), damping, 0.0)

    def chebyshev(cosine):
        terms = [jnp.ones_like(cosine), cosine]
        for _ in range(MODES - 2):
            terms.append(2.0 * cosine * terms[-1] - terms[-2])
        return terms

    for t in range(tiles):
        pieces = []
        for first in range(0, devices, tiles):
            picked = route_in[first]
            for i in range(1, tiles):
                picked = jnp.where(group_at == (t + i) % tiles, route_in[first + i], picked)
            pieces.append(picked)
        got = jnp.concatenate(pieces, 1)
        scale = got[data_rows : data_rows + 1]
        along_x = chebyshev(got[data_rows + 1 : data_rows + 2])
        along_y = jnp.concatenate(chebyshev(got[data_rows + 2 : data_rows + 3]), 0)
        basis = jnp.concatenate([(term * scale) * along_y for term in along_x], 0)
        right = jnp.concatenate([basis, got[:data_rows]], 0)
        system[t] = eye + lax.dot_general(
            basis, right, NT, preferred_element_type=jnp.float32, precision=lax.Precision.HIGHEST
        )
    for k in range(TERMS):
        row = system[:, k : k + 1, :]
        scaled = row * (1.0 / row[:, :, k : k + 1])
        whole = system[...]
        system[...] = whole - whole[:, :, k : k + 1] * scaled
        system[:, k : k + 1, :] = scaled
    solved = [jnp.transpose(system[t])[TERMS:] for t in range(tiles)]
    for a in range(MODES):
        line = jnp.concatenate([one[:, a * MODES : (a + 1) * MODES] for one in solved], 1)
        for part in range(2):
            for f in range(F):
                at = part * F + f
                coef_out[f, part, a : a + 1, :] = line[at : at + 1]

    arrive, leave_coef = spread(coef_out, coef_in, coef_sent, coef_got)
    coef_in[pl.ds(me, 1)] = coef_out[pl.ds(me_f, 1)]

    ky = signed(seat * band + iota((chunk, band), 1), ny)

    def band_tables(at, carry):
        first = pl.multiple_of(at * chunk, chunk)
        kx = signed(iota((chunk, band), 0) + first, nx)
        for g in range(REFS):
            even, odd = propagator(waves[1][g][1], kx, ky)
            band_even[g, pl.ds(first, chunk), :] = even
            band_odd[g, pl.ds(first, chunk), :] = odd
        return carry

    lax.fori_loop(0, nx // chunk, band_tables, 0)

    def split_step(depth_at, velocity):
        cosine = jnp.zeros(velocity.shape, jnp.float32)
        sine = jnp.zeros(velocity.shape, jnp.float32)
        for i in range(nvel):
            shift = slow_ref[depth_at, i] - waves[depth_at][i // per_group][0]
            angle = jnp.full((8, 128), frequency * shift * depth_step, jnp.float32)
            squared = angle * angle
            cosine_i = series(squared, 0, 9)[0:1, 0:1]
            sine_i = (angle * series(squared, 1, 9))[0:1, 0:1]
            cosine = jnp.where(velocity == i, cosine_i, cosine)
            sine = jnp.where(velocity == i, sine_i, sine)
        return cosine, sine

    along_last[...], across_last[...] = split_step(1, vel_last[...])
    mirror.wait_recv()
    for one in range(2):
        along_first[one], across_first[one] = split_step(0, vel_first[one])
    arrive()

    def part_of(which):
        return hart[which, 0], hart[which, 1]

    even_k, odd_k, odd_k_t = part_of(0), part_of(1), part_of(2)

    def from_modes_of(parts):
        return jnp.concatenate([parts[0], parts[1], parts[0]], 1)

    per_row = (ny // TB) // tiles
    tile_rows = nx // TB
    mode_rows = tile_rows // 2 * MODES
    mode_columns = ny // TB // 2 * MODES
    sums, differences = [], []
    for part in range(2):
        lines = [
            jnp.concatenate([coef_in[tile_row * per_row + j, part] for j in range(per_row)], 1)
            for tile_row in range(tile_rows)
        ]
        upper = jnp.concatenate(lines[: tile_rows // 2], 0)
        lower = jnp.concatenate(lines[tile_rows // 2 :], 0)
        for one in (upper + lower, upper - lower):
            left, right = one[:, :mode_columns], one[:, mode_columns:]
            sums.append(left + right)
            differences.append(left - right)
    spread_y = [
        dot(from_modes_of(split2(jnp.concatenate(one, 0))), modes_y[parity])
        for parity, one in enumerate((sums, differences))
    ]
    seat_rows = pl.ds(pl.multiple_of(seat * rows, rows), rows)
    made = [[None, None] for _ in range(REFS)]
    for parity in range(2):
        picked = [
            one[(2 * p + parity) * mode_rows : (2 * p + parity + 1) * mode_rows]
            for p in range(2)
            for one in spread_y
        ]
        high, low = split2(jnp.concatenate(picked, 1))
        spectrum = dot(modes_x[parity], jnp.concatenate([high, high, low], 0))
        real, imag = spectrum[:, :ny], spectrum[:, ny:]
        which = 0 if parity == 0 else 2
        own_high, own_low = hart[which, 0, seat_rows, :], hart[which, 1, seat_rows, :]
        both = jnp.concatenate([own_high, own_low], 0)
        part = slice(parity * half_x, (parity + 1) * half_x)
        for g in range(REFS):
            even, odd = wide_even[g, part, :], wide_odd[g, part, :]
            moved = split2(jnp.concatenate([real * even - imag * odd, real * odd + imag * even], 1))
            back = dot(both, moved[0])
            made[g][parity] = back[:rows] + (back[rows:] + dot(own_high, moved[1]))
    pieces = []
    for g in range(REFS):
        slabs = (made[g][0] + made[g][1], made[g][0] - made[g][1])
        for p in range(2):
            pieces += [slab[:, p * ny : (p + 1) * ny] for slab in slabs]

    def inverse_y(x):
        u = dot3(split2(x[:, :half_y]), even_k)
        v = dot3(split2(x[:, half_y:]), odd_k)
        return jnp.concatenate([u + v, u - v], 1)

    def choose(made, velocity):
        real, imag = made[0]
        for g in range(1, REFS):
            chosen = velocity >= g * per_group
            real = jnp.where(chosen, made[g][0], real)
            imag = jnp.where(chosen, made[g][1], imag)
        return real, imag

    image_piece = ny // F

    def send_image(depth_at, real):
        for f in range(F):
            image_out[depth_at, f] = real[:, f * image_piece : (f + 1) * image_piece]
        copies = []
        for step in range(1, F):
            other = lax.rem(me_f + step, F)
            copies.append(
                pltpu.make_async_remote_copy(
                    src_ref=image_out.at[depth_at, other],
                    dst_ref=image_in.at[depth_at, me_f],
                    send_sem=image_sent.at[depth_at, step],
                    recv_sem=image_got.at[depth_at, step],
                    device_id={"freq": other},
                    device_id_type=MESH,
                )
            )
        for copy in copies:
            copy.start()
        image_in[depth_at, pl.ds(me_f, 1)] = image_out[depth_at, pl.ds(me_f, 1)]
        return copies

    def exchange(at, out, into, sent, landed):
        copies = []
        for step in range(1, group):
            other = lax.rem(seat + step, group)
            copies.append(
                pltpu.make_async_remote_copy(
                    src_ref=out.at[at, other],
                    dst_ref=into.at[at, seat],
                    send_sem=sent.at[at, step],
                    recv_sem=landed.at[at, step],
                    device_id={"lat": side * group + other},
                    device_id_type=MESH,
                )
            )
        for copy in copies:
            copy.start()
        into[at, pl.ds(seat, 1)] = out[at, pl.ds(seat, 1)]
        return copies

    field = inverse_y(jnp.concatenate(pieces, 0))
    two = 2 * rows
    real, imag = choose(
        [(field[2 * g * two : (2 * g + 1) * two], field[(2 * g + 1) * two : (2 * g + 2) * two]) for g in range(REFS)],
        vel_first[...].reshape(two, ny),
    )
    cosine, sine = along_first[...].reshape(two, ny), across_first[...].reshape(two, ny)
    real, imag = real * cosine - imag * sine, real * sine + imag * cosine
    forward = []
    for p, one in enumerate((real, imag)):
        left, right = one[:, :half_y], one[:, half_y:]
        line = jnp.concatenate(
            [dot3(split2(left + right), even_k), dot3(split2(left - right), odd_k_t)], 1
        )
        for dst in range(group):
            fwd_out[p, dst] = line[:, dst * band : (dst + 1) * band].reshape(2, rows, band)
        forward.append(exchange(p, fwd_out, fwd_in, fwd_sent, fwd_got))
    first_image = send_image(0, jnp.where(side == 0, real[:rows], real[rows:]))

    spectrum = []
    for p in range(2):
        for copy in forward[p]:
            copy.wait_recv()
        upper = jnp.concatenate([fwd_in[p, src, 0] for src in range(group)], 0)
        lower = jnp.concatenate([fwd_in[p, src, 1] for src in range(group)], 0)
        lines = []
        for one, table in ((upper + lower, even_k), (upper - lower, odd_k)):
            high, low = split2(one)
            line = dot(table[0], jnp.concatenate([high, low], 1))
            lines.append(line[:, :band] + (line[:, band:] + dot(table[1], high)))
        spectrum.append(lines)
    turn = (1 - 2 * side).astype(jnp.float32)
    backward = []
    for g in range(REFS):
        sides = []
        for parity, table in enumerate((even_k, odd_k_t)):
            part = slice(parity * half_x, (parity + 1) * half_x)
            even, odd = band_even[g, part, :], band_odd[g, part, :]
            real, imag = spectrum[0][parity], spectrum[1][parity]
            moved = jnp.concatenate([real * even - imag * odd, real * odd + imag * even], 1)
            sides.append(dot3(table, split2(moved)))
        back_out[g] = (sides[0] + turn * sides[1]).reshape(group, rows, 2 * band)
        backward.append(exchange(g, back_out, back_in, back_sent, back_got))
    made = []
    for g in range(REFS):
        for copy in backward[g]:
            copy.wait_recv()
        lines = [
            jnp.concatenate([back_in[g, src, :, p * band : (p + 1) * band] for src in range(group)], 1)
            for p in range(2)
        ]
        field = inverse_y(jnp.concatenate(lines, 0))
        made.append((field[:rows], field[rows:]))
    real, imag = choose(made, vel_last[...])
    cosine, sine = along_last[...], across_last[...]
    moved = real * cosine - imag * sine
    last_image = send_image(1, moved)
    wave_ref[0] = moved
    wave_ref[1] = real * sine + imag * cosine

    leave_route()
    leave_coef()
    mirror.wait_send()
    for copies in forward + backward:
        for copy in copies:
            copy.wait_send()
    for depth_at, copies in enumerate((first_image, last_image)):
        for copy in copies:
            copy.wait()
        total = image_in[depth_at, 0]
        for f in range(1, F):
            total = total + image_in[depth_at, f]
        image_ref[depth_at] = total


def stay(x):
    return pltpu.with_memory_space_constraint(x, pltpu.HBM)


def local(spectra, tile_route, bin_in_tile, trace_offset, weights, frequency, slowness, vel_index):
    F = lax.axis_size("freq")
    L = lax.axis_size("lat")
    devices = F * L
    steps, rows, ny = vel_index.shape
    assert steps == 2
    nx = rows * L
    tiles = (nx // TB) * (ny // TB) // devices
    slots = tiles * CAP
    count = spectra.shape[2]
    data_rows = 2 * spectra.shape[1]
    padded = -(-(data_rows + 3) // 16) * 16
    group = L // 2
    band = ny // group
    nvel = slowness.shape[1]
    cfg = (F, L, tiles, nx, ny, rows, data_rows, padded, nvel)

    hart = jnp.asarray(half_tables(nx))
    modes_x, modes_y = (jnp.asarray(one) for one in mode_tables(nx))

    f32, bf16, i32 = jnp.float32, jnp.bfloat16, jnp.int32
    dma = pltpu.SemaphoreType.DMA
    wave, image = pl.pallas_call(
        functools.partial(program, cfg),
        out_shape=[
            jax.ShapeDtypeStruct((2, rows, ny), f32),
            jax.ShapeDtypeStruct((2, rows, ny // F), f32),
        ],
        in_specs=[HBM] * 5 + [SMEM] * 2 + [HBM] * 4,
        out_specs=[VMEM, VMEM],
        scratch_shapes=[
            pltpu.VMEM(spectra.shape, f32),
            pltpu.VMEM((1, count), i32),
            pltpu.VMEM((1, count), i32),
            pltpu.VMEM((2, count), f32),
            pltpu.VMEM((1, count), f32),
            pltpu.VMEM(hart.shape, bf16),
            pltpu.VMEM(modes_x.shape, bf16),
            pltpu.VMEM(modes_y.shape, bf16),
            pltpu.VMEM((2, rows, ny), i32),
            pltpu.VMEM((rows, ny), i32),
            pltpu.VMEM((devices, padded, slots), f32),
            pltpu.VMEM((devices, padded, slots), f32),
            pltpu.VMEM((tiles, TERMS, TERMS + data_rows), f32),
            pltpu.VMEM((F, 2, MODES, tiles * MODES), f32),
            pltpu.VMEM((devices, 2, MODES, tiles * MODES), f32),
            pltpu.VMEM((REFS, nx, ny), f32),
            pltpu.VMEM((REFS, nx, ny), f32),
            pltpu.VMEM((REFS, nx, band), f32),
            pltpu.VMEM((REFS, nx, band), f32),
            pltpu.VMEM((2, rows, ny), f32),
            pltpu.VMEM((2, rows, ny), f32),
            pltpu.VMEM((rows, ny), f32),
            pltpu.VMEM((rows, ny), f32),
            pltpu.VMEM((2, group, 2, rows, band), f32),
            pltpu.VMEM((2, group, 2, rows, band), f32),
            pltpu.VMEM((REFS, group, rows, 2 * band), f32),
            pltpu.VMEM((REFS, group, rows, 2 * band), f32),
            pltpu.VMEM((2, F, rows, ny // F), f32),
            pltpu.VMEM((2, F, rows, ny // F), f32),
            dma((5,)),
            dma((5,)),
            dma((devices,)),
            dma((devices,)),
            dma((devices,)),
            dma((devices,)),
            dma((2,)),
            dma((2, group)),
            dma((2, group)),
            dma((REFS, group)),
            dma((REFS, group)),
            dma((2, F)),
            dma((2, F)),
        ],
        compiler_params=pltpu.CompilerParams(
            collective_id=0, has_side_effects=True, vmem_limit_bytes=40 << 20
        ),
    )(
        *map(stay, (spectra, tile_route.reshape(1, count), bin_in_tile.reshape(1, count))),
        *map(stay, (trace_offset, weights.reshape(1, count))),
        frequency,
        stay(slowness),
        *map(stay, (vel_index, hart, modes_x, modes_y)),
    )
    return wave[:, None], image


def solution(mesh):
    return jax.shard_map(
        local,
        mesh=mesh,
        in_specs=(
            P(None, None, ("freq", "lat")),
            P(("freq", "lat"), None),
            P(("freq", "lat")),
            P(None, ("freq", "lat")),
            P(("freq", "lat")),
            P("freq"),
            P(),
            P(None, "lat", None),
        ),
        out_specs=(P(None, "freq", "lat", None), P(None, "lat", "freq")),
        check_vma=False,
    )
```

```python
import functools
import math

import jax
import jax.numpy as jnp
import numpy as np
from jax import lax
from jax.experimental import pallas as pl
from jax.experimental.pallas import tpu as pltpu
from jax.sharding import PartitionSpec as P

TB = 32
MODES = 8
CAP = 8
TERMS = MODES * MODES
REFS = 2

damping = 1.0
depth_step = 1.0

NN = (((1,), (0,)), ((), ()))
NT = (((1,), (1,)), ((), ()))
VMEM = pl.BlockSpec(memory_space=pltpu.VMEM)
SMEM = pl.BlockSpec(memory_space=pltpu.SMEM)
HBM = pl.BlockSpec(memory_space=pltpu.HBM)
MESH = pl.DeviceIdType.MESH


def two_parts(exact):
    high = exact.astype(jnp.bfloat16)
    low = (exact - high.astype(np.float64)).astype(jnp.bfloat16)
    return high, low


def hartley(length):
    at = np.arange(length)
    angle = 2.0 * math.pi / length * (at[:, None] * at[None, :] % length)
    return (np.cos(angle) + np.sin(angle)) / math.sqrt(length)


def half_tables(length):
    whole = hartley(length)[:, : length // 2]
    even, odd = whole[0::2], whole[1::2]
    return np.stack([np.stack(two_parts(one), 0) for one in (even, odd, odd.T)], 0)


def mode_tables(length):
    cosines = np.cos(math.pi * np.arange(MODES)[:, None] * (np.arange(TB)[None, :] + 0.5) / TB)
    count = length // TB // 2
    fold = np.zeros((count, MODES, length))
    for tile in range(count):
        fold[tile, :, tile * TB : (tile + 1) * TB] = cosines
    whole = fold.reshape(count * MODES, length) @ hartley(length)
    left, right = [], []
    for parity in range(2):
        high, low = two_parts(whole[:, parity::2])
        right.append(np.concatenate([high, high, low], 0))
        left.append(np.concatenate([high.T, low.T, high.T], 1))
    return np.stack(left, 0), np.stack(right, 0)


def split2(x):
    high = x.astype(jnp.bfloat16)
    return high, (x - high.astype(jnp.float32)).astype(jnp.bfloat16)


def dot(a, b, dims=NN):
    return lax.dot_general(a, b, dims, preferred_element_type=jnp.float32)


def dot3(a, b, dims=NN):
    return dot(a[0], b[0], dims) + (dot(a[0], b[1], dims) + dot(a[1], b[0], dims))


def series(value, first, count):
    total = jnp.full(value.shape, 1.0 / math.factorial(2 * (count - 1) + first), jnp.float32)
    for n in range(count - 2, -1, -1):
        total = 1.0 / math.factorial(2 * n + first) - value * total
    return total


def cosine_of(cell):
    angle = (0.5 * TB - (cell + 0.5)) * (math.pi / TB)
    return angle * series(angle * angle, 1, 9)


def propagator(wave_squared, kx, ky):
    vertical = wave_squared - kx * kx - ky * ky
    root = jnp.sqrt(jnp.abs(vertical)) * depth_step
    squared = root * root
    moving = vertical > 0.0
    even = jnp.where(moving, series(squared, 0, 10), jnp.exp(-root))
    odd = jnp.where(moving, root * series(squared, 1, 10), 0.0)
    return even, odd


def signed(place, length):
    half = length // 2
    index = 2 * lax.rem(place, half) + lax.div(place, half)
    return 2.0 * math.pi / length * jnp.where(index >= half, index - length, index).astype(jnp.float32)


def iota(shape, axis):
    return lax.broadcasted_iota(jnp.int32, shape, axis)


def program(
    cfg,
    spectra_hbm,
    tile_hbm,
    bin_hbm,
    offset_hbm,
    weight_hbm,
    freq_ref,
    slow_ref,
    vel_hbm,
    hart_hbm,
    modes_x_hbm,
    modes_y_hbm,
    wave_ref,
    image_ref,
    spectra_ref,
    tile_ref,
    bin_ref,
    offset_ref,
    weight_ref,
    hart,
    modes_x,
    modes_y,
    vel_first,
    vel_last,
    route_out,
    route_in,
    system,
    coef_out,
    coef_in,
    wide_even,
    wide_odd,
    band_even,
    band_odd,
    along_first,
    across_first,
    along_last,
    across_last,
    fwd_out,
    fwd_in,
    back_out,
    back_in,
    image_out,
    image_in,
    trace_sem,
    table_sem,
    route_sent,
    route_got,
    coef_sent,
    coef_got,
    vel_sem,
    fwd_sent,
    fwd_got,
    back_sent,
    back_got,
    image_sent,
    image_got,
):
    F, L, tiles, nx, ny, rows, data_rows, padded, nvel = cfg
    devices = F * L
    group = L // 2
    half_x, half_y = nx // 2, ny // 2
    band = ny // group
    slots = tiles * CAP
    per_group = nvel // REFS
    me_f = lax.axis_index("freq")
    me_l = lax.axis_index("lat")
    me = me_l * F + me_f
    side = lax.div(me_l, group)
    seat = lax.rem(me_l, group)

    barrier = pltpu.get_barrier_semaphore()

    def partner_of(at):
        other = lax.rem(me + at, devices)
        return other, {"freq": lax.rem(other, F), "lat": lax.div(other, F)}

    def greet(at, carry):
        _, device = partner_of(at)
        pl.semaphore_signal(barrier, inc=1, device_id=device, device_id_type=MESH)
        return carry

    inputs = [
        pltpu.make_async_copy(src, dst, trace_sem.at[at])
        for at, (src, dst) in enumerate(
            [
                (tile_hbm, tile_ref),
                (bin_hbm, bin_ref),
                (offset_hbm, offset_ref),
                (weight_hbm, weight_ref),
                (spectra_hbm, spectra_ref),
            ]
        )
    ]
    for load in inputs:
        load.start()
    lax.fori_loop(1, devices, greet, 0)
    loads = [
        pltpu.make_async_copy(src, dst, table_sem.at[at])
        for at, (src, dst) in enumerate(
            [
                (vel_hbm.at[0], vel_first.at[side]),
                (vel_hbm.at[1], vel_last),
                (modes_x_hbm, modes_x),
                (modes_y_hbm, modes_y),
                (hart_hbm, hart),
            ]
        )
    ]
    for load in loads:
        load.start()
    for load in inputs:
        load.wait()

    count = tile_ref.shape[1]
    width = 128
    tile = tile_ref[...]
    columns = [
        jnp.transpose(jnp.broadcast_to(tile[:, at : at + width], (width, width)))
        for at in range(0, count, width)
    ]
    earlier = iota((width, width), 0) < iota((width, width), 1)
    ranks = []
    for at in range(count // width):
        row = jnp.broadcast_to(tile[:, at * width : (at + 1) * width], (width, width))
        same = jnp.where((columns[at] == row) & earlier, 1, 0)
        for before in range(at):
            same = same + jnp.where(columns[before] == row, 1, 0)
        ranks.append(jnp.sum(same, 0, keepdims=True))
    rank = jnp.concatenate(ranks, 1)
    turned = lax.rem(lax.rem(tile, tiles) + me, tiles)
    slot = lax.div(tile, tiles) * slots + turned * CAP + rank

    cell = bin_ref[...]
    root_weight = jnp.sqrt(weight_ref[...])
    cell_x = lax.div(cell, TB).astype(jnp.float32) + offset_ref[0:1, :]
    cell_y = lax.rem(cell, TB).astype(jnp.float32) + offset_ref[1:2, :]
    feats = jnp.concatenate(
        [spectra_ref[0] * root_weight, spectra_ref[1] * root_weight]
        + [root_weight, cosine_of(cell_x), cosine_of(cell_y)]
        + [jnp.zeros((padded - data_rows - 3, count), jnp.float32)],
        0,
    )
    high = feats.astype(jnp.bfloat16)
    rest = feats - high.astype(jnp.float32)
    middle = rest.astype(jnp.bfloat16)
    low = (rest - middle.astype(jnp.float32)).astype(jnp.bfloat16)
    parts = jnp.concatenate([high, middle, low], 0)
    wide = 256
    for at in range(0, devices * slots, wide):
        places = iota((wide, count), 0) + at
        chosen = jnp.where(places == slot, 1.0, 0.0).astype(jnp.bfloat16)
        got = dot(parts, chosen, NT)
        got = got[:padded] + got[padded : 2 * padded] + got[2 * padded :]
        for piece in range(wide // slots):
            block = got[:, piece * slots : (piece + 1) * slots]
            route_out[at // slots + piece] = jnp.concatenate([block[:data_rows], block[data_rows:]], 1)

    pl.semaphore_wait(barrier, devices - 1)

    def spread(out, into, sent, landed):
        def copy_of(at):
            other, device = partner_of(at)
            return pltpu.make_async_remote_copy(
                src_ref=out.at[other] if out.shape[0] == devices else out.at[lax.rem(other, F)],
                dst_ref=into.at[me],
                send_sem=sent.at[at],
                recv_sem=landed.at[at],
                device_id=device,
                device_id_type=MESH,
            )

        def start(at, carry):
            copy_of(at).start()
            return carry

        def arrive(at, carry):
            copy_of(at).wait_recv()
            return carry

        def leave(at, carry):
            copy_of(at).wait_send()
            return carry

        lax.fori_loop(1, devices, start, 0)
        return (
            lambda: lax.fori_loop(1, devices, arrive, 0),
            lambda: lax.fori_loop(1, devices, leave, 0),
        )

    arrive, leave_route = spread(route_out, route_in, route_sent, route_got)
    route_in[pl.ds(me, 1)] = route_out[pl.ds(me, 1)]

    frequency = freq_ref[0]
    waves = []
    for depth_at in range(2):
        squares = []
        for g in range(REFS):
            total = slow_ref[depth_at, g * per_group]
            for i in range(1, per_group):
                total = total + slow_ref[depth_at, g * per_group + i]
            reference = total * (1.0 / per_group)
            squares.append((reference, (frequency * reference) * (frequency * reference)))
        waves.append(squares)

    chunk = 8

    def wide_tables(at, carry):
        first = pl.multiple_of(at * chunk, chunk)
        kx = signed(iota((chunk, ny), 0) + first, nx)
        ky = signed(iota((chunk, ny), 1), ny)
        for g in range(REFS):
            even, odd = propagator(waves[0][g][1], kx, ky)
            wide_even[g, pl.ds(first, chunk), :] = even
            wide_odd[g, pl.ds(first, chunk), :] = odd
        return carry

    lax.fori_loop(0, nx // chunk, wide_tables, 0)
    for load in loads:
        load.wait()
    arrive()

    mirror = pltpu.make_async_remote_copy(
        src_ref=vel_first.at[side],
        dst_ref=vel_first.at[side],
        send_sem=vel_sem.at[0],
        recv_sem=vel_sem.at[1],
        device_id={"lat": lax.rem(me_l + group, L)},
        device_id_type=MESH,
    )
    mirror.start()

    group_at = lax.div(lax.rem(iota((data_rows, 2 * slots), 1), slots), CAP)
    eye = jnp.where(iota((TERMS, TERMS + data_rows), 0) == iota((TERMS, TERMS + data_rows), 1), damping, 0.0)

    def chebyshev(cosine):
        terms = [jnp.ones_like(cosine), cosine]
        for _ in range(MODES - 2):
            terms.append(2.0 * cosine * terms[-1] - terms[-2])
        return terms

    for t in range(tiles):
        pieces = []
        for first in range(0, devices, tiles):
            picked = route_in[first]
            for i in range(1, tiles):
                picked = jnp.where(group_at == (t + i) % tiles, route_in[first + i], picked)
            pieces.append(picked)
        data = jnp.concatenate([piece[:, :slots] for piece in pieces], 1)
        place = jnp.concatenate([piece[:8, slots:] for piece in pieces], 1)
        scale = place[0:1]
        along_x = chebyshev(place[1:2])
        along_y = jnp.concatenate(chebyshev(place[2:3]), 0)
        basis = jnp.concatenate([(term * scale) * along_y for term in along_x], 0)
        right = jnp.concatenate([basis, data], 0)
        system[t] = eye + lax.dot_general(
            basis, right, NT, preferred_element_type=jnp.float32, precision=lax.Precision.HIGHEST
        )
    for k in range(TERMS):
        row = system[:, k : k + 1, :]
        scaled = row * (1.0 / row[:, :, k : k + 1])
        whole = system[...]
        system[...] = whole - whole[:, :, k : k + 1] * scaled
        system[:, k : k + 1, :] = scaled
    solved = [jnp.transpose(system[t])[TERMS:] for t in range(tiles)]
    width = tiles * MODES
    for a in range(MODES):
        line = jnp.concatenate([one[:, a * MODES : (a + 1) * MODES] for one in solved], 1)
        for part in range(2):
            for f in range(F):
                at = part * F + f
                coef_out[f, a : a + 1, part * width : (part + 1) * width] = line[at : at + 1]

    arrive, leave_coef = spread(coef_out, coef_in, coef_sent, coef_got)
    coef_in[pl.ds(me, 1)] = coef_out[pl.ds(me_f, 1)]

    ky = signed(seat * band + iota((chunk, band), 1), ny)

    def band_tables(at, carry):
        first = pl.multiple_of(at * chunk, chunk)
        kx = signed(iota((chunk, band), 0) + first, nx)
        for g in range(REFS):
            even, odd = propagator(waves[1][g][1], kx, ky)
            band_even[g, pl.ds(first, chunk), :] = even
            band_odd[g, pl.ds(first, chunk), :] = odd
        return carry

    lax.fori_loop(0, nx // chunk, band_tables, 0)

    def split_step(depth_at, velocity):
        cosine = jnp.zeros(velocity.shape, jnp.float32)
        sine = jnp.zeros(velocity.shape, jnp.float32)
        for i in range(nvel):
            shift = slow_ref[depth_at, i] - waves[depth_at][i // per_group][0]
            angle = jnp.full((8, 128), frequency * shift * depth_step, jnp.float32)
            squared = angle * angle
            cosine_i = series(squared, 0, 9)[0:1, 0:1]
            sine_i = (angle * series(squared, 1, 9))[0:1, 0:1]
            cosine = jnp.where(velocity == i, cosine_i, cosine)
            sine = jnp.where(velocity == i, sine_i, sine)
        return cosine, sine

    along_last[...], across_last[...] = split_step(1, vel_last[...])
    mirror.wait_recv()
    for one in range(2):
        along_first[one], across_first[one] = split_step(0, vel_first[one])
    arrive()

    def part_of(which):
        return hart[which, 0], hart[which, 1]

    even_k, odd_k, odd_k_t = part_of(0), part_of(1), part_of(2)

    def from_modes_of(parts):
        return jnp.concatenate([parts[0], parts[1], parts[0]], 1)

    per_row = (ny // TB) // tiles
    tile_rows = nx // TB
    mode_rows = tile_rows // 2 * MODES
    mode_columns = ny // TB // 2 * MODES
    sums, differences = [], []
    for part in range(2):
        lines = [
            jnp.concatenate(
                [
                    coef_in[tile_row * per_row + j, :, part * width : (part + 1) * width]
                    for j in range(per_row)
                ],
                1,
            )
            for tile_row in range(tile_rows)
        ]
        upper = jnp.concatenate(lines[: tile_rows // 2], 0)
        lower = jnp.concatenate(lines[tile_rows // 2 :], 0)
        for one in (upper + lower, upper - lower):
            left, right = one[:, :mode_columns], one[:, mode_columns:]
            sums.append(left + right)
            differences.append(left - right)
    spread_y = [
        dot(from_modes_of(split2(jnp.concatenate(one, 0))), modes_y[parity])
        for parity, one in enumerate((sums, differences))
    ]
    seat_rows = pl.ds(pl.multiple_of(seat * rows, rows), rows)
    made = [[None, None] for _ in range(REFS)]
    for parity in range(2):
        picked = [
            one[(2 * p + parity) * mode_rows : (2 * p + parity + 1) * mode_rows]
            for p in range(2)
            for one in spread_y
        ]
        high, low = split2(jnp.concatenate(picked, 1))
        spectrum = dot(modes_x[parity], jnp.concatenate([high, high, low], 0))
        real, imag = spectrum[:, :ny], spectrum[:, ny:]
        which = 0 if parity == 0 else 2
        own_high, own_low = hart[which, 0, seat_rows, :], hart[which, 1, seat_rows, :]
        both = jnp.concatenate([own_high, own_low], 0)
        part = slice(parity * half_x, (parity + 1) * half_x)
        for g in range(REFS):
            even, odd = wide_even[g, part, :], wide_odd[g, part, :]
            moved = split2(jnp.concatenate([real * even - imag * odd, real * odd + imag * even], 1))
            back = dot(both, moved[0])
            made[g][parity] = back[:rows] + (back[rows:] + dot(own_high, moved[1]))
    pieces = []
    for g in range(REFS):
        slabs = (made[g][0] + made[g][1], made[g][0] - made[g][1])
        for p in range(2):
            pieces += [slab[:, p * ny : (p + 1) * ny] for slab in slabs]

    def inverse_y(x):
        u = dot3(split2(x[:, :half_y]), even_k)
        v = dot3(split2(x[:, half_y:]), odd_k)
        return jnp.concatenate([u + v, u - v], 1)

    def choose(made, velocity):
        real, imag = made[0]
        for g in range(1, REFS):
            chosen = velocity >= g * per_group
            real = jnp.where(chosen, made[g][0], real)
            imag = jnp.where(chosen, made[g][1], imag)
        return real, imag

    image_piece = ny // F

    def send_image(depth_at, real):
        for f in range(F):
            image_out[depth_at, f] = real[:, f * image_piece : (f + 1) * image_piece]
        copies = []
        for step in range(1, F):
            other = lax.rem(me_f + step, F)
            copies.append(
                pltpu.make_async_remote_copy(
                    src_ref=image_out.at[depth_at, other],
                    dst_ref=image_in.at[depth_at, me_f],
                    send_sem=image_sent.at[depth_at, step],
                    recv_sem=image_got.at[depth_at, step],
                    device_id={"freq": other},
                    device_id_type=MESH,
                )
            )
        for copy in copies:
            copy.start()
        image_in[depth_at, pl.ds(me_f, 1)] = image_out[depth_at, pl.ds(me_f, 1)]
        return copies

    def exchange(at, out, into, sent, landed):
        copies = []
        for step in range(1, group):
            other = lax.rem(seat + step, group)
            copies.append(
                pltpu.make_async_remote_copy(
                    src_ref=out.at[at, other],
                    dst_ref=into.at[at, seat],
                    send_sem=sent.at[at, step],
                    recv_sem=landed.at[at, step],
                    device_id={"lat": side * group + other},
                    device_id_type=MESH,
                )
            )
        for copy in copies:
            copy.start()
        into[at, pl.ds(seat, 1)] = out[at, pl.ds(seat, 1)]
        return copies

    field = inverse_y(jnp.concatenate(pieces, 0))
    two = 2 * rows
    real, imag = choose(
        [(field[2 * g * two : (2 * g + 1) * two], field[(2 * g + 1) * two : (2 * g + 2) * two]) for g in range(REFS)],
        vel_first[...].reshape(two, ny),
    )
    cosine, sine = along_first[...].reshape(two, ny), across_first[...].reshape(two, ny)
    real, imag = real * cosine - imag * sine, real * sine + imag * cosine
    forward = []
    for p, one in enumerate((real, imag)):
        left, right = one[:, :half_y], one[:, half_y:]
        line = jnp.concatenate(
            [dot3(split2(left + right), even_k), dot3(split2(left - right), odd_k_t)], 1
        )
        for dst in range(group):
            fwd_out[p, dst] = line[:, dst * band : (dst + 1) * band].reshape(2, rows, band)
        forward.append(exchange(p, fwd_out, fwd_in, fwd_sent, fwd_got))
    first_image = send_image(0, jnp.where(side == 0, real[:rows], real[rows:]))

    spectrum = []
    for p in range(2):
        for copy in forward[p]:
            copy.wait_recv()
        upper = jnp.concatenate([fwd_in[p, src, 0] for src in range(group)], 0)
        lower = jnp.concatenate([fwd_in[p, src, 1] for src in range(group)], 0)
        lines = []
        for one, table in ((upper + lower, even_k), (upper - lower, odd_k)):
            high, low = split2(one)
            line = dot(table[0], jnp.concatenate([high, low], 1))
            lines.append(line[:, :band] + (line[:, band:] + dot(table[1], high)))
        spectrum.append(lines)
    turn = (1 - 2 * side).astype(jnp.float32)
    backward = []
    for g in range(REFS):
        sides = []
        for parity, table in enumerate((even_k, odd_k_t)):
            part = slice(parity * half_x, (parity + 1) * half_x)
            even, odd = band_even[g, part, :], band_odd[g, part, :]
            real, imag = spectrum[0][parity], spectrum[1][parity]
            moved = jnp.concatenate([real * even - imag * odd, real * odd + imag * even], 1)
            sides.append(dot3(table, split2(moved)))
        back_out[g] = (sides[0] + turn * sides[1]).reshape(group, rows, 2 * band)
        backward.append(exchange(g, back_out, back_in, back_sent, back_got))
    made = []
    for g in range(REFS):
        for copy in backward[g]:
            copy.wait_recv()
        lines = [
            jnp.concatenate([back_in[g, src, :, p * band : (p + 1) * band] for src in range(group)], 1)
            for p in range(2)
        ]
        field = inverse_y(jnp.concatenate(lines, 0))
        made.append((field[:rows], field[rows:]))
    real, imag = choose(made, vel_last[...])
    cosine, sine = along_last[...], across_last[...]
    moved = real * cosine - imag * sine
    last_image = send_image(1, moved)
    wave_ref[0] = moved
    wave_ref[1] = real * sine + imag * cosine

    leave_route()
    leave_coef()
    mirror.wait_send()
    for copies in forward + backward:
        for copy in copies:
            copy.wait_send()
    for depth_at, copies in enumerate((first_image, last_image)):
        for copy in copies:
            copy.wait()
        total = image_in[depth_at, 0]
        for f in range(1, F):
            total = total + image_in[depth_at, f]
        image_ref[depth_at] = total


def stay(x):
    return pltpu.with_memory_space_constraint(x, pltpu.HBM)


def local(spectra, tile_route, bin_in_tile, trace_offset, weights, frequency, slowness, vel_index):
    F = lax.axis_size("freq")
    L = lax.axis_size("lat")
    devices = F * L
    steps, rows, ny = vel_index.shape
    assert steps == 2
    nx = rows * L
    tiles = (nx // TB) * (ny // TB) // devices
    slots = tiles * CAP
    count = spectra.shape[2]
    data_rows = 2 * spectra.shape[1]
    padded = 2 * data_rows
    group = L // 2
    band = ny // group
    nvel = slowness.shape[1]
    cfg = (F, L, tiles, nx, ny, rows, data_rows, padded, nvel)

    hart = jnp.asarray(half_tables(nx))
    modes_x, modes_y = (jnp.asarray(one) for one in mode_tables(nx))

    f32, bf16, i32 = jnp.float32, jnp.bfloat16, jnp.int32
    dma = pltpu.SemaphoreType.DMA
    wave, image = pl.pallas_call(
        functools.partial(program, cfg),
        out_shape=[
            jax.ShapeDtypeStruct((2, rows, ny), f32),
            jax.ShapeDtypeStruct((2, rows, ny // F), f32),
        ],
        in_specs=[HBM] * 5 + [SMEM] * 2 + [HBM] * 4,
        out_specs=[VMEM, VMEM],
        scratch_shapes=[
            pltpu.VMEM(spectra.shape, f32),
            pltpu.VMEM((1, count), i32),
            pltpu.VMEM((1, count), i32),
            pltpu.VMEM((2, count), f32),
            pltpu.VMEM((1, count), f32),
            pltpu.VMEM(hart.shape, bf16),
            pltpu.VMEM(modes_x.shape, bf16),
            pltpu.VMEM(modes_y.shape, bf16),
            pltpu.VMEM((2, rows, ny), i32),
            pltpu.VMEM((rows, ny), i32),
            pltpu.VMEM((devices, data_rows, 2 * slots), f32),
            pltpu.VMEM((devices, data_rows, 2 * slots), f32),
            pltpu.VMEM((tiles, TERMS, TERMS + data_rows), f32),
            pltpu.VMEM((F, MODES, 2 * tiles * MODES), f32),
            pltpu.VMEM((devices, MODES, 2 * tiles * MODES), f32),
            pltpu.VMEM((REFS, nx, ny), f32),
            pltpu.VMEM((REFS, nx, ny), f32),
            pltpu.VMEM((REFS, nx, band), f32),
            pltpu.VMEM((REFS, nx, band), f32),
            pltpu.VMEM((2, rows, ny), f32),
            pltpu.VMEM((2, rows, ny), f32),
            pltpu.VMEM((rows, ny), f32),
            pltpu.VMEM((rows, ny), f32),
            pltpu.VMEM((2, group, 2, rows, band), f32),
            pltpu.VMEM((2, group, 2, rows, band), f32),
            pltpu.VMEM((REFS, group, rows, 2 * band), f32),
            pltpu.VMEM((REFS, group, rows, 2 * band), f32),
            pltpu.VMEM((2, F, rows, ny // F), f32),
            pltpu.VMEM((2, F, rows, ny // F), f32),
            dma((5,)),
            dma((5,)),
            dma((devices,)),
            dma((devices,)),
            dma((devices,)),
            dma((devices,)),
            dma((2,)),
            dma((2, group)),
            dma((2, group)),
            dma((REFS, group)),
            dma((REFS, group)),
            dma((2, F)),
            dma((2, F)),
        ],
        compiler_params=pltpu.CompilerParams(
            collective_id=0, has_side_effects=True, vmem_limit_bytes=40 << 20
        ),
    )(
        *map(stay, (spectra, tile_route.reshape(1, count), bin_in_tile.reshape(1, count))),
        *map(stay, (trace_offset, weights.reshape(1, count))),
        frequency,
        stay(slowness),
        *map(stay, (vel_index, hart, modes_x, modes_y)),
    )
    return wave[:, None], image


def solution(mesh):
    return jax.shard_map(
        local,
        mesh=mesh,
        in_specs=(
            P(None, None, ("freq", "lat")),
            P(("freq", "lat"), None),
            P(("freq", "lat")),
            P(None, ("freq", "lat")),
            P(("freq", "lat")),
            P("freq"),
            P(),
            P(None, "lat", None),
        ),
        out_specs=(P(None, "freq", "lat", None), P(None, "lat", "freq")),
        check_vma=False,
    )
```

```python
import functools
import math

import jax
import jax.numpy as jnp
import numpy as np
from jax import lax
from jax.experimental import pallas as pl
from jax.experimental.pallas import tpu as pltpu
from jax.sharding import PartitionSpec as P

TB = 32
MODES = 8
CAP = 8
TERMS = MODES * MODES
REFS = 2

damping = 1.0
depth_step = 1.0

NN = (((1,), (0,)), ((), ()))
NT = (((1,), (1,)), ((), ()))
VMEM = pl.BlockSpec(memory_space=pltpu.VMEM)
SMEM = pl.BlockSpec(memory_space=pltpu.SMEM)
HBM = pl.BlockSpec(memory_space=pltpu.HBM)
MESH = pl.DeviceIdType.MESH


def two_parts(exact):
    high = exact.astype(jnp.bfloat16)
    low = (exact - high.astype(np.float64)).astype(jnp.bfloat16)
    return high, low


def hartley(length):
    at = np.arange(length)
    angle = 2.0 * math.pi / length * (at[:, None] * at[None, :] % length)
    return (np.cos(angle) + np.sin(angle)) / math.sqrt(length)


def orders(length):
    at = np.arange(length // 4)
    even = np.concatenate([2 * at, (length - 2 * at) % length])
    even[length // 4] = length // 2
    return even, np.concatenate([2 * at + 1, length - 1 - 2 * at])


def half_tables(length):
    whole = hartley(length)[:, : length // 2]
    even, odd = (whole[order] for order in orders(length))
    return np.stack([np.stack(two_parts(one), 0) for one in (even, even.T, odd, odd.T)], 0)


def mode_tables(length, inner):
    cosines = np.cos(math.pi * np.arange(MODES)[:, None] * (np.arange(TB)[None, :] + 0.5) / TB)
    count = length // TB // 2
    fold = np.zeros((count, MODES, length))
    for tile in range(count):
        fold[tile, :, tile * TB : (tile + 1) * TB] = cosines
    whole = fold @ hartley(length)
    turned = whole.reshape(count, MODES // inner, inner, length).swapaxes(1, 2)
    left, right = [], []
    for order in orders(length):
        high, low = two_parts(whole.reshape(count * MODES, length)[:, order])
        right.append(np.concatenate([high, high, low], 0))
        high, low = two_parts(turned.reshape(count * MODES, length)[:, order])
        left.append(np.concatenate([high.T, low.T, high.T], 1))
    return np.stack(left, 0), np.stack(right, 0)


def split2(x):
    high = x.astype(jnp.bfloat16)
    return high, (x - high.astype(jnp.float32)).astype(jnp.bfloat16)


def dot(a, b, dims=NN):
    return lax.dot_general(a, b, dims, preferred_element_type=jnp.float32)


def dot3(a, b, dims=NN):
    return dot(a[0], b[0], dims) + (dot(a[0], b[1], dims) + dot(a[1], b[0], dims))


def series(value, first, count):
    total = jnp.full(value.shape, 1.0 / math.factorial(2 * (count - 1) + first), jnp.float32)
    for n in range(count - 2, -1, -1):
        total = 1.0 / math.factorial(2 * n + first) - value * total
    return total


def cosine_of(cell):
    angle = (0.5 * TB - (cell + 0.5)) * (math.pi / TB)
    return angle * series(angle * angle, 1, 9)


def propagator(wave_squared, kx, ky):
    vertical = wave_squared - kx * kx - ky * ky
    root = jnp.sqrt(jnp.abs(vertical)) * depth_step
    squared = root * root
    moving = vertical > 0.0
    even = jnp.where(moving, series(squared, 0, 10), jnp.exp(-root))
    odd = jnp.where(moving, root * series(squared, 1, 10), 0.0)
    return even, odd


def wave_number(place, length):
    half, quarter = length // 2, length // 4
    index = 2 * lax.rem(place, quarter) + lax.div(place, half)
    index = jnp.where(place == quarter, half, index)
    return 2.0 * math.pi / length * index.astype(jnp.float32)


def take_lanes(x, index):
    return jnp.take_along_axis(x, index, axis=1, mode="promise_in_bounds")


def iota(shape, axis):
    return lax.broadcasted_iota(jnp.int32, shape, axis)


def program(
    cfg,
    spectra_hbm,
    tile_hbm,
    bin_hbm,
    offset_hbm,
    weight_hbm,
    freq_ref,
    slow_hbm,
    vel_hbm,
    hart_hbm,
    modes_x_hbm,
    modes_y_hbm,
    wave_ref,
    image_ref,
    spectra_ref,
    tile_ref,
    bin_ref,
    offset_ref,
    weight_ref,
    slow_ref,
    hart,
    modes_x,
    modes_y,
    vel_first,
    vel_last,
    route_out,
    route_in,
    coef_out,
    coef_in,
    wide_even,
    wide_odd,
    band_even,
    band_odd,
    along_first,
    across_first,
    along_last,
    across_last,
    fwd_out,
    fwd_in,
    back_out,
    back_in,
    image_out,
    image_in,
    trace_sem,
    table_sem,
    route_sent,
    route_got,
    coef_sent,
    coef_got,
    vel_sem,
    fwd_sent,
    fwd_got,
    back_sent,
    back_got,
    image_sent,
    image_got,
):
    F, L, tiles, nx, ny, rows, data_rows, padded, nvel = cfg
    devices = F * L
    group = L // 2
    half_x, half_y = nx // 2, ny // 2
    band = ny // group
    slots = tiles * CAP
    per_group = nvel // REFS
    me_f = lax.axis_index("freq")
    me_l = lax.axis_index("lat")
    me = me_l * F + me_f
    side = lax.div(me_l, group)
    seat = lax.rem(me_l, group)

    barrier = pltpu.get_barrier_semaphore()

    def partner_of(at):
        other = lax.rem(me + at, devices)
        return other, {"freq": lax.rem(other, F), "lat": lax.div(other, F)}

    def greet(at, carry):
        _, device = partner_of(at)
        pl.semaphore_signal(barrier, inc=1, device_id=device, device_id_type=MESH)
        return carry

    lax.fori_loop(1, devices, greet, 0)
    inputs = [
        pltpu.make_async_copy(src, dst, trace_sem.at[at])
        for at, (src, dst) in enumerate(
            [
                (tile_hbm, tile_ref),
                (bin_hbm, bin_ref),
                (offset_hbm, offset_ref),
                (weight_hbm, weight_ref),
                (spectra_hbm, spectra_ref),
            ]
        )
    ]
    for load in inputs:
        load.start()
    loads = [
        pltpu.make_async_copy(src, dst, table_sem.at[at])
        for at, (src, dst) in enumerate(
            [
                (vel_hbm.at[0], vel_first.at[side]),
                (vel_hbm.at[1], vel_last),
                (modes_x_hbm, modes_x),
                (modes_y_hbm, modes_y),
                (hart_hbm, hart),
                (slow_hbm, slow_ref),
            ]
        )
    ]
    for load in loads:
        load.start()
    for load in inputs:
        load.wait()

    count = tile_ref.shape[1]
    width = 128
    tile = tile_ref[...]
    columns = [
        jnp.transpose(jnp.broadcast_to(tile[:, at : at + width], (width, width)))
        for at in range(0, count, width)
    ]
    earlier = iota((width, width), 0) < iota((width, width), 1)
    ranks = []
    for at in range(count // width):
        row = jnp.broadcast_to(tile[:, at * width : (at + 1) * width], (width, width))
        same = jnp.where((columns[at] == row) & earlier, 1, 0)
        for before in range(at):
            same = same + jnp.where(columns[before] == row, 1, 0)
        ranks.append(jnp.sum(same, 0, keepdims=True))
    rank = jnp.concatenate(ranks, 1)
    turned = lax.rem(lax.rem(tile, tiles) + me, tiles)
    slot = lax.div(tile, tiles) * slots + turned * CAP + rank

    cell = bin_ref[...]
    root_weight = jnp.sqrt(weight_ref[...])
    cell_x = lax.div(cell, TB).astype(jnp.float32) + offset_ref[0:1, :]
    cell_y = lax.rem(cell, TB).astype(jnp.float32) + offset_ref[1:2, :]
    feats = jnp.concatenate(
        [spectra_ref[0] * root_weight, spectra_ref[1] * root_weight]
        + [root_weight, cosine_of(cell_x), cosine_of(cell_y)]
        + [jnp.zeros((padded - data_rows - 3, count), jnp.float32)],
        0,
    )
    high = feats.astype(jnp.bfloat16)
    rest = feats - high.astype(jnp.float32)
    middle = rest.astype(jnp.bfloat16)
    low = (rest - middle.astype(jnp.float32)).astype(jnp.bfloat16)
    parts = jnp.concatenate([high, middle, low], 0)
    wide = 256
    for at in range(0, devices * slots, wide):
        places = iota((wide, count), 0) + at
        chosen = jnp.where(places == slot, 1.0, 0.0).astype(jnp.bfloat16)
        got = dot(parts, chosen, NT)
        got = got[:padded] + got[padded : 2 * padded] + got[2 * padded :]
        for piece in range(wide // slots):
            block = got[:, piece * slots : (piece + 1) * slots]
            route_out[at // slots + piece] = jnp.concatenate([block[:data_rows], block[data_rows:]], 1)

    pl.semaphore_wait(barrier, devices - 1)

    def spread(out, into, sent, landed):
        def copy_of(at):
            other, device = partner_of(at)
            return pltpu.make_async_remote_copy(
                src_ref=out.at[other] if out.shape[0] == devices else out.at[lax.rem(other, F)],
                dst_ref=into.at[me],
                send_sem=sent.at[at],
                recv_sem=landed.at[at],
                device_id=device,
                device_id_type=MESH,
            )

        def start(at, carry):
            copy_of(at).start()
            return carry

        def arrive(at, carry):
            copy_of(at).wait_recv()
            return carry

        def leave(at, carry):
            copy_of(at).wait_send()
            return carry

        lax.fori_loop(1, devices, start, 0)
        return (
            lambda: lax.fori_loop(1, devices, arrive, 0),
            lambda: lax.fori_loop(1, devices, leave, 0),
        )

    arrive, leave_route = spread(route_out, route_in, route_sent, route_got)
    route_in[pl.ds(me, 1)] = route_out[pl.ds(me, 1)]

    for load in loads:
        load.wait()
    frequency = freq_ref[0]
    waves = []
    for depth_at in range(2):
        squares = []
        for g in range(REFS):
            total = slow_ref[depth_at, g * per_group]
            for i in range(1, per_group):
                total = total + slow_ref[depth_at, g * per_group + i]
            reference = total * (1.0 / per_group)
            squares.append((reference, (frequency * reference) * (frequency * reference)))
        waves.append(squares)

    chunk = 16
    quarter_x, quarter_y = nx // 4, ny // 4
    lane = iota((chunk, quarter_y), 1)
    first_ky = [wave_number(lane + parity * half_y, ny) for parity in range(2)]
    middle_ky = jnp.full((chunk, quarter_y), math.pi, jnp.float32)

    def wide_rows(g, kx):
        made = [propagator(waves[0][g][1], kx, ky) for ky in (*first_ky, middle_ky)]
        return [
            jnp.concatenate([even, jnp.where(lane == 0, middle, even), odd, odd], 1)
            for even, odd, middle in zip(*made)
        ]

    def wide_tables(at, carry):
        first = pl.multiple_of(lax.rem(at, quarter_x // chunk) * chunk, chunk)
        base = pl.multiple_of(lax.div(at, quarter_x // chunk) * half_x, half_x)
        kx = wave_number(iota((chunk, quarter_y), 0) + (first + base), nx)
        for g in range(REFS):
            for one, table in zip(wide_rows(g, kx), (wide_even, wide_odd)):
                for copy in range(2):
                    table[g, pl.ds(base + copy * quarter_x + first, chunk), :] = one
        return carry

    lax.fori_loop(0, half_x // chunk, wide_tables, 0)
    middle_kx = jnp.full((chunk, quarter_y), math.pi, jnp.float32)
    for g in range(REFS):
        for one, table in zip(wide_rows(g, middle_kx), (wide_even, wide_odd)):
            table[g, quarter_x : quarter_x + 1, :] = one[:1]
    arrive()

    mirror = pltpu.make_async_remote_copy(
        src_ref=vel_first.at[side],
        dst_ref=vel_first.at[side],
        send_sem=vel_sem.at[0],
        recv_sem=vel_sem.at[1],
        device_id={"lat": lax.rem(me_l + group, L)},
        device_id_type=MESH,
    )
    mirror.start()

    group_at = lax.div(lax.rem(iota((data_rows, 2 * slots), 1), slots), CAP)
    eye = jnp.where(iota((TERMS + data_rows, TERMS), 0) == iota((TERMS + data_rows, TERMS), 1), damping, 0.0)

    def chebyshev(cosine):
        terms = [jnp.ones_like(cosine), cosine]
        for _ in range(MODES - 2):
            terms.append(2.0 * cosine * terms[-1] - terms[-2])
        return terms

    normals = []
    for t in range(tiles):
        pieces = []
        for first in range(0, devices, tiles):
            picked = route_in[first]
            for i in range(1, tiles):
                picked = jnp.where(group_at == (t + i) % tiles, route_in[first + i], picked)
            pieces.append(picked)
        data = jnp.concatenate([piece[:, :slots] for piece in pieces], 1)
        place = jnp.concatenate([piece[:8, slots:] for piece in pieces], 1)
        scale = place[0:1]
        along_x = chebyshev(place[1:2])
        along_y = jnp.concatenate(chebyshev(place[2:3]), 0)
        basis = jnp.concatenate([(term * scale) * along_y for term in along_x], 0)
        right = jnp.concatenate([basis, data], 0)
        normals.append(
            eye
            + lax.dot_general(
                right, basis, NT, preferred_element_type=jnp.float32, precision=lax.Precision.HIGHEST
            )
        )
    inner = 128 // tiles
    outer = TERMS // inner
    lines = (TERMS + data_rows) // 8
    rest = []
    for at in range(outer):
        line = jnp.concatenate([one[:, at * inner : (at + 1) * inner] for one in normals], 1)
        rest.append([line[8 * j : 8 * (j + 1)] for j in range(lines)])
    lane = iota((8, 128), 1)
    within = lax.rem(lane, inner)
    for block in range(TERMS // 8):
        todo = range(block, lines)
        pivots = []
        for s in range(8):
            at, own = (8 * block + s) // inner, (8 * block + s) % inner
            pick = lane - within + own
            pivots.append({j: take_lanes(rest[at][j], pick) for j in todo})
        for s in range(8):
            at, own = (8 * block + s) // inner, (8 * block + s) % inner
            scale = 1.0 / pivots[s][block][s : s + 1]
            scaled = {j: pivots[s][j] * scale for j in todo}
            for later in range(s + 1, 8):
                factor = pivots[later][block][s : s + 1]
                pivots[later] = {j: pivots[later][j] - factor * scaled[j] for j in todo}
            for one in range(outer):
                factor = rest[one][block][s : s + 1]
                for j in todo:
                    value = rest[one][j] - factor * scaled[j]
                    rest[one][j] = jnp.where(within == own, scaled[j], value) if one == at else value
    width = tiles * MODES
    place = lax.rem(lane, width)
    pick = lax.div(place, MODES) * inner + lax.div(lane, width) * MODES + lax.rem(place, MODES)
    for one in range(outer):
        for j in range(TERMS // 8, lines):
            line = take_lanes(rest[one][j], pick)
            for s in range(8):
                part, f = divmod(8 * (j - TERMS // 8) + s, F)
                coef_out[f, part * outer + one : part * outer + one + 1, :] = line[s : s + 1]

    arrive, leave_coef = spread(coef_out, coef_in, coef_sent, coef_got)
    coef_in[pl.ds(me, 1)] = coef_out[pl.ds(me_f, 1)]

    band_ky = wave_number(seat * band + iota((chunk, band), 1), ny)

    def band_tables(at, carry):
        first = pl.multiple_of(lax.rem(at, quarter_x // chunk) * chunk, chunk)
        base = pl.multiple_of(lax.div(at, quarter_x // chunk) * half_x, half_x)
        kx = wave_number(iota((chunk, band), 0) + (first + base), nx)
        for g in range(REFS):
            for one, table in zip(propagator(waves[1][g][1], kx, band_ky), (band_even, band_odd)):
                for copy in range(2):
                    table[g, pl.ds(base + copy * quarter_x + first, chunk), :] = one
        return carry

    lax.fori_loop(0, half_x // chunk, band_tables, 0)
    for g in range(REFS):
        middle = propagator(waves[1][g][1], jnp.full((chunk, band), math.pi, jnp.float32), band_ky)
        for one, table in zip(middle, (band_even, band_odd)):
            table[g, quarter_x : quarter_x + 1, :] = one[:1]

    def split_step(depth_at, velocity):
        cosine = jnp.zeros(velocity.shape, jnp.float32)
        sine = jnp.zeros(velocity.shape, jnp.float32)
        for i in range(nvel):
            shift = slow_ref[depth_at, i] - waves[depth_at][i // per_group][0]
            angle = jnp.full((8, 128), frequency * shift * depth_step, jnp.float32)
            squared = angle * angle
            cosine_i = series(squared, 0, 9)[0:1, 0:1]
            sine_i = (angle * series(squared, 1, 9))[0:1, 0:1]
            cosine = jnp.where(velocity == i, cosine_i, cosine)
            sine = jnp.where(velocity == i, sine_i, sine)
        return cosine, sine

    along_last[...], across_last[...] = split_step(1, vel_last[...])
    mirror.wait_recv()
    for one in range(2):
        along_first[one], across_first[one] = split_step(0, vel_first[one])
    arrive()

    def part_of(which):
        return hart[which, 0], hart[which, 1]

    even_k, even_k_t, odd_k, odd_k_t = (part_of(which) for which in range(4))

    def from_modes_of(parts):
        return jnp.concatenate([parts[0], parts[1], parts[0]], 1)

    per_row = (ny // TB) // tiles
    tile_rows = nx // TB
    mode_rows = tile_rows // 2 * MODES
    mode_columns = ny // TB // 2 * MODES
    sums, differences = [], []
    for part in range(2):
        lines = [
            jnp.concatenate(
                [
                    jnp.concatenate(
                        [
                            coef_in[
                                tile_row * per_row + j,
                                part * outer : (part + 1) * outer,
                                a * width : (a + 1) * width,
                            ]
                            for a in range(MODES // outer)
                        ],
                        0,
                    )
                    for j in range(per_row)
                ],
                1,
            )
            for tile_row in range(tile_rows)
        ]
        upper = jnp.concatenate(lines[: tile_rows // 2], 0)
        lower = jnp.concatenate(lines[tile_rows // 2 :], 0)
        for one in (upper + lower, upper - lower):
            left, right = one[:, :mode_columns], one[:, mode_columns:]
            sums.append(left + right)
            differences.append(left - right)
    spread_y = [
        dot(from_modes_of(split2(jnp.concatenate(one, 0))), modes_y[parity])
        for parity, one in enumerate((sums, differences))
    ]
    seat_rows = pl.ds(pl.multiple_of(seat * rows, rows), rows)
    made = [[None, None] for _ in range(REFS)]
    for parity in range(2):
        picked = [
            one[(2 * p + parity) * mode_rows : (2 * p + parity + 1) * mode_rows]
            for p in range(2)
            for one in spread_y
        ]
        high, low = split2(jnp.concatenate(picked, 1))
        spectrum = dot(modes_x[parity], jnp.concatenate([high, high, low], 0))
        real, imag = spectrum[:, :ny], spectrum[:, ny:]
        which = 2 * parity + 1
        own_high, own_low = hart[which, 0, seat_rows, :], hart[which, 1, seat_rows, :]
        both = jnp.concatenate([own_high, own_low], 0)
        part = slice(parity * half_x, (parity + 1) * half_x)
        for g in range(REFS):
            even, odd = wide_even[g, part, :], wide_odd[g, part, :]
            moved = split2(jnp.concatenate([real * even - imag * odd, real * odd + imag * even], 1))
            back = dot(both, moved[0])
            made[g][parity] = back[:rows] + (back[rows:] + dot(own_high, moved[1]))
    pieces = []
    for g in range(REFS):
        slabs = (made[g][0] + made[g][1], made[g][0] - made[g][1])
        for p in range(2):
            pieces += [slab[:, p * ny : (p + 1) * ny] for slab in slabs]

    def inverse_y(x):
        u = dot3(split2(x[:, :half_y]), even_k)
        v = dot3(split2(x[:, half_y:]), odd_k)
        return jnp.concatenate([u + v, u - v], 1)

    def choose(made, velocity):
        real, imag = made[0]
        for g in range(1, REFS):
            chosen = velocity >= g * per_group
            real = jnp.where(chosen, made[g][0], real)
            imag = jnp.where(chosen, made[g][1], imag)
        return real, imag

    image_piece = ny // F

    def send_image(depth_at, real):
        for f in range(F):
            image_out[depth_at, f] = real[:, f * image_piece : (f + 1) * image_piece]
        copies = []
        for step in range(1, F):
            other = lax.rem(me_f + step, F)
            copies.append(
                pltpu.make_async_remote_copy(
                    src_ref=image_out.at[depth_at, other],
                    dst_ref=image_in.at[depth_at, me_f],
                    send_sem=image_sent.at[depth_at, step],
                    recv_sem=image_got.at[depth_at, step],
                    device_id={"freq": other},
                    device_id_type=MESH,
                )
            )
        for copy in copies:
            copy.start()
        image_in[depth_at, pl.ds(me_f, 1)] = image_out[depth_at, pl.ds(me_f, 1)]
        return copies

    def exchange(at, out, into, sent, landed):
        copies = []
        for step in range(1, group):
            other = lax.rem(seat + step, group)
            copies.append(
                pltpu.make_async_remote_copy(
                    src_ref=out.at[at, other],
                    dst_ref=into.at[at, seat],
                    send_sem=sent.at[at, step],
                    recv_sem=landed.at[at, step],
                    device_id={"lat": side * group + other},
                    device_id_type=MESH,
                )
            )
        for copy in copies:
            copy.start()
        into[at, pl.ds(seat, 1)] = out[at, pl.ds(seat, 1)]
        return copies

    field = inverse_y(jnp.concatenate(pieces, 0))
    two = 2 * rows
    real, imag = choose(
        [(field[2 * g * two : (2 * g + 1) * two], field[(2 * g + 1) * two : (2 * g + 2) * two]) for g in range(REFS)],
        vel_first[...].reshape(two, ny),
    )
    cosine, sine = along_first[...].reshape(two, ny), across_first[...].reshape(two, ny)
    real, imag = real * cosine - imag * sine, real * sine + imag * cosine
    forward = []
    for p, one in enumerate((real, imag)):
        left, right = one[:, :half_y], one[:, half_y:]
        line = jnp.concatenate(
            [dot3(split2(left + right), even_k_t), dot3(split2(left - right), odd_k_t)], 1
        )
        for dst in range(group):
            fwd_out[p, dst] = line[:, dst * band : (dst + 1) * band].reshape(2, rows, band)
        forward.append(exchange(p, fwd_out, fwd_in, fwd_sent, fwd_got))
    first_image = send_image(0, jnp.where(side == 0, real[:rows], real[rows:]))

    spectrum = []
    for p in range(2):
        for copy in forward[p]:
            copy.wait_recv()
        upper = jnp.concatenate([fwd_in[p, src, 0] for src in range(group)], 0)
        lower = jnp.concatenate([fwd_in[p, src, 1] for src in range(group)], 0)
        lines = []
        for one, table in ((upper + lower, even_k), (upper - lower, odd_k)):
            high, low = split2(one)
            line = dot(table[0], jnp.concatenate([high, low], 1))
            lines.append(line[:, :band] + (line[:, band:] + dot(table[1], high)))
        spectrum.append(lines)
    turn = (1 - 2 * side).astype(jnp.float32)
    backward = []
    for g in range(REFS):
        sides = []
        for parity, table in enumerate((even_k_t, odd_k_t)):
            part = slice(parity * half_x, (parity + 1) * half_x)
            even, odd = band_even[g, part, :], band_odd[g, part, :]
            real, imag = spectrum[0][parity], spectrum[1][parity]
            moved = jnp.concatenate([real * even - imag * odd, real * odd + imag * even], 1)
            sides.append(dot3(table, split2(moved)))
        back_out[g] = (sides[0] + turn * sides[1]).reshape(group, rows, 2 * band)
        backward.append(exchange(g, back_out, back_in, back_sent, back_got))
    made = []
    for g in range(REFS):
        for copy in backward[g]:
            copy.wait_recv()
        lines = [
            jnp.concatenate([back_in[g, src, :, p * band : (p + 1) * band] for src in range(group)], 1)
            for p in range(2)
        ]
        field = inverse_y(jnp.concatenate(lines, 0))
        made.append((field[:rows], field[rows:]))
    real, imag = choose(made, vel_last[...])
    cosine, sine = along_last[...], across_last[...]
    moved = real * cosine - imag * sine
    last_image = send_image(1, moved)
    wave_ref[0] = moved
    wave_ref[1] = real * sine + imag * cosine

    leave_route()
    leave_coef()
    mirror.wait_send()
    for copies in forward + backward:
        for copy in copies:
            copy.wait_send()
    for depth_at, copies in enumerate((first_image, last_image)):
        for copy in copies:
            copy.wait()
        total = image_in[depth_at, 0]
        for f in range(1, F):
            total = total + image_in[depth_at, f]
        image_ref[depth_at] = total


def stay(x):
    return pltpu.with_memory_space_constraint(x, pltpu.HBM)


def local(spectra, tile_route, bin_in_tile, trace_offset, weights, frequency, slowness, vel_index):
    F = lax.axis_size("freq")
    L = lax.axis_size("lat")
    devices = F * L
    steps, rows, ny = vel_index.shape
    assert steps == 2
    nx = rows * L
    tiles = (nx // TB) * (ny // TB) // devices
    slots = tiles * CAP
    count = spectra.shape[2]
    data_rows = 2 * spectra.shape[1]
    padded = 2 * data_rows
    group = L // 2
    band = ny // group
    nvel = slowness.shape[1]
    cfg = (F, L, tiles, nx, ny, rows, data_rows, padded, nvel)

    hart = jnp.asarray(half_tables(nx))
    outer = TERMS * tiles // 128
    modes_x, modes_y = (jnp.asarray(one) for one in mode_tables(nx, MODES // outer))

    f32, bf16, i32 = jnp.float32, jnp.bfloat16, jnp.int32
    dma = pltpu.SemaphoreType.DMA
    wave, image = pl.pallas_call(
        functools.partial(program, cfg),
        out_shape=[
            jax.ShapeDtypeStruct((2, rows, ny), f32),
            jax.ShapeDtypeStruct((2, rows, ny // F), f32),
        ],
        in_specs=[HBM] * 5 + [SMEM] + [HBM] * 5,
        out_specs=[VMEM, VMEM],
        scratch_shapes=[
            pltpu.VMEM(spectra.shape, f32),
            pltpu.VMEM((1, count), i32),
            pltpu.VMEM((1, count), i32),
            pltpu.VMEM((2, count), f32),
            pltpu.VMEM((1, count), f32),
            pltpu.SMEM(slowness.shape, f32),
            pltpu.VMEM(hart.shape, bf16),
            pltpu.VMEM(modes_x.shape, bf16),
            pltpu.VMEM(modes_y.shape, bf16),
            pltpu.VMEM((2, rows, ny), i32),
            pltpu.VMEM((rows, ny), i32),
            pltpu.VMEM((devices, data_rows, 2 * slots), f32),
            pltpu.VMEM((devices, data_rows, 2 * slots), f32),
            pltpu.VMEM((F, 2 * outer, 128), f32),
            pltpu.VMEM((devices, 2 * outer, 128), f32),
            pltpu.VMEM((REFS, nx, ny), f32),
            pltpu.VMEM((REFS, nx, ny), f32),
            pltpu.VMEM((REFS, nx, band), f32),
            pltpu.VMEM((REFS, nx, band), f32),
            pltpu.VMEM((2, rows, ny), f32),
            pltpu.VMEM((2, rows, ny), f32),
            pltpu.VMEM((rows, ny), f32),
            pltpu.VMEM((rows, ny), f32),
            pltpu.VMEM((2, group, 2, rows, band), f32),
            pltpu.VMEM((2, group, 2, rows, band), f32),
            pltpu.VMEM((REFS, group, rows, 2 * band), f32),
            pltpu.VMEM((REFS, group, rows, 2 * band), f32),
            pltpu.VMEM((2, F, rows, ny // F), f32),
            pltpu.VMEM((2, F, rows, ny // F), f32),
            dma((5,)),
            dma((6,)),
            dma((devices,)),
            dma((devices,)),
            dma((devices,)),
            dma((devices,)),
            dma((2,)),
            dma((2, group)),
            dma((2, group)),
            dma((REFS, group)),
            dma((REFS, group)),
            dma((2, F)),
            dma((2, F)),
        ],
        compiler_params=pltpu.CompilerParams(
            collective_id=0, has_side_effects=True, vmem_limit_bytes=40 << 20
        ),
    )(
        *map(stay, (spectra, tile_route.reshape(1, count), bin_in_tile.reshape(1, count))),
        *map(stay, (trace_offset, weights.reshape(1, count))),
        frequency,
        stay(slowness),
        *map(stay, (vel_index, hart, modes_x, modes_y)),
    )
    return wave[:, None], image


def solution(mesh):
    return jax.shard_map(
        local,
        mesh=mesh,
        in_specs=(
            P(None, None, ("freq", "lat")),
            P(("freq", "lat"), None),
            P(("freq", "lat")),
            P(None, ("freq", "lat")),
            P(("freq", "lat")),
            P("freq"),
            P(),
            P(None, "lat", None),
        ),
        out_specs=(P(None, "freq", "lat", None), P(None, "lat", "freq")),
        check_vma=False,
    )
```

```python
import functools
import math

import jax
import jax.numpy as jnp
import numpy as np
from jax import lax
from jax.experimental import pallas as pl
from jax.experimental.pallas import tpu as pltpu
from jax.sharding import PartitionSpec as P

TB = 32
MODES = 8
CAP = 8
TERMS = MODES * MODES
REFS = 2

damping = 1.0
depth_step = 1.0

NN = (((1,), (0,)), ((), ()))
NT = (((1,), (1,)), ((), ()))
VMEM = pl.BlockSpec(memory_space=pltpu.VMEM)
SMEM = pl.BlockSpec(memory_space=pltpu.SMEM)
HBM = pl.BlockSpec(memory_space=pltpu.HBM)
MESH = pl.DeviceIdType.MESH


def two_parts(exact):
    high = exact.astype(jnp.bfloat16)
    low = (exact - high.astype(np.float64)).astype(jnp.bfloat16)
    return high, low


def hartley(length):
    at = np.arange(length)
    angle = 2.0 * math.pi / length * (at[:, None] * at[None, :] % length)
    return (np.cos(angle) + np.sin(angle)) / math.sqrt(length)


def orders(length):
    at = np.arange(length // 4)
    even = np.concatenate([2 * at, (length - 2 * at) % length])
    even[length // 4] = length // 2
    return even, np.concatenate([2 * at + 1, length - 1 - 2 * at])


def half_tables(length):
    whole = hartley(length)[:, : length // 2]
    even, odd = (whole[order] for order in orders(length))
    return np.stack([np.stack(two_parts(one), 0) for one in (even, even.T, odd, odd.T)], 0)


def mode_tables(length, inner):
    cosines = np.cos(math.pi * np.arange(MODES)[:, None] * (np.arange(TB)[None, :] + 0.5) / TB)
    count = length // TB // 2
    fold = np.zeros((count, MODES, length))
    for tile in range(count):
        fold[tile, :, tile * TB : (tile + 1) * TB] = cosines
    whole = fold @ hartley(length)
    turned = whole.reshape(count, MODES // inner, inner, length).swapaxes(1, 2)
    left, right = [], []
    for order in orders(length):
        high, low = two_parts(whole.reshape(count * MODES, length)[:, order])
        right.append(np.concatenate([high, high, low], 0))
        high, low = two_parts(turned.reshape(count * MODES, length)[:, order])
        left.append(np.concatenate([high.T, low.T, high.T], 1))
    return np.stack(left, 0), np.stack(right, 0)


def split2(x):
    high = x.astype(jnp.bfloat16)
    return high, (x - high.astype(jnp.float32)).astype(jnp.bfloat16)


def dot(a, b, dims=NN):
    return lax.dot_general(a, b, dims, preferred_element_type=jnp.float32)


def dot3(a, b, dims=NN):
    return dot(a[0], b[0], dims) + (dot(a[0], b[1], dims) + dot(a[1], b[0], dims))


def series(value, first, count):
    total = jnp.full(value.shape, 1.0 / math.factorial(2 * (count - 1) + first), jnp.float32)
    for n in range(count - 2, -1, -1):
        total = 1.0 / math.factorial(2 * n + first) - value * total
    return total


def cosine_of(cell):
    angle = (0.5 * TB - (cell + 0.5)) * (math.pi / TB)
    return angle * series(angle * angle, 1, 9)


def propagator(wave_squared, kx, ky):
    vertical = wave_squared - kx * kx - ky * ky
    root = jnp.sqrt(jnp.abs(vertical)) * depth_step
    squared = root * root
    moving = vertical > 0.0
    even = jnp.where(moving, series(squared, 0, 10), jnp.exp(-root))
    odd = jnp.where(moving, root * series(squared, 1, 10), 0.0)
    return even, odd


def wave_number(place, length):
    half, quarter = length // 2, length // 4
    index = 2 * lax.rem(place, quarter) + lax.div(place, half)
    index = jnp.where(place == quarter, half, index)
    return 2.0 * math.pi / length * index.astype(jnp.float32)


def take_lanes(x, index):
    return jnp.take_along_axis(x, index, axis=1, mode="promise_in_bounds")


def iota(shape, axis):
    return lax.broadcasted_iota(jnp.int32, shape, axis)


def program(
    cfg,
    spectra_hbm,
    tile_hbm,
    bin_hbm,
    offset_hbm,
    weight_hbm,
    freq_ref,
    slow_hbm,
    vel_hbm,
    hart_hbm,
    modes_x_hbm,
    modes_y_hbm,
    wave_ref,
    image_in,
    spectra_ref,
    tile_ref,
    bin_ref,
    offset_ref,
    weight_ref,
    slow_ref,
    hart,
    modes_x,
    modes_y,
    vel_first,
    vel_last,
    route_out,
    route_in,
    coef_out,
    coef_in,
    wide_even,
    wide_odd,
    band_even,
    band_odd,
    along_first,
    across_first,
    along_last,
    across_last,
    slabs,
    first_real,
    fwd_out,
    fwd_in,
    back_out,
    back_in,
    image_out,
    trace_sem,
    table_sem,
    route_sent,
    route_got,
    coef_sent,
    coef_got,
    vel_sem,
    fwd_sent,
    fwd_got,
    back_sent,
    back_got,
    image_sent,
    image_got,
):
    F, L, tiles, nx, ny, rows, data_rows, padded, nvel = cfg
    devices = F * L
    group = L // 2
    half_x, half_y = nx // 2, ny // 2
    band = ny // group
    slots = tiles * CAP
    per_group = nvel // REFS
    me_f = lax.axis_index("freq")
    me_l = lax.axis_index("lat")
    me = me_l * F + me_f
    side = lax.div(me_l, group)
    seat = lax.rem(me_l, group)

    barrier = pltpu.get_barrier_semaphore()

    def partner_of(at):
        other = lax.rem(me + at, devices)
        return other, {"freq": lax.rem(other, F), "lat": lax.div(other, F)}

    def greet(at, carry):
        _, device = partner_of(at)
        pl.semaphore_signal(barrier, inc=1, device_id=device, device_id_type=MESH)
        return carry

    inputs = [
        pltpu.make_async_copy(src, dst, trace_sem.at[at])
        for at, (src, dst) in enumerate(
            [
                (tile_hbm, tile_ref),
                (bin_hbm, bin_ref),
                (offset_hbm, offset_ref),
                (weight_hbm, weight_ref),
                (spectra_hbm, spectra_ref),
            ]
        )
    ]
    for load in inputs:
        load.start()
    lax.fori_loop(1, devices, greet, 0)
    loads = [
        pltpu.make_async_copy(src, dst, table_sem.at[at])
        for at, (src, dst) in enumerate(
            [
                (vel_hbm.at[0], vel_first.at[side]),
                (vel_hbm.at[1], vel_last),
                (modes_x_hbm, modes_x),
                (modes_y_hbm, modes_y),
                (hart_hbm, hart),
                (slow_hbm, slow_ref),
            ]
        )
    ]
    for load in loads:
        load.start()
    for load in inputs:
        load.wait()

    count = tile_ref.shape[1]
    width = 128
    tile = tile_ref[...]
    columns = [
        jnp.transpose(jnp.broadcast_to(tile[:, at : at + width], (width, width)))
        for at in range(0, count, width)
    ]
    earlier = iota((width, width), 0) < iota((width, width), 1)
    ranks = []
    for at in range(count // width):
        row = jnp.broadcast_to(tile[:, at * width : (at + 1) * width], (width, width))
        same = jnp.where((columns[at] == row) & earlier, 1, 0)
        for before in range(at):
            same = same + jnp.where(columns[before] == row, 1, 0)
        ranks.append(jnp.sum(same, 0, keepdims=True))
    rank = jnp.concatenate(ranks, 1)
    turned = lax.rem(lax.rem(tile, tiles) + me, tiles)
    slot = lax.div(tile, tiles) * slots + turned * CAP + rank

    cell = bin_ref[...]
    root_weight = jnp.sqrt(weight_ref[...])
    cell_x = lax.div(cell, TB).astype(jnp.float32) + offset_ref[0:1, :]
    cell_y = lax.rem(cell, TB).astype(jnp.float32) + offset_ref[1:2, :]
    feats = jnp.concatenate(
        [spectra_ref[0] * root_weight, spectra_ref[1] * root_weight]
        + [root_weight, cosine_of(cell_x), cosine_of(cell_y)]
        + [jnp.zeros((padded - data_rows - 3, count), jnp.float32)],
        0,
    )
    high = feats.astype(jnp.bfloat16)
    rest = feats - high.astype(jnp.float32)
    middle = rest.astype(jnp.bfloat16)
    low = (rest - middle.astype(jnp.float32)).astype(jnp.bfloat16)
    parts = jnp.concatenate([high, middle, low], 0)
    wide = 256
    for at in range(0, devices * slots, wide):
        places = iota((wide, count), 0) + at
        chosen = jnp.where(places == slot, 1.0, 0.0).astype(jnp.bfloat16)
        got = dot(parts, chosen, NT)
        got = got[:padded] + got[padded : 2 * padded] + got[2 * padded :]
        for piece in range(wide // slots):
            block = got[:, piece * slots : (piece + 1) * slots]
            route_out[at // slots + piece] = jnp.concatenate([block[:data_rows], block[data_rows:]], 1)

    pl.semaphore_wait(barrier, devices - 1)

    def spread(out, into, sent, landed):
        def copy_of(at):
            other, device = partner_of(at)
            return pltpu.make_async_remote_copy(
                src_ref=out.at[other] if out.shape[0] == devices else out.at[lax.rem(other, F)],
                dst_ref=into.at[me],
                send_sem=sent.at[at],
                recv_sem=landed.at[at],
                device_id=device,
                device_id_type=MESH,
            )

        def start(at, carry):
            copy_of(at).start()
            return carry

        def arrive(at, carry):
            copy_of(at).wait_recv()
            return carry

        def leave(at, carry):
            copy_of(at).wait_send()
            return carry

        lax.fori_loop(1, devices, start, 0)
        return (
            lambda: lax.fori_loop(1, devices, arrive, 0),
            lambda: lax.fori_loop(1, devices, leave, 0),
        )

    arrive, leave_route = spread(route_out, route_in, route_sent, route_got)
    route_in[pl.ds(me, 1)] = route_out[pl.ds(me, 1)]

    parts = F if rows % (8 * F) == 0 else 1
    part_rows = rows // parts
    own_part = pl.ds(pl.multiple_of((me_f if parts > 1 else 0) * part_rows, part_rows), part_rows)
    loads[0].wait()
    mirror = pltpu.make_async_remote_copy(
        src_ref=vel_first.at[side, own_part],
        dst_ref=vel_first.at[side, own_part],
        send_sem=vel_sem.at[0],
        recv_sem=vel_sem.at[1],
        device_id={"lat": lax.rem(me_l + group, L)},
        device_id_type=MESH,
    )
    mirror.start()

    for load in loads[1:]:
        load.wait()
    frequency = freq_ref[0]
    waves = []
    for depth_at in range(2):
        squares = []
        for g in range(REFS):
            total = slow_ref[depth_at, g * per_group]
            for i in range(1, per_group):
                total = total + slow_ref[depth_at, g * per_group + i]
            reference = total * (1.0 / per_group)
            squares.append((reference, (frequency * reference) * (frequency * reference)))
        waves.append(squares)

    chunk = 16
    quarter_x, quarter_y = nx // 4, ny // 4
    lane = iota((chunk, quarter_y), 1)
    first_ky = [wave_number(lane + parity * half_y, ny) for parity in range(2)]
    middle_ky = jnp.full((chunk, quarter_y), math.pi, jnp.float32)

    def wide_rows(g, kx):
        made = [propagator(waves[0][g][1], kx, ky) for ky in (*first_ky, middle_ky)]
        return [
            jnp.concatenate([even, jnp.where(lane == 0, middle, even), odd, odd], 1)
            for even, odd, middle in zip(*made)
        ]

    def wide_tables(at, carry):
        first = pl.multiple_of(lax.rem(at, quarter_x // chunk) * chunk, chunk)
        base = pl.multiple_of(lax.div(at, quarter_x // chunk) * half_x, half_x)
        kx = wave_number(iota((chunk, quarter_y), 0) + (first + base), nx)
        for g in range(REFS):
            for one, table in zip(wide_rows(g, kx), (wide_even, wide_odd)):
                for copy in range(2):
                    table[g, pl.ds(base + copy * quarter_x + first, chunk), :] = one
        return carry

    lax.fori_loop(0, half_x // chunk, wide_tables, 0)
    middle_kx = jnp.full((chunk, quarter_y), math.pi, jnp.float32)
    for g in range(REFS):
        for one, table in zip(wide_rows(g, middle_kx), (wide_even, wide_odd)):
            table[g, quarter_x : quarter_x + 1, :] = one[:1]
    arrive()

    mirror.wait_recv()
    handed = []
    for step in range(1, parts):
        other = lax.rem(me_f + step, F)
        handed.append(
            pltpu.make_async_remote_copy(
                src_ref=vel_first.at[1 - side, own_part],
                dst_ref=vel_first.at[1 - side, own_part],
                send_sem=vel_sem.at[2 * step],
                recv_sem=vel_sem.at[2 * step + 1],
                device_id={"freq": other},
                device_id_type=MESH,
            )
        )
    for copy in handed:
        copy.start()

    group_at = lax.div(lax.rem(iota((data_rows, 2 * slots), 1), slots), CAP)
    eye = jnp.where(iota((TERMS + data_rows, TERMS), 0) == iota((TERMS + data_rows, TERMS), 1), damping, 0.0)

    def chebyshev(cosine):
        terms = [jnp.ones_like(cosine), cosine]
        for _ in range(MODES - 2):
            terms.append(2.0 * cosine * terms[-1] - terms[-2])
        return terms

    normals = []
    for t in range(tiles):
        pieces = []
        for first in range(0, devices, tiles):
            picked = route_in[first]
            for i in range(1, tiles):
                picked = jnp.where(group_at == (t + i) % tiles, route_in[first + i], picked)
            pieces.append(picked)
        data = jnp.concatenate([piece[:, :slots] for piece in pieces], 1)
        place = jnp.concatenate([piece[:8, slots:] for piece in pieces], 1)
        scale = place[0:1]
        along_x = chebyshev(place[1:2])
        along_y = jnp.concatenate(chebyshev(place[2:3]), 0)
        basis = jnp.concatenate([(term * scale) * along_y for term in along_x], 0)
        right = jnp.concatenate([basis, data], 0)
        normals.append(
            eye
            + lax.dot_general(
                right, basis, NT, preferred_element_type=jnp.float32, precision=lax.Precision.HIGHEST
            )
        )
    inner = 128 // tiles
    outer = TERMS // inner
    lines = (TERMS + data_rows) // 8
    rest = []
    for at in range(outer):
        line = jnp.concatenate([one[:, at * inner : (at + 1) * inner] for one in normals], 1)
        rest.append([line[8 * j : 8 * (j + 1)] for j in range(lines)])
    lane = iota((8, 128), 1)
    within = lax.rem(lane, inner)
    for block in range(TERMS // 8):
        todo = range(block, lines)
        pivots = []
        for s in range(8):
            at, own = (8 * block + s) // inner, (8 * block + s) % inner
            pick = lane - within + own
            pivots.append({j: take_lanes(rest[at][j], pick) for j in todo})
        for s in range(8):
            at, own = (8 * block + s) // inner, (8 * block + s) % inner
            scale = 1.0 / pivots[s][block][s : s + 1]
            scaled = {j: pivots[s][j] * scale for j in todo}
            for later in range(s + 1, 8):
                factor = pivots[later][block][s : s + 1]
                pivots[later] = {j: pivots[later][j] - factor * scaled[j] for j in todo}
            for one in range(outer):
                factor = rest[one][block][s : s + 1]
                for j in todo:
                    value = rest[one][j] - factor * scaled[j]
                    rest[one][j] = jnp.where(within == own, scaled[j], value) if one == at else value
    width = tiles * MODES
    place = lax.rem(lane, width)
    pick = lax.div(place, MODES) * inner + lax.div(lane, width) * MODES + lax.rem(place, MODES)
    for one in range(outer):
        for j in range(TERMS // 8, lines):
            line = take_lanes(rest[one][j], pick)
            for s in range(8):
                part, f = divmod(8 * (j - TERMS // 8) + s, F)
                coef_out[f, part * outer + one : part * outer + one + 1, :] = line[s : s + 1]

    arrive, leave_coef = spread(coef_out, coef_in, coef_sent, coef_got)
    coef_in[pl.ds(me, 1)] = coef_out[pl.ds(me_f, 1)]

    band_ky = wave_number(seat * band + iota((chunk, band), 1), ny)

    def band_tables(at, carry):
        first = pl.multiple_of(lax.rem(at, quarter_x // chunk) * chunk, chunk)
        base = pl.multiple_of(lax.div(at, quarter_x // chunk) * half_x, half_x)
        kx = wave_number(iota((chunk, band), 0) + (first + base), nx)
        for g in range(REFS):
            for one, table in zip(propagator(waves[1][g][1], kx, band_ky), (band_even, band_odd)):
                for copy in range(2):
                    table[g, pl.ds(base + copy * quarter_x + first, chunk), :] = one
        return carry

    lax.fori_loop(0, half_x // chunk, band_tables, 0)
    for g in range(REFS):
        middle = propagator(waves[1][g][1], jnp.full((chunk, band), math.pi, jnp.float32), band_ky)
        for one, table in zip(middle, (band_even, band_odd)):
            table[g, quarter_x : quarter_x + 1, :] = one[:1]

    def split_step(depth_at, velocity):
        cosine = jnp.zeros(velocity.shape, jnp.float32)
        sine = jnp.zeros(velocity.shape, jnp.float32)
        for i in range(nvel):
            shift = slow_ref[depth_at, i] - waves[depth_at][i // per_group][0]
            angle = jnp.full((8, 128), frequency * shift * depth_step, jnp.float32)
            squared = angle * angle
            cosine_i = series(squared, 0, 9)[0:1, 0:1]
            sine_i = (angle * series(squared, 1, 9))[0:1, 0:1]
            cosine = jnp.where(velocity == i, cosine_i, cosine)
            sine = jnp.where(velocity == i, sine_i, sine)
        return cosine, sine

    along_last[...], across_last[...] = split_step(1, vel_last[...])
    for copy in handed:
        copy.wait_recv()
    for one in range(2):
        along_first[one], across_first[one] = split_step(0, vel_first[one])
    arrive()

    def part_of(which):
        return hart[which, 0], hart[which, 1]

    even_k, even_k_t, odd_k, odd_k_t = (part_of(which) for which in range(4))

    def from_modes_of(parts):
        return jnp.concatenate([parts[0], parts[1], parts[0]], 1)

    per_row = (ny // TB) // tiles
    tile_rows = nx // TB
    mode_rows = tile_rows // 2 * MODES
    mode_columns = ny // TB // 2 * MODES
    sums, differences = [], []
    for part in range(2):
        lines = [
            jnp.concatenate(
                [
                    jnp.concatenate(
                        [
                            coef_in[
                                tile_row * per_row + j,
                                part * outer : (part + 1) * outer,
                                a * width : (a + 1) * width,
                            ]
                            for a in range(MODES // outer)
                        ],
                        0,
                    )
                    for j in range(per_row)
                ],
                1,
            )
            for tile_row in range(tile_rows)
        ]
        upper = jnp.concatenate(lines[: tile_rows // 2], 0)
        lower = jnp.concatenate(lines[tile_rows // 2 :], 0)
        for one in (upper + lower, upper - lower):
            left, right = one[:, :mode_columns], one[:, mode_columns:]
            sums.append(left + right)
            differences.append(left - right)
    spread_y = [
        dot(from_modes_of(split2(jnp.concatenate(one, 0))), modes_y[parity])
        for parity, one in enumerate((sums, differences))
    ]
    seat_rows = pl.ds(pl.multiple_of(seat * rows, rows), rows)
    made = [[None, None] for _ in range(REFS)]
    for parity in range(2):
        picked = [
            one[(2 * p + parity) * mode_rows : (2 * p + parity + 1) * mode_rows]
            for p in range(2)
            for one in spread_y
        ]
        high, low = split2(jnp.concatenate(picked, 1))
        spectrum = dot(modes_x[parity], jnp.concatenate([high, high, low], 0))
        real, imag = spectrum[:, :ny], spectrum[:, ny:]
        which = 2 * parity + 1
        own_high, own_low = hart[which, 0, seat_rows, :], hart[which, 1, seat_rows, :]
        both = jnp.concatenate([own_high, own_low], 0)
        part = slice(parity * half_x, (parity + 1) * half_x)
        for g in range(REFS):
            even, odd = wide_even[g, part, :], wide_odd[g, part, :]
            moved = split2(jnp.concatenate([real * even - imag * odd, real * odd + imag * even], 1))
            back = dot(both, moved[0])
            made[g][parity] = back[:rows] + (back[rows:] + dot(own_high, moved[1]))
    for g in range(REFS):
        for p in range(2):
            part = slice(p * ny, (p + 1) * ny)
            for at, slab in enumerate((made[g][0] + made[g][1], made[g][0] - made[g][1])):
                slabs[at, 2 * g + p] = slab[:, part]

    def inverse_y(x):
        u = dot3(split2(x[:, :half_y]), even_k)
        v = dot3(split2(x[:, half_y:]), odd_k)
        return jnp.concatenate([u + v, u - v], 1)

    def choose(made, velocity):
        real, imag = made[0]
        for g in range(1, REFS):
            chosen = velocity >= g * per_group
            real = jnp.where(chosen, made[g][0], real)
            imag = jnp.where(chosen, made[g][1], imag)
        return real, imag

    image_piece = ny // F

    def send_image(depth_at, real):
        for f in range(F):
            image_out[depth_at, f] = real[:, f * image_piece : (f + 1) * image_piece]
        copies = []
        for step in range(1, F):
            other = lax.rem(me_f + step, F)
            copies.append(
                pltpu.make_async_remote_copy(
                    src_ref=image_out.at[depth_at, other],
                    dst_ref=image_in.at[depth_at, me_f],
                    send_sem=image_sent.at[depth_at, step],
                    recv_sem=image_got.at[depth_at, step],
                    device_id={"freq": other},
                    device_id_type=MESH,
                )
            )
        for copy in copies:
            copy.start()
        image_in[depth_at, pl.ds(me_f, 1)] = image_out[depth_at, pl.ds(me_f, 1)]
        return copies

    def copies_of(at, out, into, sent, landed):
        copies = []
        for step in range(1, group):
            other = lax.rem(seat + step, group)
            copies.append(
                pltpu.make_async_remote_copy(
                    src_ref=out.at[at, other],
                    dst_ref=into.at[at, seat],
                    send_sem=sent.at[at, step],
                    recv_sem=landed.at[at, step],
                    device_id={"lat": side * group + other},
                    device_id_type=MESH,
                )
            )
        return copies

    def exchange(at, out, into, sent, landed):
        copies = copies_of(at, out, into, sent, landed)
        for copy in copies:
            copy.start()
        into[at, pl.ds(seat, 1)] = out[at, pl.ds(seat, 1)]
        return copies

    def first_rows(at, carry):
        field = inverse_y(slabs[at].reshape(2 * REFS * rows, ny))
        made = [
            (field[2 * g * rows : (2 * g + 1) * rows], field[(2 * g + 1) * rows : (2 * g + 2) * rows])
            for g in range(REFS)
        ]
        real, imag = choose(made, vel_first[at])
        cosine, sine = along_first[at], across_first[at]
        real, imag = real * cosine - imag * sine, real * sine + imag * cosine
        first_real[at] = real
        both = jnp.concatenate([real, imag], 0)
        left, right = both[:, :half_y], both[:, half_y:]
        line = jnp.concatenate(
            [dot3(split2(left + right), even_k_t), dot3(split2(left - right), odd_k_t)], 1
        )
        for dst in range(group):
            fwd_out[at, dst] = line[:, dst * band : (dst + 1) * band].reshape(2, rows, band)
        exchange(at, fwd_out, fwd_in, fwd_sent, fwd_got)
        return carry

    lax.fori_loop(0, 2, first_rows, 0)
    forward = [copies_of(at, fwd_out, fwd_in, fwd_sent, fwd_got) for at in range(2)]
    first_image = send_image(0, first_real[pl.ds(side, 1)].reshape(rows, ny))

    spectrum = []
    for copy in forward[0] + forward[1]:
        copy.wait_recv()
    for p in range(2):
        upper = jnp.concatenate([fwd_in[0, src, p] for src in range(group)], 0)
        lower = jnp.concatenate([fwd_in[1, src, p] for src in range(group)], 0)
        lines = []
        for one, table in ((upper + lower, even_k), (upper - lower, odd_k)):
            high, low = split2(one)
            line = dot(table[0], jnp.concatenate([high, low], 1))
            lines.append(line[:, :band] + (line[:, band:] + dot(table[1], high)))
        spectrum.append(lines)
    turn = (1 - 2 * side).astype(jnp.float32)
    backward = []
    for g in range(REFS):
        sides = []
        for parity, table in enumerate((even_k_t, odd_k_t)):
            part = slice(parity * half_x, (parity + 1) * half_x)
            even, odd = band_even[g, part, :], band_odd[g, part, :]
            real, imag = spectrum[0][parity], spectrum[1][parity]
            moved = jnp.concatenate([real * even - imag * odd, real * odd + imag * even], 1)
            sides.append(dot3(table, split2(moved)))
        back_out[g] = (sides[0] + turn * sides[1]).reshape(group, rows, 2 * band)
        backward.append(exchange(g, back_out, back_in, back_sent, back_got))
    made = []
    for g in range(REFS):
        for copy in backward[g]:
            copy.wait_recv()
        lines = [
            jnp.concatenate([back_in[g, src, :, p * band : (p + 1) * band] for src in range(group)], 1)
            for p in range(2)
        ]
        field = inverse_y(jnp.concatenate(lines, 0))
        made.append((field[:rows], field[rows:]))
    real, imag = choose(made, vel_last[...])
    cosine, sine = along_last[...], across_last[...]
    moved = real * cosine - imag * sine
    last_image = send_image(1, moved)
    wave_ref[0] = moved
    wave_ref[1] = real * sine + imag * cosine

    leave_route()
    leave_coef()
    mirror.wait_send()
    for copy in handed:
        copy.wait_send()
    for copies in forward + backward:
        for copy in copies:
            copy.wait_send()
    for copy in first_image + last_image:
        copy.wait()


def finish(wave_ref, part_ref, wave_hbm, image_hbm, total, sem):
    store = pltpu.make_async_copy(wave_ref, wave_hbm.at[:, 0], sem.at[0])
    store.start()
    image = part_ref[:, 0]
    for f in range(1, part_ref.shape[1]):
        image = image + part_ref[:, f]
    total[...] = image
    last = pltpu.make_async_copy(total, image_hbm, sem.at[1])
    last.start()
    store.wait()
    last.wait()


def stay(x):
    return pltpu.with_memory_space_constraint(x, pltpu.HBM)


def local(spectra, tile_route, bin_in_tile, trace_offset, weights, frequency, slowness, vel_index):
    F = lax.axis_size("freq")
    L = lax.axis_size("lat")
    devices = F * L
    steps, rows, ny = vel_index.shape
    assert steps == 2
    nx = rows * L
    tiles = (nx // TB) * (ny // TB) // devices
    slots = tiles * CAP
    count = spectra.shape[2]
    data_rows = 2 * spectra.shape[1]
    padded = 2 * data_rows
    group = L // 2
    band = ny // group
    nvel = slowness.shape[1]
    cfg = (F, L, tiles, nx, ny, rows, data_rows, padded, nvel)

    hart = jnp.asarray(half_tables(nx))
    outer = TERMS * tiles // 128
    modes_x, modes_y = (jnp.asarray(one) for one in mode_tables(nx, MODES // outer))

    f32, bf16, i32 = jnp.float32, jnp.bfloat16, jnp.int32
    dma = pltpu.SemaphoreType.DMA
    wave, images = pl.pallas_call(
        functools.partial(program, cfg),
        out_shape=[
            jax.ShapeDtypeStruct((2, rows, ny), f32),
            jax.ShapeDtypeStruct((2, F, rows, ny // F), f32),
        ],
        in_specs=[HBM] * 5 + [SMEM] + [HBM] * 5,
        out_specs=[VMEM, VMEM],
        scratch_shapes=[
            pltpu.VMEM(spectra.shape, f32),
            pltpu.VMEM((1, count), i32),
            pltpu.VMEM((1, count), i32),
            pltpu.VMEM((2, count), f32),
            pltpu.VMEM((1, count), f32),
            pltpu.SMEM(slowness.shape, f32),
            pltpu.VMEM(hart.shape, bf16),
            pltpu.VMEM(modes_x.shape, bf16),
            pltpu.VMEM(modes_y.shape, bf16),
            pltpu.VMEM((2, rows, ny), i32),
            pltpu.VMEM((rows, ny), i32),
            pltpu.VMEM((devices, data_rows, 2 * slots), f32),
            pltpu.VMEM((devices, data_rows, 2 * slots), f32),
            pltpu.VMEM((F, 2 * outer, 128), f32),
            pltpu.VMEM((devices, 2 * outer, 128), f32),
            pltpu.VMEM((REFS, nx, ny), f32),
            pltpu.VMEM((REFS, nx, ny), f32),
            pltpu.VMEM((REFS, nx, band), f32),
            pltpu.VMEM((REFS, nx, band), f32),
            pltpu.VMEM((2, rows, ny), f32),
            pltpu.VMEM((2, rows, ny), f32),
            pltpu.VMEM((rows, ny), f32),
            pltpu.VMEM((rows, ny), f32),
            pltpu.VMEM((2, 2 * REFS, rows, ny), f32),
            pltpu.VMEM((2, rows, ny), f32),
            pltpu.VMEM((2, group, 2, rows, band), f32),
            pltpu.VMEM((2, group, 2, rows, band), f32),
            pltpu.VMEM((REFS, group, rows, 2 * band), f32),
            pltpu.VMEM((REFS, group, rows, 2 * band), f32),
            pltpu.VMEM((2, F, rows, ny // F), f32),
            dma((5,)),
            dma((6,)),
            dma((devices,)),
            dma((devices,)),
            dma((devices,)),
            dma((devices,)),
            dma((2 * F,)),
            dma((2, group)),
            dma((2, group)),
            dma((REFS, group)),
            dma((REFS, group)),
            dma((2, F)),
            dma((2, F)),
        ],
        compiler_params=pltpu.CompilerParams(
            collective_id=0, has_side_effects=True, vmem_limit_bytes=40 << 20
        ),
    )(
        *map(stay, (spectra, tile_route.reshape(1, count), bin_in_tile.reshape(1, count))),
        *map(stay, (trace_offset, weights.reshape(1, count))),
        frequency,
        stay(slowness),
        *map(stay, (vel_index, hart, modes_x, modes_y)),
    )
    return pl.pallas_call(
        finish,
        out_shape=[
            jax.ShapeDtypeStruct((2, 1, rows, ny), f32),
            jax.ShapeDtypeStruct((2, rows, ny // F), f32),
        ],
        in_specs=[VMEM, VMEM],
        out_specs=[HBM, HBM],
        scratch_shapes=[pltpu.VMEM((2, rows, ny // F), f32), dma((2,))],
        compiler_params=pltpu.CompilerParams(vmem_limit_bytes=8 << 20),
    )(wave, images)


def solution(mesh):
    return jax.shard_map(
        local,
        mesh=mesh,
        in_specs=(
            P(None, None, ("freq", "lat")),
            P(("freq", "lat"), None),
            P(("freq", "lat")),
            P(None, ("freq", "lat")),
            P(("freq", "lat")),
            P("freq"),
            P(),
            P(None, "lat", None),
        ),
        out_specs=(P(None, "freq", "lat", None), P(None, "lat", "freq")),
        check_vma=False,
    )
```

```python
import functools
import math

import jax
import jax.numpy as jnp
import numpy as np
from jax import lax
from jax.experimental import pallas as pl
from jax.experimental.pallas import tpu as pltpu
from jax.sharding import PartitionSpec as P

TB = 32
MODES = 8
CAP = 8
TERMS = MODES * MODES
REFS = 2

damping = 1.0
depth_step = 1.0

NN = (((1,), (0,)), ((), ()))
NT = (((1,), (1,)), ((), ()))
VMEM = pl.BlockSpec(memory_space=pltpu.VMEM)
SMEM = pl.BlockSpec(memory_space=pltpu.SMEM)
HBM = pl.BlockSpec(memory_space=pltpu.HBM)
MESH = pl.DeviceIdType.MESH


def two_parts(exact):
    high = exact.astype(jnp.bfloat16)
    low = (exact - high.astype(np.float64)).astype(jnp.bfloat16)
    return high, low


def hartley(length):
    at = np.arange(length)
    angle = 2.0 * math.pi / length * (at[:, None] * at[None, :] % length)
    return (np.cos(angle) + np.sin(angle)) / math.sqrt(length)


def orders(length):
    at = np.arange(length // 4)
    even = np.concatenate([2 * at, (length - 2 * at) % length])
    even[length // 4] = length // 2
    return even, np.concatenate([2 * at + 1, length - 1 - 2 * at])


def half_tables(length):
    whole = hartley(length)[:, : length // 2]
    even, odd = (whole[order] for order in orders(length))
    return np.stack([np.stack(two_parts(one), 0) for one in (even, even.T, odd, odd.T)], 0)


def mode_tables(length, inner):
    cosines = np.cos(math.pi * np.arange(MODES)[:, None] * (np.arange(TB)[None, :] + 0.5) / TB)
    count = length // TB // 2
    fold = np.zeros((count, MODES, length))
    for tile in range(count):
        fold[tile, :, tile * TB : (tile + 1) * TB] = cosines
    whole = fold @ hartley(length)
    turned = whole.reshape(count, MODES // inner, inner, length).swapaxes(1, 2)
    left, right = [], []
    for order in orders(length):
        high, low = two_parts(whole.reshape(count * MODES, length)[:, order])
        right.append(np.concatenate([high, high, low], 0))
        high, low = two_parts(turned.reshape(count * MODES, length)[:, order])
        left.append(np.concatenate([high.T, low.T, high.T], 1))
    return np.stack(left, 0), np.stack(right, 0)


def split2(x):
    high = x.astype(jnp.bfloat16)
    return high, (x - high.astype(jnp.float32)).astype(jnp.bfloat16)


def dot(a, b, dims=NN):
    return lax.dot_general(a, b, dims, preferred_element_type=jnp.float32)


def dot3(a, b, dims=NN):
    return dot(a[0], b[0], dims) + (dot(a[0], b[1], dims) + dot(a[1], b[0], dims))


def series(value, first, count):
    total = jnp.full(value.shape, 1.0 / math.factorial(2 * (count - 1) + first), jnp.float32)
    for n in range(count - 2, -1, -1):
        total = 1.0 / math.factorial(2 * n + first) - value * total
    return total


def cosine_of(cell):
    angle = (0.5 * TB - (cell + 0.5)) * (math.pi / TB)
    return angle * series(angle * angle, 1, 9)


def propagator(wave_squared, kx, ky):
    vertical = wave_squared - kx * kx - ky * ky
    root = jnp.sqrt(jnp.abs(vertical)) * depth_step
    squared = root * root
    moving = vertical > 0.0
    even = jnp.where(moving, series(squared, 0, 10), jnp.exp(-root))
    odd = jnp.where(moving, root * series(squared, 1, 10), 0.0)
    return even, odd


def wave_number(place, length):
    half, quarter = length // 2, length // 4
    index = 2 * lax.rem(place, quarter) + lax.div(place, half)
    index = jnp.where(place == quarter, half, index)
    return 2.0 * math.pi / length * index.astype(jnp.float32)


def take_lanes(x, index):
    return jnp.take_along_axis(x, index, axis=1, mode="promise_in_bounds")


def iota(shape, axis):
    return lax.broadcasted_iota(jnp.int32, shape, axis)


def program(
    cfg,
    spectra_hbm,
    tile_hbm,
    bin_hbm,
    offset_hbm,
    weight_hbm,
    freq_ref,
    slow_hbm,
    vel_hbm,
    hart_hbm,
    modes_x_hbm,
    modes_y_hbm,
    wave_ref,
    image_in,
    spectra_ref,
    tile_ref,
    bin_ref,
    offset_ref,
    weight_ref,
    slow_ref,
    hart,
    modes_x,
    modes_y,
    vel_first,
    vel_last,
    route_out,
    route_in,
    coef_out,
    coef_in,
    wide_even,
    wide_odd,
    band_even,
    band_odd,
    along_first,
    across_first,
    along_last,
    across_last,
    slabs,
    first_real,
    fwd_out,
    fwd_in,
    back_out,
    back_in,
    image_out,
    trace_sem,
    table_sem,
    route_sent,
    route_got,
    coef_sent,
    coef_got,
    vel_sem,
    fwd_sent,
    fwd_got,
    back_sent,
    back_got,
    image_sent,
    image_got,
):
    F, L, tiles, nx, ny, rows, data_rows, padded, nvel = cfg
    devices = F * L
    group = L // 2
    half_x, half_y = nx // 2, ny // 2
    band = ny // group
    slots = tiles * CAP
    per_group = nvel // REFS
    me_f = lax.axis_index("freq")
    me_l = lax.axis_index("lat")
    me = me_l * F + me_f
    side = lax.div(me_l, group)
    seat = lax.rem(me_l, group)

    barrier = pltpu.get_barrier_semaphore()

    def partner_of(at):
        other = lax.rem(me + at, devices)
        return other, {"freq": lax.rem(other, F), "lat": lax.div(other, F)}

    def greet(at, carry):
        _, device = partner_of(at)
        pl.semaphore_signal(barrier, inc=1, device_id=device, device_id_type=MESH)
        return carry

    inputs = [
        pltpu.make_async_copy(src, dst, trace_sem.at[at])
        for at, (src, dst) in enumerate(
            [
                (tile_hbm, tile_ref),
                (bin_hbm, bin_ref),
                (offset_hbm, offset_ref),
                (weight_hbm, weight_ref),
                (spectra_hbm, spectra_ref),
            ]
        )
    ]
    for load in inputs:
        load.start()
    lax.fori_loop(1, devices, greet, 0)
    loads = [
        pltpu.make_async_copy(src, dst, table_sem.at[at])
        for at, (src, dst) in enumerate(
            [
                (vel_hbm.at[0], vel_first.at[side]),
                (vel_hbm.at[1], vel_last),
                (modes_x_hbm, modes_x),
                (modes_y_hbm, modes_y),
                (hart_hbm, hart),
                (slow_hbm, slow_ref),
            ]
        )
    ]
    for load in loads:
        load.start()
    for load in inputs:
        load.wait()

    count = tile_ref.shape[1]
    width = 128
    tile = tile_ref[...]
    columns = [
        jnp.transpose(jnp.broadcast_to(tile[:, at : at + width], (width, width)))
        for at in range(0, count, width)
    ]
    earlier = iota((width, width), 0) < iota((width, width), 1)
    ranks = []
    for at in range(count // width):
        row = jnp.broadcast_to(tile[:, at * width : (at + 1) * width], (width, width))
        same = jnp.where((columns[at] == row) & earlier, 1, 0)
        for before in range(at):
            same = same + jnp.where(columns[before] == row, 1, 0)
        ranks.append(jnp.sum(same, 0, keepdims=True))
    rank = jnp.concatenate(ranks, 1)
    turned = lax.rem(lax.rem(tile, tiles) + me, tiles)
    slot = lax.div(tile, tiles) * slots + turned * CAP + rank

    cell = bin_ref[...]
    root_weight = jnp.sqrt(weight_ref[...])
    cell_x = lax.div(cell, TB).astype(jnp.float32) + offset_ref[0:1, :]
    cell_y = lax.rem(cell, TB).astype(jnp.float32) + offset_ref[1:2, :]
    feats = jnp.concatenate(
        [spectra_ref[0] * root_weight, spectra_ref[1] * root_weight]
        + [root_weight, cosine_of(cell_x), cosine_of(cell_y)]
        + [jnp.zeros((padded - data_rows - 3, count), jnp.float32)],
        0,
    )
    high = feats.astype(jnp.bfloat16)
    rest = feats - high.astype(jnp.float32)
    middle = rest.astype(jnp.bfloat16)
    low = (rest - middle.astype(jnp.float32)).astype(jnp.bfloat16)
    parts = jnp.concatenate([high, middle, low], 0)
    fold = (data_rows + 4) // 2
    wide = 256
    for at in range(0, devices * slots, wide):
        places = iota((wide, count), 0) + at
        chosen = jnp.where(places == slot, 1.0, 0.0).astype(jnp.bfloat16)
        got = dot(parts, chosen, NT)
        got = got[:padded] + got[padded : 2 * padded] + got[2 * padded :]
        for piece in range(wide // slots):
            block = got[:, piece * slots : (piece + 1) * slots]
            route_out[at // slots + piece] = jnp.concatenate([block[:fold], block[fold : 2 * fold]], 1)

    pl.semaphore_wait(barrier, devices - 1)

    def spread(out, into, sent, landed):
        def copy_of(at):
            other, device = partner_of(at)
            return pltpu.make_async_remote_copy(
                src_ref=out.at[other] if out.shape[0] == devices else out.at[lax.rem(other, F)],
                dst_ref=into.at[me],
                send_sem=sent.at[at],
                recv_sem=landed.at[at],
                device_id=device,
                device_id_type=MESH,
            )

        def start(at, carry):
            copy_of(at).start()
            return carry

        def arrive(at, carry):
            copy_of(at).wait_recv()
            return carry

        def leave(at, carry):
            copy_of(at).wait_send()
            return carry

        lax.fori_loop(1, devices, start, 0)
        return (
            lambda: lax.fori_loop(1, devices, arrive, 0),
            lambda: lax.fori_loop(1, devices, leave, 0),
        )

    arrive, leave_route = spread(route_out, route_in, route_sent, route_got)
    route_in[pl.ds(me, 1)] = route_out[pl.ds(me, 1)]

    for load in loads:
        load.wait()
    frequency = freq_ref[0]
    waves = []
    for depth_at in range(2):
        squares = []
        for g in range(REFS):
            total = slow_ref[depth_at, g * per_group]
            for i in range(1, per_group):
                total = total + slow_ref[depth_at, g * per_group + i]
            reference = total * (1.0 / per_group)
            squares.append((reference, (frequency * reference) * (frequency * reference)))
        waves.append(squares)

    chunk = 16
    quarter_x, quarter_y = nx // 4, ny // 4
    lane = iota((chunk, quarter_y), 1)
    first_ky = [wave_number(lane + parity * half_y, ny) for parity in range(2)]
    middle_ky = jnp.full((chunk, quarter_y), math.pi, jnp.float32)

    def wide_rows(g, kx):
        made = [propagator(waves[0][g][1], kx, ky) for ky in (*first_ky, middle_ky)]
        return [
            jnp.concatenate([even, jnp.where(lane == 0, middle, even), odd, odd], 1)
            for even, odd, middle in zip(*made)
        ]

    def wide_tables(at, carry):
        first = pl.multiple_of(lax.rem(at, quarter_x // chunk) * chunk, chunk)
        base = pl.multiple_of(lax.div(at, quarter_x // chunk) * half_x, half_x)
        kx = wave_number(iota((chunk, quarter_y), 0) + (first + base), nx)
        for g in range(REFS):
            for one, table in zip(wide_rows(g, kx), (wide_even, wide_odd)):
                for copy in range(2):
                    table[g, pl.ds(base + copy * quarter_x + first, chunk), :] = one
        return carry

    lax.fori_loop(0, half_x // chunk, wide_tables, 0)
    middle_kx = jnp.full((chunk, quarter_y), math.pi, jnp.float32)
    for g in range(REFS):
        for one, table in zip(wide_rows(g, middle_kx), (wide_even, wide_odd)):
            table[g, quarter_x : quarter_x + 1, :] = one[:1]
    arrive()

    parts = F if rows % (8 * F) == 0 else 1
    part_rows = rows // parts
    own_part = pl.ds(pl.multiple_of((me_f if parts > 1 else 0) * part_rows, part_rows), part_rows)
    mirror = pltpu.make_async_remote_copy(
        src_ref=vel_first.at[side, own_part],
        dst_ref=vel_first.at[side, own_part],
        send_sem=vel_sem.at[0],
        recv_sem=vel_sem.at[1],
        device_id={"lat": lax.rem(me_l + group, L)},
        device_id_type=MESH,
    )
    mirror.start()

    group_at = lax.div(lax.rem(iota((fold, 2 * slots), 1), slots), CAP)
    eye = jnp.where(iota((TERMS + data_rows, TERMS), 0) == iota((TERMS + data_rows, TERMS), 1), damping, 0.0)

    def chebyshev(cosine):
        terms = [jnp.ones_like(cosine), cosine]
        for _ in range(MODES - 2):
            terms.append(2.0 * cosine * terms[-1] - terms[-2])
        return terms

    normals = []
    for t in range(tiles):
        pieces = []
        for first in range(0, devices, tiles):
            picked = route_in[first]
            for i in range(1, tiles):
                picked = jnp.where(group_at == (t + i) % tiles, route_in[first + i], picked)
            pieces.append(picked)
        data = jnp.concatenate([piece[:, :slots] for piece in pieces], 1)
        place = jnp.concatenate([piece[:, slots:] for piece in pieces], 1)
        data = jnp.concatenate([data, place[: data_rows - fold]], 0)
        place = place[data_rows - fold :]
        scale = place[0:1]
        along_x = chebyshev(place[1:2])
        along_y = jnp.concatenate(chebyshev(place[2:3]), 0)
        basis = jnp.concatenate([(term * scale) * along_y for term in along_x], 0)
        right = jnp.concatenate([basis, data], 0)
        normals.append(
            eye
            + lax.dot_general(
                right, basis, NT, preferred_element_type=jnp.float32, precision=lax.Precision.HIGHEST
            )
        )
    inner = 128 // tiles
    outer = TERMS // inner
    lines = (TERMS + data_rows) // 8
    rest = []
    for at in range(outer):
        line = jnp.concatenate([one[:, at * inner : (at + 1) * inner] for one in normals], 1)
        rest.append([line[8 * j : 8 * (j + 1)] for j in range(lines)])
    lane = iota((8, 128), 1)
    within = lax.rem(lane, inner)
    for block in range(TERMS // 8):
        todo = range(block, lines)
        pivots = []
        for s in range(8):
            at, own = (8 * block + s) // inner, (8 * block + s) % inner
            pick = lane - within + own
            pivots.append({j: take_lanes(rest[at][j], pick) for j in todo})
        for s in range(8):
            at, own = (8 * block + s) // inner, (8 * block + s) % inner
            scale = 1.0 / pivots[s][block][s : s + 1]
            scaled = {j: pivots[s][j] * scale for j in todo}
            for later in range(s + 1, 8):
                factor = pivots[later][block][s : s + 1]
                pivots[later] = {j: pivots[later][j] - factor * scaled[j] for j in todo}
            for one in range(outer):
                factor = rest[one][block][s : s + 1]
                for j in todo:
                    value = rest[one][j] - factor * scaled[j]
                    rest[one][j] = jnp.where(within == own, scaled[j], value) if one == at else value
    width = tiles * MODES
    place = lax.rem(lane, width)
    pick = lax.div(place, MODES) * inner + lax.div(lane, width) * MODES + lax.rem(place, MODES)
    for one in range(outer):
        for j in range(TERMS // 8, lines):
            line = take_lanes(rest[one][j], pick)
            for s in range(8):
                part, f = divmod(8 * (j - TERMS // 8) + s, F)
                coef_out[f, part * outer + one : part * outer + one + 1, :] = line[s : s + 1]

    arrive, leave_coef = spread(coef_out, coef_in, coef_sent, coef_got)
    coef_in[pl.ds(me, 1)] = coef_out[pl.ds(me_f, 1)]

    mirror.wait_recv()
    handed = []
    for step in range(1, parts):
        other = lax.rem(me_f + step, F)
        handed.append(
            pltpu.make_async_remote_copy(
                src_ref=vel_first.at[1 - side, own_part],
                dst_ref=vel_first.at[1 - side, own_part],
                send_sem=vel_sem.at[2 * step],
                recv_sem=vel_sem.at[2 * step + 1],
                device_id={"freq": other},
                device_id_type=MESH,
            )
        )
    for copy in handed:
        copy.start()

    band_ky = wave_number(seat * band + iota((chunk, band), 1), ny)

    def band_tables(at, carry):
        first = pl.multiple_of(lax.rem(at, quarter_x // chunk) * chunk, chunk)
        base = pl.multiple_of(lax.div(at, quarter_x // chunk) * half_x, half_x)
        kx = wave_number(iota((chunk, band), 0) + (first + base), nx)
        for g in range(REFS):
            for one, table in zip(propagator(waves[1][g][1], kx, band_ky), (band_even, band_odd)):
                for copy in range(2):
                    table[g, pl.ds(base + copy * quarter_x + first, chunk), :] = one
        return carry

    lax.fori_loop(0, half_x // chunk, band_tables, 0)
    for g in range(REFS):
        middle = propagator(waves[1][g][1], jnp.full((chunk, band), math.pi, jnp.float32), band_ky)
        for one, table in zip(middle, (band_even, band_odd)):
            table[g, quarter_x : quarter_x + 1, :] = one[:1]

    def split_step(depth_at, velocity):
        cosine = jnp.zeros(velocity.shape, jnp.float32)
        sine = jnp.zeros(velocity.shape, jnp.float32)
        for i in range(nvel):
            shift = slow_ref[depth_at, i] - waves[depth_at][i // per_group][0]
            angle = jnp.full((8, 128), frequency * shift * depth_step, jnp.float32)
            squared = angle * angle
            cosine_i = series(squared, 0, 9)[0:1, 0:1]
            sine_i = (angle * series(squared, 1, 9))[0:1, 0:1]
            cosine = jnp.where(velocity == i, cosine_i, cosine)
            sine = jnp.where(velocity == i, sine_i, sine)
        return cosine, sine

    along_last[...], across_last[...] = split_step(1, vel_last[...])
    for copy in handed:
        copy.wait_recv()
    for one in range(2):
        along_first[one], across_first[one] = split_step(0, vel_first[one])
    arrive()

    def part_of(which):
        return hart[which, 0], hart[which, 1]

    even_k, even_k_t, odd_k, odd_k_t = (part_of(which) for which in range(4))

    def from_modes_of(parts):
        return jnp.concatenate([parts[0], parts[1], parts[0]], 1)

    per_row = (ny // TB) // tiles
    tile_rows = nx // TB
    mode_rows = tile_rows // 2 * MODES
    mode_columns = ny // TB // 2 * MODES
    sums, differences = [], []
    for part in range(2):
        lines = [
            jnp.concatenate(
                [
                    jnp.concatenate(
                        [
                            coef_in[
                                tile_row * per_row + j,
                                part * outer : (part + 1) * outer,
                                a * width : (a + 1) * width,
                            ]
                            for a in range(MODES // outer)
                        ],
                        0,
                    )
                    for j in range(per_row)
                ],
                1,
            )
            for tile_row in range(tile_rows)
        ]
        upper = jnp.concatenate(lines[: tile_rows // 2], 0)
        lower = jnp.concatenate(lines[tile_rows // 2 :], 0)
        for one in (upper + lower, upper - lower):
            left, right = one[:, :mode_columns], one[:, mode_columns:]
            sums.append(left + right)
            differences.append(left - right)
    spread_y = [
        dot(from_modes_of(split2(jnp.concatenate(one, 0))), modes_y[parity])
        for parity, one in enumerate((sums, differences))
    ]
    seat_rows = pl.ds(pl.multiple_of(seat * rows, rows), rows)
    made = [[None, None] for _ in range(REFS)]
    for parity in range(2):
        picked = [
            one[(2 * p + parity) * mode_rows : (2 * p + parity + 1) * mode_rows]
            for p in range(2)
            for one in spread_y
        ]
        high, low = split2(jnp.concatenate(picked, 1))
        spectrum = dot(modes_x[parity], jnp.concatenate([high, high, low], 0))
        real, imag = spectrum[:, :ny], spectrum[:, ny:]
        which = 2 * parity + 1
        own_high, own_low = hart[which, 0, seat_rows, :], hart[which, 1, seat_rows, :]
        both = jnp.concatenate([own_high, own_low], 0)
        part = slice(parity * half_x, (parity + 1) * half_x)
        for g in range(REFS):
            even, odd = wide_even[g, part, :], wide_odd[g, part, :]
            moved = split2(jnp.concatenate([real * even - imag * odd, real * odd + imag * even], 1))
            back = dot(both, moved[0])
            made[g][parity] = back[:rows] + (back[rows:] + dot(own_high, moved[1]))
    for g in range(REFS):
        for p in range(2):
            part = slice(p * ny, (p + 1) * ny)
            for at, slab in enumerate((made[g][0] + made[g][1], made[g][0] - made[g][1])):
                slabs[at, 2 * g + p] = slab[:, part]

    def inverse_y(x):
        u = dot3(split2(x[:, :half_y]), even_k)
        v = dot3(split2(x[:, half_y:]), odd_k)
        return jnp.concatenate([u + v, u - v], 1)

    def choose(made, velocity):
        real, imag = made[0]
        for g in range(1, REFS):
            chosen = velocity >= g * per_group
            real = jnp.where(chosen, made[g][0], real)
            imag = jnp.where(chosen, made[g][1], imag)
        return real, imag

    image_piece = ny // F

    def send_image(depth_at, real):
        for f in range(F):
            image_out[depth_at, f] = real[:, f * image_piece : (f + 1) * image_piece]
        copies = []
        for step in range(1, F):
            other = lax.rem(me_f + step, F)
            copies.append(
                pltpu.make_async_remote_copy(
                    src_ref=image_out.at[depth_at, other],
                    dst_ref=image_in.at[depth_at, me_f],
                    send_sem=image_sent.at[depth_at, step],
                    recv_sem=image_got.at[depth_at, step],
                    device_id={"freq": other},
                    device_id_type=MESH,
                )
            )
        for copy in copies:
            copy.start()
        image_in[depth_at, pl.ds(me_f, 1)] = image_out[depth_at, pl.ds(me_f, 1)]
        return copies

    def copies_of(at, out, into, sent, landed):
        copies = []
        for step in range(1, group):
            other = lax.rem(seat + step, group)
            copies.append(
                pltpu.make_async_remote_copy(
                    src_ref=out.at[at, other],
                    dst_ref=into.at[at, seat],
                    send_sem=sent.at[at, step],
                    recv_sem=landed.at[at, step],
                    device_id={"lat": side * group + other},
                    device_id_type=MESH,
                )
            )
        return copies

    def exchange(at, out, into, sent, landed):
        copies = copies_of(at, out, into, sent, landed)
        for copy in copies:
            copy.start()
        into[at, pl.ds(seat, 1)] = out[at, pl.ds(seat, 1)]
        return copies

    def first_rows(at, carry):
        field = inverse_y(slabs[at].reshape(2 * REFS * rows, ny))
        made = [
            (field[2 * g * rows : (2 * g + 1) * rows], field[(2 * g + 1) * rows : (2 * g + 2) * rows])
            for g in range(REFS)
        ]
        real, imag = choose(made, vel_first[at])
        cosine, sine = along_first[at], across_first[at]
        real, imag = real * cosine - imag * sine, real * sine + imag * cosine
        first_real[at] = real
        both = jnp.concatenate([real, imag], 0)
        left, right = both[:, :half_y], both[:, half_y:]
        line = jnp.concatenate(
            [dot3(split2(left + right), even_k_t), dot3(split2(left - right), odd_k_t)], 1
        )
        for dst in range(group):
            fwd_out[at, dst] = line[:, dst * band : (dst + 1) * band].reshape(2, rows, band)
        exchange(at, fwd_out, fwd_in, fwd_sent, fwd_got)
        return carry

    lax.fori_loop(0, 2, first_rows, 0)
    forward = [copies_of(at, fwd_out, fwd_in, fwd_sent, fwd_got) for at in range(2)]
    first_image = send_image(0, first_real[pl.ds(side, 1)].reshape(rows, ny))

    spectrum = []
    for copy in forward[0] + forward[1]:
        copy.wait_recv()
    for p in range(2):
        upper = jnp.concatenate([fwd_in[0, src, p] for src in range(group)], 0)
        lower = jnp.concatenate([fwd_in[1, src, p] for src in range(group)], 0)
        lines = []
        for one, table in ((upper + lower, even_k), (upper - lower, odd_k)):
            high, low = split2(one)
            line = dot(table[0], jnp.concatenate([high, low], 1))
            lines.append(line[:, :band] + (line[:, band:] + dot(table[1], high)))
        spectrum.append(lines)
    turn = (1 - 2 * side).astype(jnp.float32)
    backward = []
    for g in range(REFS):
        sides = []
        for parity, table in enumerate((even_k_t, odd_k_t)):
            part = slice(parity * half_x, (parity + 1) * half_x)
            even, odd = band_even[g, part, :], band_odd[g, part, :]
            real, imag = spectrum[0][parity], spectrum[1][parity]
            moved = jnp.concatenate([real * even - imag * odd, real * odd + imag * even], 1)
            sides.append(dot3(table, split2(moved)))
        back_out[g] = (sides[0] + turn * sides[1]).reshape(group, rows, 2 * band)
        backward.append(exchange(g, back_out, back_in, back_sent, back_got))
    made = []
    for g in range(REFS):
        for copy in backward[g]:
            copy.wait_recv()
        lines = [
            jnp.concatenate([back_in[g, src, :, p * band : (p + 1) * band] for src in range(group)], 1)
            for p in range(2)
        ]
        field = inverse_y(jnp.concatenate(lines, 0))
        made.append((field[:rows], field[rows:]))
    real, imag = choose(made, vel_last[...])
    cosine, sine = along_last[...], across_last[...]
    moved = real * cosine - imag * sine
    last_image = send_image(1, moved)
    wave_ref[0] = moved
    wave_ref[1] = real * sine + imag * cosine

    leave_route()
    leave_coef()
    mirror.wait_send()
    for copy in handed:
        copy.wait_send()
    for copies in forward + backward:
        for copy in copies:
            copy.wait_send()
    for copy in first_image + last_image:
        copy.wait()


def finish(wave_ref, part_ref, wave_hbm, image_hbm, total, sem):
    store = pltpu.make_async_copy(wave_ref, wave_hbm.at[:, 0], sem.at[0])
    store.start()
    image = part_ref[:, 0]
    for f in range(1, part_ref.shape[1]):
        image = image + part_ref[:, f]
    total[...] = image
    last = pltpu.make_async_copy(total, image_hbm, sem.at[1])
    last.start()
    store.wait()
    last.wait()


def stay(x):
    return pltpu.with_memory_space_constraint(x, pltpu.HBM)


def local(spectra, tile_route, bin_in_tile, trace_offset, weights, frequency, slowness, vel_index):
    F = lax.axis_size("freq")
    L = lax.axis_size("lat")
    devices = F * L
    steps, rows, ny = vel_index.shape
    assert steps == 2
    nx = rows * L
    tiles = (nx // TB) * (ny // TB) // devices
    slots = tiles * CAP
    count = spectra.shape[2]
    data_rows = 2 * spectra.shape[1]
    padded = 2 * data_rows
    group = L // 2
    band = ny // group
    nvel = slowness.shape[1]
    cfg = (F, L, tiles, nx, ny, rows, data_rows, padded, nvel)

    hart = jnp.asarray(half_tables(nx))
    outer = TERMS * tiles // 128
    modes_x, modes_y = (jnp.asarray(one) for one in mode_tables(nx, MODES // outer))

    f32, bf16, i32 = jnp.float32, jnp.bfloat16, jnp.int32
    dma = pltpu.SemaphoreType.DMA
    wave, images = pl.pallas_call(
        functools.partial(program, cfg),
        out_shape=[
            jax.ShapeDtypeStruct((2, rows, ny), f32),
            jax.ShapeDtypeStruct((2, F, rows, ny // F), f32),
        ],
        in_specs=[HBM] * 5 + [SMEM] + [HBM] * 5,
        out_specs=[VMEM, VMEM],
        scratch_shapes=[
            pltpu.VMEM(spectra.shape, f32),
            pltpu.VMEM((1, count), i32),
            pltpu.VMEM((1, count), i32),
            pltpu.VMEM((2, count), f32),
            pltpu.VMEM((1, count), f32),
            pltpu.SMEM(slowness.shape, f32),
            pltpu.VMEM(hart.shape, bf16),
            pltpu.VMEM(modes_x.shape, bf16),
            pltpu.VMEM(modes_y.shape, bf16),
            pltpu.VMEM((2, rows, ny), i32),
            pltpu.VMEM((rows, ny), i32),
            pltpu.VMEM((devices, (data_rows + 4) // 2, 2 * slots), f32),
            pltpu.VMEM((devices, (data_rows + 4) // 2, 2 * slots), f32),
            pltpu.VMEM((F, 2 * outer, 128), f32),
            pltpu.VMEM((devices, 2 * outer, 128), f32),
            pltpu.VMEM((REFS, nx, ny), f32),
            pltpu.VMEM((REFS, nx, ny), f32),
            pltpu.VMEM((REFS, nx, band), f32),
            pltpu.VMEM((REFS, nx, band), f32),
            pltpu.VMEM((2, rows, ny), f32),
            pltpu.VMEM((2, rows, ny), f32),
            pltpu.VMEM((rows, ny), f32),
            pltpu.VMEM((rows, ny), f32),
            pltpu.VMEM((2, 2 * REFS, rows, ny), f32),
            pltpu.VMEM((2, rows, ny), f32),
            pltpu.VMEM((2, group, 2, rows, band), f32),
            pltpu.VMEM((2, group, 2, rows, band), f32),
            pltpu.VMEM((REFS, group, rows, 2 * band), f32),
            pltpu.VMEM((REFS, group, rows, 2 * band), f32),
            pltpu.VMEM((2, F, rows, ny // F), f32),
            dma((5,)),
            dma((6,)),
            dma((devices,)),
            dma((devices,)),
            dma((devices,)),
            dma((devices,)),
            dma((2 * F,)),
            dma((2, group)),
            dma((2, group)),
            dma((REFS, group)),
            dma((REFS, group)),
            dma((2, F)),
            dma((2, F)),
        ],
        compiler_params=pltpu.CompilerParams(
            collective_id=0, has_side_effects=True, vmem_limit_bytes=40 << 20
        ),
    )(
        *map(stay, (spectra, tile_route.reshape(1, count), bin_in_tile.reshape(1, count))),
        *map(stay, (trace_offset, weights.reshape(1, count))),
        frequency,
        stay(slowness),
        *map(stay, (vel_index, hart, modes_x, modes_y)),
    )
    return pl.pallas_call(
        finish,
        out_shape=[
            jax.ShapeDtypeStruct((2, 1, rows, ny), f32),
            jax.ShapeDtypeStruct((2, rows, ny // F), f32),
        ],
        in_specs=[VMEM, VMEM],
        out_specs=[HBM, HBM],
        scratch_shapes=[pltpu.VMEM((2, rows, ny // F), f32), dma((2,))],
        compiler_params=pltpu.CompilerParams(vmem_limit_bytes=8 << 20),
    )(wave, images)


def solution(mesh):
    return jax.shard_map(
        local,
        mesh=mesh,
        in_specs=(
            P(None, None, ("freq", "lat")),
            P(("freq", "lat"), None),
            P(("freq", "lat")),
            P(None, ("freq", "lat")),
            P(("freq", "lat")),
            P("freq"),
            P(),
            P(None, "lat", None),
        ),
        out_specs=(P(None, "freq", "lat", None), P(None, "lat", "freq")),
        check_vma=False,
    )
```

```python
import functools
import math

import jax
import jax.numpy as jnp
import numpy as np
from jax import lax
from jax.experimental import pallas as pl
from jax.experimental.pallas import tpu as pltpu
from jax.sharding import PartitionSpec as P

TB = 32
MODES = 8
CAP = 8
TERMS = MODES * MODES
REFS = 2
CHUNKS = 2

damping = 1.0
depth_step = 1.0

NN = (((1,), (0,)), ((), ()))
NT = (((1,), (1,)), ((), ()))
VMEM = pl.BlockSpec(memory_space=pltpu.VMEM)
SMEM = pl.BlockSpec(memory_space=pltpu.SMEM)
HBM = pl.BlockSpec(memory_space=pltpu.HBM)
MESH = pl.DeviceIdType.MESH


def two_parts(exact):
    high = exact.astype(jnp.bfloat16)
    low = (exact - high.astype(np.float64)).astype(jnp.bfloat16)
    return high, low


def hartley(length):
    at = np.arange(length)
    angle = 2.0 * math.pi / length * (at[:, None] * at[None, :] % length)
    return (np.cos(angle) + np.sin(angle)) / math.sqrt(length)


def orders(length):
    at = np.arange(length // 4)
    even = np.concatenate([2 * at, (length - 2 * at) % length])
    even[length // 4] = length // 2
    return even, np.concatenate([2 * at + 1, length - 1 - 2 * at])


def half_tables(length):
    whole = hartley(length)[:, : length // 2]
    even, odd = (whole[order] for order in orders(length))
    return np.stack([np.stack(two_parts(one), 0) for one in (even, even.T, odd, odd.T)], 0)


def mode_tables(length, inner):
    cosines = np.cos(math.pi * np.arange(MODES)[:, None] * (np.arange(TB)[None, :] + 0.5) / TB)
    count = length // TB // 2
    fold = np.zeros((count, MODES, length))
    for tile in range(count):
        fold[tile, :, tile * TB : (tile + 1) * TB] = cosines
    whole = fold @ hartley(length)
    turned = whole.reshape(count, MODES // inner, inner, length).swapaxes(1, 2)
    left, right = [], []
    for order in orders(length):
        high, low = two_parts(whole.reshape(count * MODES, length)[:, order])
        right.append(np.concatenate([high, high, low], 0))
        high, low = two_parts(turned.reshape(count * MODES, length)[:, order])
        left.append(np.concatenate([high.T, low.T, high.T], 1))
    return np.stack(left, 0), np.stack(right, 0)


def split2(x):
    high = x.astype(jnp.bfloat16)
    return high, (x - high.astype(jnp.float32)).astype(jnp.bfloat16)


def dot(a, b, dims=NN):
    return lax.dot_general(a, b, dims, preferred_element_type=jnp.float32)


def dot3(a, b, dims=NN):
    return dot(a[0], b[0], dims) + (dot(a[0], b[1], dims) + dot(a[1], b[0], dims))


def series(value, first, count):
    total = jnp.full(value.shape, 1.0 / math.factorial(2 * (count - 1) + first), jnp.float32)
    for n in range(count - 2, -1, -1):
        total = 1.0 / math.factorial(2 * n + first) - value * total
    return total


def cosine_of(cell):
    angle = (0.5 * TB - (cell + 0.5)) * (math.pi / TB)
    return angle * series(angle * angle, 1, 9)


def propagator(wave_squared, kx, ky):
    vertical = wave_squared - kx * kx - ky * ky
    root = jnp.sqrt(jnp.abs(vertical)) * depth_step
    squared = root * root
    moving = vertical > 0.0
    even = jnp.where(moving, series(squared, 0, 10), jnp.exp(-root))
    odd = jnp.where(moving, root * series(squared, 1, 10), 0.0)
    return even, odd


def wave_number(place, length):
    half, quarter = length // 2, length // 4
    index = 2 * lax.rem(place, quarter) + lax.div(place, half)
    index = jnp.where(place == quarter, half, index)
    return 2.0 * math.pi / length * index.astype(jnp.float32)


def take_lanes(x, index):
    return jnp.take_along_axis(x, index, axis=1, mode="promise_in_bounds")


def iota(shape, axis):
    return lax.broadcasted_iota(jnp.int32, shape, axis)


def program(
    cfg,
    spectra_hbm,
    tile_hbm,
    bin_hbm,
    offset_hbm,
    weight_hbm,
    freq_ref,
    slow_hbm,
    vel_hbm,
    hart_hbm,
    modes_x_hbm,
    modes_y_hbm,
    wave_ref,
    image_in,
    spectra_ref,
    tile_ref,
    bin_ref,
    offset_ref,
    weight_ref,
    slow_ref,
    hart,
    modes_x,
    modes_y,
    vel_first,
    vel_last,
    route_out,
    route_in,
    coef_out,
    coef_in,
    wide_even,
    wide_odd,
    band_even,
    band_odd,
    along_first,
    across_first,
    along_last,
    across_last,
    slabs,
    first_real,
    fwd_out,
    fwd_in,
    back_out,
    back_in,
    image_out,
    trace_sem,
    table_sem,
    route_sent,
    route_got,
    coef_sent,
    coef_got,
    vel_sem,
    fwd_sent,
    fwd_got,
    back_sent,
    back_got,
    image_sent,
    image_got,
):
    F, L, tiles, nx, ny, rows, data_rows, padded, nvel = cfg
    devices = F * L
    group = L // 2
    half_x, half_y = nx // 2, ny // 2
    band = ny // group
    span = band // CHUNKS
    pair = 2 * span
    slots = tiles * CAP
    per_group = nvel // REFS
    me_f = lax.axis_index("freq")
    me_l = lax.axis_index("lat")
    me = me_l * F + me_f
    side = lax.div(me_l, group)
    seat = lax.rem(me_l, group)

    barrier = pltpu.get_barrier_semaphore()

    def partner_of(at):
        other = lax.rem(me + at, devices)
        return other, {"freq": lax.rem(other, F), "lat": lax.div(other, F)}

    def greet(at, carry):
        _, device = partner_of(at)
        pl.semaphore_signal(barrier, inc=1, device_id=device, device_id_type=MESH)
        return carry

    inputs = [
        pltpu.make_async_copy(src, dst, trace_sem.at[at])
        for at, (src, dst) in enumerate(
            [
                (tile_hbm, tile_ref),
                (bin_hbm, bin_ref),
                (offset_hbm, offset_ref),
                (weight_hbm, weight_ref),
                (spectra_hbm, spectra_ref),
            ]
        )
    ]
    for load in inputs:
        load.start()
    lax.fori_loop(1, devices, greet, 0)
    loads = [
        pltpu.make_async_copy(src, dst, table_sem.at[at])
        for at, (src, dst) in enumerate(
            [
                (vel_hbm.at[0], vel_first.at[side]),
                (vel_hbm.at[1], vel_last),
                (modes_x_hbm, modes_x),
                (modes_y_hbm, modes_y),
                (hart_hbm, hart),
                (slow_hbm, slow_ref),
            ]
        )
    ]
    for load in loads:
        load.start()
    for load in inputs:
        load.wait()

    count = tile_ref.shape[1]
    width = 128
    tile = tile_ref[...]
    columns = [
        jnp.transpose(jnp.broadcast_to(tile[:, at : at + width], (width, width)))
        for at in range(0, count, width)
    ]
    earlier = iota((width, width), 0) < iota((width, width), 1)
    ranks = []
    for at in range(count // width):
        row = jnp.broadcast_to(tile[:, at * width : (at + 1) * width], (width, width))
        same = jnp.where((columns[at] == row) & earlier, 1, 0)
        for before in range(at):
            same = same + jnp.where(columns[before] == row, 1, 0)
        ranks.append(jnp.sum(same, 0, keepdims=True))
    rank = jnp.concatenate(ranks, 1)
    turned = lax.rem(lax.rem(tile, tiles) + me, tiles)
    slot = lax.div(tile, tiles) * slots + turned * CAP + rank

    cell = bin_ref[...]
    root_weight = jnp.sqrt(weight_ref[...])
    cell_x = lax.div(cell, TB).astype(jnp.float32) + offset_ref[0:1, :]
    cell_y = lax.rem(cell, TB).astype(jnp.float32) + offset_ref[1:2, :]
    feats = jnp.concatenate(
        [spectra_ref[0] * root_weight, spectra_ref[1] * root_weight]
        + [root_weight, cosine_of(cell_x), cosine_of(cell_y)]
        + [jnp.zeros((padded - data_rows - 3, count), jnp.float32)],
        0,
    )
    high = feats.astype(jnp.bfloat16)
    rest = feats - high.astype(jnp.float32)
    middle = rest.astype(jnp.bfloat16)
    low = (rest - middle.astype(jnp.float32)).astype(jnp.bfloat16)
    parts = jnp.concatenate([high, middle, low], 0)
    fold = (data_rows + 4) // 2
    wide = 256
    for at in range(0, devices * slots, wide):
        places = iota((wide, count), 0) + at
        chosen = jnp.where(places == slot, 1.0, 0.0).astype(jnp.bfloat16)
        got = dot(parts, chosen, NT)
        got = got[:padded] + got[padded : 2 * padded] + got[2 * padded :]
        for piece in range(wide // slots):
            block = got[:, piece * slots : (piece + 1) * slots]
            route_out[at // slots + piece] = jnp.concatenate([block[:fold], block[fold : 2 * fold]], 1)

    pl.semaphore_wait(barrier, devices - 1)

    def spread(out, into, sent, landed):
        def copy_of(at):
            other, device = partner_of(at)
            return pltpu.make_async_remote_copy(
                src_ref=out.at[other] if out.shape[0] == devices else out.at[lax.rem(other, F)],
                dst_ref=into.at[me],
                send_sem=sent.at[at],
                recv_sem=landed.at[at],
                device_id=device,
                device_id_type=MESH,
            )

        def start(at, carry):
            copy_of(at).start()
            return carry

        def arrive(at, carry):
            copy_of(at).wait_recv()
            return carry

        def leave(at, carry):
            copy_of(at).wait_send()
            return carry

        lax.fori_loop(1, devices, start, 0)
        return (
            lambda: lax.fori_loop(1, devices, arrive, 0),
            lambda: lax.fori_loop(1, devices, leave, 0),
        )

    arrive, leave_route = spread(route_out, route_in, route_sent, route_got)
    route_in[pl.ds(me, 1)] = route_out[pl.ds(me, 1)]

    for load in loads:
        load.wait()
    frequency = freq_ref[0]
    waves = []
    for depth_at in range(2):
        squares = []
        for g in range(REFS):
            total = slow_ref[depth_at, g * per_group]
            for i in range(1, per_group):
                total = total + slow_ref[depth_at, g * per_group + i]
            reference = total * (1.0 / per_group)
            squares.append((reference, (frequency * reference) * (frequency * reference)))
        waves.append(squares)

    chunk = 16
    quarter_x, quarter_y = nx // 4, ny // 4
    lane = iota((chunk, quarter_y), 1)
    first_ky = [wave_number(lane + parity * half_y, ny) for parity in range(2)]
    middle_ky = jnp.full((chunk, quarter_y), math.pi, jnp.float32)

    def wide_rows(g, kx):
        made = [propagator(waves[0][g][1], kx, ky) for ky in (*first_ky, middle_ky)]
        return [
            jnp.concatenate([even, jnp.where(lane == 0, middle, even), odd, odd], 1)
            for even, odd, middle in zip(*made)
        ]

    def wide_tables(at, carry):
        first = pl.multiple_of(lax.rem(at, quarter_x // chunk) * chunk, chunk)
        base = pl.multiple_of(lax.div(at, quarter_x // chunk) * half_x, half_x)
        kx = wave_number(iota((chunk, quarter_y), 0) + (first + base), nx)
        for g in range(REFS):
            for one, table in zip(wide_rows(g, kx), (wide_even, wide_odd)):
                for copy in range(2):
                    table[g, pl.ds(base + copy * quarter_x + first, chunk), :] = one
        return carry

    lax.fori_loop(0, half_x // chunk, wide_tables, 0)
    middle_kx = jnp.full((chunk, quarter_y), math.pi, jnp.float32)
    for g in range(REFS):
        for one, table in zip(wide_rows(g, middle_kx), (wide_even, wide_odd)):
            table[g, quarter_x : quarter_x + 1, :] = one[:1]
    arrive()

    parts = F if rows % (8 * F) == 0 else 1
    part_rows = rows // parts
    own_part = pl.ds(pl.multiple_of((me_f if parts > 1 else 0) * part_rows, part_rows), part_rows)
    mirror = pltpu.make_async_remote_copy(
        src_ref=vel_first.at[side, own_part],
        dst_ref=vel_first.at[side, own_part],
        send_sem=vel_sem.at[0],
        recv_sem=vel_sem.at[1],
        device_id={"lat": lax.rem(me_l + group, L)},
        device_id_type=MESH,
    )
    mirror.start()

    group_at = lax.div(lax.rem(iota((fold, 2 * slots), 1), slots), CAP)
    eye = jnp.where(iota((TERMS + data_rows, TERMS), 0) == iota((TERMS + data_rows, TERMS), 1), damping, 0.0)

    def chebyshev(cosine):
        terms = [jnp.ones_like(cosine), cosine]
        for _ in range(MODES - 2):
            terms.append(2.0 * cosine * terms[-1] - terms[-2])
        return terms

    normals = []
    for t in range(tiles):
        pieces = []
        for first in range(0, devices, tiles):
            picked = route_in[first]
            for i in range(1, tiles):
                picked = jnp.where(group_at == (t + i) % tiles, route_in[first + i], picked)
            pieces.append(picked)
        data = jnp.concatenate([piece[:, :slots] for piece in pieces], 1)
        place = jnp.concatenate([piece[:, slots:] for piece in pieces], 1)
        data = jnp.concatenate([data, place[: data_rows - fold]], 0)
        place = place[data_rows - fold :]
        scale = place[0:1]
        along_x = chebyshev(place[1:2])
        along_y = jnp.concatenate(chebyshev(place[2:3]), 0)
        basis = jnp.concatenate([(term * scale) * along_y for term in along_x], 0)
        right = jnp.concatenate([basis, data], 0)
        normals.append(
            eye
            + lax.dot_general(
                right, basis, NT, preferred_element_type=jnp.float32, precision=lax.Precision.HIGHEST
            )
        )
    inner = 128 // tiles
    outer = TERMS // inner
    lines = (TERMS + data_rows) // 8
    rest = []
    for at in range(outer):
        line = jnp.concatenate([one[:, at * inner : (at + 1) * inner] for one in normals], 1)
        rest.append([line[8 * j : 8 * (j + 1)] for j in range(lines)])
    lane = iota((8, 128), 1)
    within = lax.rem(lane, inner)
    for block in range(TERMS // 8):
        todo = range(block, lines)
        pivots = []
        for s in range(8):
            at, own = (8 * block + s) // inner, (8 * block + s) % inner
            pick = lane - within + own
            pivots.append({j: take_lanes(rest[at][j], pick) for j in todo})
        for s in range(8):
            at, own = (8 * block + s) // inner, (8 * block + s) % inner
            scale = 1.0 / pivots[s][block][s : s + 1]
            scaled = {j: pivots[s][j] * scale for j in todo}
            for later in range(s + 1, 8):
                factor = pivots[later][block][s : s + 1]
                pivots[later] = {j: pivots[later][j] - factor * scaled[j] for j in todo}
            for one in range(outer):
                factor = rest[one][block][s : s + 1]
                for j in todo:
                    value = rest[one][j] - factor * scaled[j]
                    rest[one][j] = jnp.where(within == own, scaled[j], value) if one == at else value
    width = tiles * MODES
    place = lax.rem(lane, width)
    pick = lax.div(place, MODES) * inner + lax.div(lane, width) * MODES + lax.rem(place, MODES)
    for one in range(outer):
        for j in range(TERMS // 8, lines):
            line = take_lanes(rest[one][j], pick)
            for s in range(8):
                part, f = divmod(8 * (j - TERMS // 8) + s, F)
                coef_out[f, part * outer + one : part * outer + one + 1, :] = line[s : s + 1]

    arrive, leave_coef = spread(coef_out, coef_in, coef_sent, coef_got)
    coef_in[pl.ds(me, 1)] = coef_out[pl.ds(me_f, 1)]

    mirror.wait_recv()
    handed = []
    for step in range(1, parts):
        other = lax.rem(me_f + step, F)
        handed.append(
            pltpu.make_async_remote_copy(
                src_ref=vel_first.at[1 - side, own_part],
                dst_ref=vel_first.at[1 - side, own_part],
                send_sem=vel_sem.at[2 * step],
                recv_sem=vel_sem.at[2 * step + 1],
                device_id={"freq": other},
                device_id_type=MESH,
            )
        )
    for copy in handed:
        copy.start()

    pair_lane = iota((chunk, pair), 1)
    sign = jnp.where(pair_lane < span, -1.0, 1.0)
    band_ky = [
        wave_number(seat * band + c * span + lax.rem(pair_lane, span), ny) for c in range(CHUNKS)
    ]

    def band_rows(c, g, kx):
        even, odd = propagator(waves[1][g][1], kx, band_ky[c])
        return (even, band_even), (odd * sign, band_odd)

    def band_tables(at, carry):
        first = pl.multiple_of(lax.rem(at, quarter_x // chunk) * chunk, chunk)
        base = pl.multiple_of(lax.div(at, quarter_x // chunk) * half_x, half_x)
        kx = wave_number(iota((chunk, pair), 0) + (first + base), nx)
        for c in range(CHUNKS):
            for g in range(REFS):
                for one, table in band_rows(c, g, kx):
                    for copy in range(2):
                        table[c, g, pl.ds(base + copy * quarter_x + first, chunk), :] = one
        return carry

    lax.fori_loop(0, half_x // chunk, band_tables, 0)
    for c in range(CHUNKS):
        for g in range(REFS):
            for one, table in band_rows(c, g, jnp.full((chunk, pair), math.pi, jnp.float32)):
                table[c, g, quarter_x : quarter_x + 1, :] = one[:1]

    def split_step(depth_at, velocity):
        cosine = jnp.zeros(velocity.shape, jnp.float32)
        sine = jnp.zeros(velocity.shape, jnp.float32)
        for i in range(nvel):
            shift = slow_ref[depth_at, i] - waves[depth_at][i // per_group][0]
            angle = jnp.full((8, 128), frequency * shift * depth_step, jnp.float32)
            squared = angle * angle
            cosine_i = series(squared, 0, 9)[0:1, 0:1]
            sine_i = (angle * series(squared, 1, 9))[0:1, 0:1]
            cosine = jnp.where(velocity == i, cosine_i, cosine)
            sine = jnp.where(velocity == i, sine_i, sine)
        return cosine, sine

    along_last[...], across_last[...] = split_step(1, vel_last[...])
    for copy in handed:
        copy.wait_recv()
    for one in range(2):
        along_first[one], across_first[one] = split_step(0, vel_first[one])
    arrive()

    def part_of(which):
        return hart[which, 0], hart[which, 1]

    even_k, even_k_t, odd_k, odd_k_t = (part_of(which) for which in range(4))

    def from_modes_of(parts):
        return jnp.concatenate([parts[0], parts[1], parts[0]], 1)

    per_row = (ny // TB) // tiles
    tile_rows = nx // TB
    mode_rows = tile_rows // 2 * MODES
    mode_columns = ny // TB // 2 * MODES
    sums, differences = [], []
    for part in range(2):
        lines = [
            jnp.concatenate(
                [
                    jnp.concatenate(
                        [
                            coef_in[
                                tile_row * per_row + j,
                                part * outer : (part + 1) * outer,
                                a * width : (a + 1) * width,
                            ]
                            for a in range(MODES // outer)
                        ],
                        0,
                    )
                    for j in range(per_row)
                ],
                1,
            )
            for tile_row in range(tile_rows)
        ]
        upper = jnp.concatenate(lines[: tile_rows // 2], 0)
        lower = jnp.concatenate(lines[tile_rows // 2 :], 0)
        for one in (upper + lower, upper - lower):
            left, right = one[:, :mode_columns], one[:, mode_columns:]
            sums.append(left + right)
            differences.append(left - right)
    spread_y = [
        dot(from_modes_of(split2(jnp.concatenate(one, 0))), modes_y[parity])
        for parity, one in enumerate((sums, differences))
    ]
    seat_rows = pl.ds(pl.multiple_of(seat * rows, rows), rows)
    spans = []
    for parity in range(2):
        parts = []
        for p in range(2):
            at = (2 * p + parity) * mode_rows
            line = jnp.concatenate([one[at : at + mode_rows] for one in spread_y], 1)
            parts.append(split2(line))
        spans.append(parts)
    seats = []
    for which in (1, 3):
        own_high, own_low = hart[which, 0, seat_rows, :], hart[which, 1, seat_rows, :]
        seats.append((own_high, jnp.concatenate([own_high, own_low], 0)))
    wide = 128
    for first in range(0, ny, wide):
        lanes = slice(first, first + wide)
        made = [[None, None] for _ in range(REFS)]
        for parity in range(2):
            high = jnp.concatenate([one[0][:, lanes] for one in spans[parity]], 1)
            low = jnp.concatenate([one[1][:, lanes] for one in spans[parity]], 1)
            spectrum = dot(modes_x[parity], jnp.concatenate([high, high, low], 0))
            real, imag = spectrum[:, :wide], spectrum[:, wide:]
            own_high, both = seats[parity]
            part = slice(parity * half_x, (parity + 1) * half_x)
            for g in range(REFS):
                even, odd = wide_even[g, part, lanes], wide_odd[g, part, lanes]
                moved = split2(
                    jnp.concatenate([real * even - imag * odd, real * odd + imag * even], 1)
                )
                back = dot(both, moved[0])
                made[g][parity] = back[:rows] + (back[rows:] + dot(own_high, moved[1]))
        for g in range(REFS):
            for at, slab in enumerate((made[g][0] + made[g][1], made[g][0] - made[g][1])):
                for p in range(2):
                    slabs[at, 2 * g + p, :, lanes] = slab[:, p * wide : (p + 1) * wide]

    def inverse_y(x):
        u = dot3(split2(x[:, :half_y]), even_k)
        v = dot3(split2(x[:, half_y:]), odd_k)
        return jnp.concatenate([u + v, u - v], 1)

    def choose(made, velocity):
        real, imag = made[0]
        for g in range(1, REFS):
            chosen = velocity >= g * per_group
            real = jnp.where(chosen, made[g][0], real)
            imag = jnp.where(chosen, made[g][1], imag)
        return real, imag

    image_piece = ny // F

    def send_image(depth_at, real):
        for f in range(F):
            image_out[depth_at, f] = real[:, f * image_piece : (f + 1) * image_piece]
        copies = []
        for step in range(1, F):
            other = lax.rem(me_f + step, F)
            copies.append(
                pltpu.make_async_remote_copy(
                    src_ref=image_out.at[depth_at, other],
                    dst_ref=image_in.at[depth_at, me_f],
                    send_sem=image_sent.at[depth_at, step],
                    recv_sem=image_got.at[depth_at, step],
                    device_id={"freq": other},
                    device_id_type=MESH,
                )
            )
        for copy in copies:
            copy.start()
        image_in[depth_at, pl.ds(me_f, 1)] = image_out[depth_at, pl.ds(me_f, 1)]
        return copies

    def copies_of(at, c, out, into, sent, landed):
        copies = []
        for step in range(1, group):
            other = lax.rem(seat + step, group)
            copies.append(
                pltpu.make_async_remote_copy(
                    src_ref=out.at[at, c, other],
                    dst_ref=into.at[at, c, seat],
                    send_sem=sent.at[at, c, step],
                    recv_sem=landed.at[at, c, step],
                    device_id={"lat": side * group + other},
                    device_id_type=MESH,
                )
            )
        return copies

    def exchange(at, c, out, into, sent, landed):
        copies = copies_of(at, c, out, into, sent, landed)
        for copy in copies:
            copy.start()
        into[at, c, pl.ds(seat, 1)] = out[at, c, pl.ds(seat, 1)]
        return copies

    def first_rows(at, carry):
        field = inverse_y(slabs[at].reshape(2 * REFS * rows, ny))
        made = [
            (field[2 * g * rows : (2 * g + 1) * rows], field[(2 * g + 1) * rows : (2 * g + 2) * rows])
            for g in range(REFS)
        ]
        real, imag = choose(made, vel_first[at])
        cosine, sine = along_first[at], across_first[at]
        real, imag = real * cosine - imag * sine, real * sine + imag * cosine
        first_real[at] = real
        both = jnp.concatenate([real, imag], 0)
        left, right = both[:, :half_y], both[:, half_y:]
        line = jnp.concatenate(
            [dot3(split2(left + right), even_k_t), dot3(split2(left - right), odd_k_t)], 1
        )
        for c in range(CHUNKS):
            for dst in range(group):
                part = slice(dst * band + c * span, dst * band + (c + 1) * span)
                fwd_out[at, c, dst] = jnp.concatenate([line[:rows, part], line[rows:, part]], 1)
        exchange(at, 0, fwd_out, fwd_in, fwd_sent, fwd_got)
        return carry

    lax.fori_loop(0, 2, first_rows, 0)
    forward = [[copies_of(at, 0, fwd_out, fwd_in, fwd_sent, fwd_got) for at in range(2)]]
    for c in range(1, CHUNKS):
        forward.append([exchange(at, c, fwd_out, fwd_in, fwd_sent, fwd_got) for at in range(2)])
    forward = [sum(copies, []) for copies in forward]
    first_image = send_image(0, first_real[pl.ds(side, 1)].reshape(rows, ny))

    turn = (1 - 2 * side).astype(jnp.float32)

    def apply(table, x):
        high, low = split2(x)
        made = dot(table[0], jnp.concatenate([high, low], 1))
        return made[:, :pair] + (made[:, pair:] + dot(table[1], high))

    backward = []
    for c in range(CHUNKS):
        for copy in forward[c]:
            copy.wait_recv()
        upper, lower = fwd_in[0, c].reshape(half_x, pair), fwd_in[1, c].reshape(half_x, pair)
        spectrum = []
        for one, table in ((upper + lower, even_k), (upper - lower, odd_k)):
            line = apply(table, one)
            spectrum.append((line, jnp.concatenate([line[:, span:], line[:, :span]], 1)))
        for g in range(REFS):
            sides = []
            for parity, table in enumerate((even_k_t, odd_k_t)):
                part = slice(parity * half_x, (parity + 1) * half_x)
                line, swapped = spectrum[parity]
                sides.append(
                    apply(table, line * band_even[c, g, part, :] + swapped * band_odd[c, g, part, :])
                )
            back_out[g, c] = (sides[0] + turn * sides[1]).reshape(group, rows, pair)
            backward.append(exchange(g, c, back_out, back_in, back_sent, back_got))
    made = []
    for g in range(REFS):
        for c in range(CHUNKS):
            for copy in backward[c * REFS + g]:
                copy.wait_recv()
        lines = [
            jnp.concatenate(
                [
                    back_in[g, c, src, :, p * span : (p + 1) * span]
                    for src in range(group)
                    for c in range(CHUNKS)
                ],
                1,
            )
            for p in range(2)
        ]
        field = inverse_y(jnp.concatenate(lines, 0))
        made.append((field[:rows], field[rows:]))
    real, imag = choose(made, vel_last[...])
    cosine, sine = along_last[...], across_last[...]
    moved = real * cosine - imag * sine
    last_image = send_image(1, moved)
    wave_ref[0] = moved
    wave_ref[1] = real * sine + imag * cosine

    leave_route()
    leave_coef()
    mirror.wait_send()
    for copy in handed:
        copy.wait_send()
    for copies in forward + backward:
        for copy in copies:
            copy.wait_send()
    for copy in first_image + last_image:
        copy.wait()


def finish(wave_ref, part_ref, wave_hbm, image_hbm, total, sem):
    store = pltpu.make_async_copy(wave_ref, wave_hbm.at[:, 0], sem.at[0])
    store.start()
    image = part_ref[:, 0]
    for f in range(1, part_ref.shape[1]):
        image = image + part_ref[:, f]
    total[...] = image
    last = pltpu.make_async_copy(total, image_hbm, sem.at[1])
    last.start()
    store.wait()
    last.wait()


def stay(x):
    return pltpu.with_memory_space_constraint(x, pltpu.HBM)


def local(spectra, tile_route, bin_in_tile, trace_offset, weights, frequency, slowness, vel_index):
    F = lax.axis_size("freq")
    L = lax.axis_size("lat")
    devices = F * L
    steps, rows, ny = vel_index.shape
    assert steps == 2
    nx = rows * L
    tiles = (nx // TB) * (ny // TB) // devices
    slots = tiles * CAP
    count = spectra.shape[2]
    data_rows = 2 * spectra.shape[1]
    padded = 2 * data_rows
    group = L // 2
    pair = 2 * (ny // group) // CHUNKS
    nvel = slowness.shape[1]
    cfg = (F, L, tiles, nx, ny, rows, data_rows, padded, nvel)

    hart = jnp.asarray(half_tables(nx))
    outer = TERMS * tiles // 128
    modes_x, modes_y = (jnp.asarray(one) for one in mode_tables(nx, MODES // outer))

    f32, bf16, i32 = jnp.float32, jnp.bfloat16, jnp.int32
    dma = pltpu.SemaphoreType.DMA
    wave, images = pl.pallas_call(
        functools.partial(program, cfg),
        out_shape=[
            jax.ShapeDtypeStruct((2, rows, ny), f32),
            jax.ShapeDtypeStruct((2, F, rows, ny // F), f32),
        ],
        in_specs=[HBM] * 5 + [SMEM] + [HBM] * 5,
        out_specs=[VMEM, VMEM],
        scratch_shapes=[
            pltpu.VMEM(spectra.shape, f32),
            pltpu.VMEM((1, count), i32),
            pltpu.VMEM((1, count), i32),
            pltpu.VMEM((2, count), f32),
            pltpu.VMEM((1, count), f32),
            pltpu.SMEM(slowness.shape, f32),
            pltpu.VMEM(hart.shape, bf16),
            pltpu.VMEM(modes_x.shape, bf16),
            pltpu.VMEM(modes_y.shape, bf16),
            pltpu.VMEM((2, rows, ny), i32),
            pltpu.VMEM((rows, ny), i32),
            pltpu.VMEM((devices, (data_rows + 4) // 2, 2 * slots), f32),
            pltpu.VMEM((devices, (data_rows + 4) // 2, 2 * slots), f32),
            pltpu.VMEM((F, 2 * outer, 128), f32),
            pltpu.VMEM((devices, 2 * outer, 128), f32),
            pltpu.VMEM((REFS, nx, ny), f32),
            pltpu.VMEM((REFS, nx, ny), f32),
            pltpu.VMEM((CHUNKS, REFS, nx, pair), f32),
            pltpu.VMEM((CHUNKS, REFS, nx, pair), f32),
            pltpu.VMEM((2, rows, ny), f32),
            pltpu.VMEM((2, rows, ny), f32),
            pltpu.VMEM((rows, ny), f32),
            pltpu.VMEM((rows, ny), f32),
            pltpu.VMEM((2, 2 * REFS, rows, ny), f32),
            pltpu.VMEM((2, rows, ny), f32),
            pltpu.VMEM((2, CHUNKS, group, rows, pair), f32),
            pltpu.VMEM((2, CHUNKS, group, rows, pair), f32),
            pltpu.VMEM((REFS, CHUNKS, group, rows, pair), f32),
            pltpu.VMEM((REFS, CHUNKS, group, rows, pair), f32),
            pltpu.VMEM((2, F, rows, ny // F), f32),
            dma((5,)),
            dma((6,)),
            dma((devices,)),
            dma((devices,)),
            dma((devices,)),
            dma((devices,)),
            dma((2 * F,)),
            dma((2, CHUNKS, group)),
            dma((2, CHUNKS, group)),
            dma((REFS, CHUNKS, group)),
            dma((REFS, CHUNKS, group)),
            dma((2, F)),
            dma((2, F)),
        ],
        compiler_params=pltpu.CompilerParams(
            collective_id=0, has_side_effects=True, vmem_limit_bytes=40 << 20
        ),
    )(
        *map(stay, (spectra, tile_route.reshape(1, count), bin_in_tile.reshape(1, count))),
        *map(stay, (trace_offset, weights.reshape(1, count))),
        frequency,
        stay(slowness),
        *map(stay, (vel_index, hart, modes_x, modes_y)),
    )
    return pl.pallas_call(
        finish,
        out_shape=[
            jax.ShapeDtypeStruct((2, 1, rows, ny), f32),
            jax.ShapeDtypeStruct((2, rows, ny // F), f32),
        ],
        in_specs=[VMEM, VMEM],
        out_specs=[HBM, HBM],
        scratch_shapes=[pltpu.VMEM((2, rows, ny // F), f32), dma((2,))],
        compiler_params=pltpu.CompilerParams(vmem_limit_bytes=8 << 20),
    )(wave, images)


def solution(mesh):
    return jax.shard_map(
        local,
        mesh=mesh,
        in_specs=(
            P(None, None, ("freq", "lat")),
            P(("freq", "lat"), None),
            P(("freq", "lat")),
            P(None, ("freq", "lat")),
            P(("freq", "lat")),
            P("freq"),
            P(),
            P(None, "lat", None),
        ),
        out_specs=(P(None, "freq", "lat", None), P(None, "lat", "freq")),
        check_vma=False,
    )
```

```python
import functools
import math

import jax
import jax.numpy as jnp
import numpy as np
from jax import lax
from jax.experimental import pallas as pl
from jax.experimental.pallas import tpu as pltpu
from jax.sharding import PartitionSpec as P

TB = 32
MODES = 8
CAP = 8
TERMS = MODES * MODES
REFS = 2
CHUNKS = 2

damping = 1.0
depth_step = 1.0

NN = (((1,), (0,)), ((), ()))
NT = (((1,), (1,)), ((), ()))
VMEM = pl.BlockSpec(memory_space=pltpu.VMEM)
SMEM = pl.BlockSpec(memory_space=pltpu.SMEM)
HBM = pl.BlockSpec(memory_space=pltpu.HBM)
MESH = pl.DeviceIdType.MESH


def two_parts(exact):
    high = exact.astype(jnp.bfloat16)
    low = (exact - high.astype(np.float64)).astype(jnp.bfloat16)
    return high, low


def hartley(length):
    at = np.arange(length)
    angle = 2.0 * math.pi / length * (at[:, None] * at[None, :] % length)
    return (np.cos(angle) + np.sin(angle)) / math.sqrt(length)


def orders(length):
    at = np.arange(length // 4)
    even = np.concatenate([2 * at, (length - 2 * at) % length])
    even[length // 4] = length // 2
    return even, np.concatenate([2 * at + 1, length - 1 - 2 * at])


def half_tables(length):
    whole = hartley(length)[:, : length // 2]
    even, odd = (whole[order] for order in orders(length))
    return np.stack([np.stack(two_parts(one), 0) for one in (even, even.T, odd, odd.T)], 0)


def mode_tables(length, inner):
    cosines = np.cos(math.pi * np.arange(MODES)[:, None] * (np.arange(TB)[None, :] + 0.5) / TB)
    count = length // TB // 2
    fold = np.zeros((count, MODES, length))
    for tile in range(count):
        fold[tile, :, tile * TB : (tile + 1) * TB] = cosines
    whole = fold @ hartley(length)
    turned = whole.reshape(count, MODES // inner, inner, length).swapaxes(1, 2)
    left, right = [], []
    for order in orders(length):
        high, low = two_parts(whole.reshape(count * MODES, length)[:, order])
        right.append(np.concatenate([high, high, low], 0))
        high, low = two_parts(turned.reshape(count * MODES, length)[:, order])
        left.append(np.concatenate([high.T, low.T, high.T], 1))
    return np.stack(left, 0), np.stack(right, 0)


def split2(x):
    high = x.astype(jnp.bfloat16)
    return high, (x - high.astype(jnp.float32)).astype(jnp.bfloat16)


def dot(a, b, dims=NN):
    return lax.dot_general(a, b, dims, preferred_element_type=jnp.float32)


def dot3(a, b, dims=NN):
    return dot(a[0], b[0], dims) + (dot(a[0], b[1], dims) + dot(a[1], b[0], dims))


def series(value, first, count):
    total = jnp.full(value.shape, 1.0 / math.factorial(2 * (count - 1) + first), jnp.float32)
    for n in range(count - 2, -1, -1):
        total = 1.0 / math.factorial(2 * n + first) - value * total
    return total


def cosine_of(cell):
    angle = (0.5 * TB - (cell + 0.5)) * (math.pi / TB)
    return angle * series(angle * angle, 1, 9)


def propagator(wave_squared, kx, ky):
    vertical = wave_squared - kx * kx - ky * ky
    root = jnp.sqrt(jnp.abs(vertical)) * depth_step
    squared = root * root
    moving = vertical > 0.0
    even = jnp.where(moving, series(squared, 0, 10), jnp.exp(-root))
    odd = jnp.where(moving, root * series(squared, 1, 10), 0.0)
    return even, odd


def wave_number(place, length):
    half, quarter = length // 2, length // 4
    index = 2 * lax.rem(place, quarter) + lax.div(place, half)
    index = jnp.where(place == quarter, half, index)
    return 2.0 * math.pi / length * index.astype(jnp.float32)


def take_lanes(x, index):
    return jnp.take_along_axis(x, index, axis=1, mode="promise_in_bounds")


def iota(shape, axis):
    return lax.broadcasted_iota(jnp.int32, shape, axis)


def program(
    cfg,
    spectra_hbm,
    tile_hbm,
    bin_hbm,
    offset_hbm,
    weight_hbm,
    freq_ref,
    slow_hbm,
    vel_hbm,
    hart_hbm,
    modes_x_hbm,
    modes_y_hbm,
    wave_ref,
    image_in,
    spectra_ref,
    tile_ref,
    bin_ref,
    offset_ref,
    weight_ref,
    slow_ref,
    hart,
    modes_x,
    modes_y,
    vel_first,
    vel_last,
    route_out,
    route_in,
    coef_out,
    coef_in,
    wide_even,
    wide_odd,
    band_even,
    band_odd,
    along_first,
    across_first,
    along_last,
    across_last,
    slabs,
    first_real,
    fwd_out,
    fwd_in,
    back_out,
    back_in,
    image_out,
    trace_sem,
    table_sem,
    route_sent,
    route_got,
    coef_sent,
    coef_got,
    vel_sem,
    fwd_sent,
    fwd_got,
    back_sent,
    back_got,
    image_sent,
    image_got,
):
    F, L, tiles, nx, ny, rows, data_rows, padded, nvel = cfg
    devices = F * L
    group = L // 2
    half_x, half_y = nx // 2, ny // 2
    band = ny // group
    span = band // CHUNKS
    pair = 2 * span
    slots = tiles * CAP
    per_group = nvel // REFS
    me_f = lax.axis_index("freq")
    me_l = lax.axis_index("lat")
    me = me_l * F + me_f
    side = lax.div(me_l, group)
    seat = lax.rem(me_l, group)

    barrier = pltpu.get_barrier_semaphore()

    def partner_of(at):
        other = lax.rem(me + at, devices)
        return other, {"freq": lax.rem(other, F), "lat": lax.div(other, F)}

    def greet(at, carry):
        _, device = partner_of(at)
        pl.semaphore_signal(barrier, inc=1, device_id=device, device_id_type=MESH)
        return carry

    inputs = [
        pltpu.make_async_copy(src, dst, trace_sem.at[at])
        for at, (src, dst) in enumerate(
            [
                (tile_hbm, tile_ref),
                (bin_hbm, bin_ref),
                (offset_hbm, offset_ref),
                (weight_hbm, weight_ref),
                (spectra_hbm, spectra_ref),
            ]
        )
    ]
    for load in inputs:
        load.start()
    lax.fori_loop(1, devices, greet, 0)
    loads = [
        pltpu.make_async_copy(src, dst, table_sem.at[at])
        for at, (src, dst) in enumerate(
            [
                (vel_hbm.at[0], vel_first.at[side]),
                (vel_hbm.at[1], vel_last),
                (modes_x_hbm, modes_x),
                (modes_y_hbm, modes_y),
                (hart_hbm, hart),
                (slow_hbm, slow_ref),
            ]
        )
    ]
    for load in loads:
        load.start()
    for load in inputs:
        load.wait()

    count = tile_ref.shape[1]
    width = 128
    tile = tile_ref[...]
    columns = [
        jnp.transpose(jnp.broadcast_to(tile[:, at : at + width], (width, width)))
        for at in range(0, count, width)
    ]
    earlier = iota((width, width), 0) < iota((width, width), 1)
    ranks = []
    for at in range(count // width):
        row = jnp.broadcast_to(tile[:, at * width : (at + 1) * width], (width, width))
        same = jnp.where((columns[at] == row) & earlier, 1, 0)
        for before in range(at):
            same = same + jnp.where(columns[before] == row, 1, 0)
        ranks.append(jnp.sum(same, 0, keepdims=True))
    rank = jnp.concatenate(ranks, 1)
    turned = lax.rem(lax.rem(tile, tiles) + me, tiles)
    slot = lax.div(tile, tiles) * slots + turned * CAP + rank

    cell = bin_ref[...]
    root_weight = jnp.sqrt(weight_ref[...])
    cell_x = lax.div(cell, TB).astype(jnp.float32) + offset_ref[0:1, :]
    cell_y = lax.rem(cell, TB).astype(jnp.float32) + offset_ref[1:2, :]
    feats = jnp.concatenate(
        [spectra_ref[0] * root_weight, spectra_ref[1] * root_weight]
        + [root_weight, cosine_of(cell_x), cosine_of(cell_y)]
        + [jnp.zeros((padded - data_rows - 3, count), jnp.float32)],
        0,
    )
    high = feats.astype(jnp.bfloat16)
    rest = feats - high.astype(jnp.float32)
    middle = rest.astype(jnp.bfloat16)
    low = (rest - middle.astype(jnp.float32)).astype(jnp.bfloat16)
    parts = jnp.concatenate([high, middle, low], 0)
    fold = (data_rows + 4) // 2
    wide = 256
    for at in range(0, devices * slots, wide):
        places = iota((wide, count), 0) + at
        chosen = jnp.where(places == slot, 1.0, 0.0).astype(jnp.bfloat16)
        got = dot(parts, chosen, NT)
        got = got[:padded] + got[padded : 2 * padded] + got[2 * padded :]
        for piece in range(wide // slots):
            block = got[:, piece * slots : (piece + 1) * slots]
            route_out[at // slots + piece] = jnp.concatenate([block[:fold], block[fold : 2 * fold]], 1)

    pl.semaphore_wait(barrier, devices - 1)

    def spread(out, into, sent, landed):
        def copy_of(at):
            other, device = partner_of(at)
            return pltpu.make_async_remote_copy(
                src_ref=out.at[other] if out.shape[0] == devices else out.at[lax.rem(other, F)],
                dst_ref=into.at[me],
                send_sem=sent.at[at],
                recv_sem=landed.at[at],
                device_id=device,
                device_id_type=MESH,
            )

        def start(at, carry):
            copy_of(at).start()
            return carry

        def arrive(at, carry):
            copy_of(at).wait_recv()
            return carry

        def leave(at, carry):
            copy_of(at).wait_send()
            return carry

        lax.fori_loop(1, devices, start, 0)
        return (
            lambda: lax.fori_loop(1, devices, arrive, 0),
            lambda: lax.fori_loop(1, devices, leave, 0),
        )

    arrive, leave_route = spread(route_out, route_in, route_sent, route_got)
    route_in[pl.ds(me, 1)] = route_out[pl.ds(me, 1)]

    for load in loads:
        load.wait()
    frequency = freq_ref[0]
    waves = []
    for depth_at in range(2):
        squares = []
        for g in range(REFS):
            total = slow_ref[depth_at, g * per_group]
            for i in range(1, per_group):
                total = total + slow_ref[depth_at, g * per_group + i]
            reference = total * (1.0 / per_group)
            squares.append((reference, (frequency * reference) * (frequency * reference)))
        waves.append(squares)

    chunk = 16
    quarter_x, quarter_y = nx // 4, ny // 4
    lane = iota((chunk, quarter_y), 1)
    first_ky = [wave_number(lane + parity * half_y, ny) for parity in range(2)]
    middle_ky = jnp.full((chunk, quarter_y), math.pi, jnp.float32)

    def wide_rows(g, kx):
        made = [propagator(waves[0][g][1], kx, ky) for ky in (*first_ky, middle_ky)]
        return [
            jnp.concatenate([even, jnp.where(lane == 0, middle, even), odd, odd], 1)
            for even, odd, middle in zip(*made)
        ]

    def wide_tables(at, carry):
        first = pl.multiple_of(lax.rem(at, quarter_x // chunk) * chunk, chunk)
        base = pl.multiple_of(lax.div(at, quarter_x // chunk) * half_x, half_x)
        kx = wave_number(iota((chunk, quarter_y), 0) + (first + base), nx)
        for g in range(REFS):
            for one, table in zip(wide_rows(g, kx), (wide_even, wide_odd)):
                for copy in range(2):
                    table[g, pl.ds(base + copy * quarter_x + first, chunk), :] = one
        return carry

    lax.fori_loop(0, half_x // chunk, wide_tables, 0)
    middle_kx = jnp.full((chunk, quarter_y), math.pi, jnp.float32)
    for g in range(REFS):
        for one, table in zip(wide_rows(g, middle_kx), (wide_even, wide_odd)):
            table[g, quarter_x : quarter_x + 1, :] = one[:1]
    arrive()

    parts = F if rows % (8 * F) == 0 else 1
    part_rows = rows // parts
    own_part = pl.ds(pl.multiple_of((me_f if parts > 1 else 0) * part_rows, part_rows), part_rows)
    mirror = pltpu.make_async_remote_copy(
        src_ref=vel_first.at[side, own_part],
        dst_ref=vel_first.at[side, own_part],
        send_sem=vel_sem.at[0],
        recv_sem=vel_sem.at[1],
        device_id={"lat": lax.rem(me_l + group, L)},
        device_id_type=MESH,
    )
    mirror.start()

    group_at = lax.div(lax.rem(iota((fold, 2 * slots), 1), slots), CAP)
    eye = jnp.where(iota((TERMS + data_rows, TERMS), 0) == iota((TERMS + data_rows, TERMS), 1), damping, 0.0)

    def chebyshev(cosine):
        terms = [jnp.ones_like(cosine), cosine]
        for _ in range(MODES - 2):
            terms.append(2.0 * cosine * terms[-1] - terms[-2])
        return terms

    normals = []
    for t in range(tiles):
        pieces = []
        for first in range(0, devices, tiles):
            picked = route_in[first]
            for i in range(1, tiles):
                picked = jnp.where(group_at == (t + i) % tiles, route_in[first + i], picked)
            pieces.append(picked)
        data = jnp.concatenate([piece[:, :slots] for piece in pieces], 1)
        place = jnp.concatenate([piece[:, slots:] for piece in pieces], 1)
        data = jnp.concatenate([data, place[: data_rows - fold]], 0)
        place = place[data_rows - fold :]
        scale = place[0:1]
        along_x = chebyshev(place[1:2])
        along_y = jnp.concatenate(chebyshev(place[2:3]), 0)
        basis = jnp.concatenate([(term * scale) * along_y for term in along_x], 0)
        right = jnp.concatenate([basis, data], 0)
        normals.append(
            eye
            + lax.dot_general(
                right, basis, NT, preferred_element_type=jnp.float32, precision=lax.Precision.HIGHEST
            )
        )
    inner = 128 // tiles
    outer = TERMS // inner
    lines = (TERMS + data_rows) // 8
    rest = []
    for at in range(outer):
        line = jnp.concatenate([one[:, at * inner : (at + 1) * inner] for one in normals], 1)
        rest.append([line[8 * j : 8 * (j + 1)] for j in range(lines)])
    lane = iota((8, 128), 1)
    within = lax.rem(lane, inner)
    for block in range(TERMS // 8):
        todo = range(block, lines)
        pivots = []
        for s in range(8):
            at, own = (8 * block + s) // inner, (8 * block + s) % inner
            pick = lane - within + own
            pivots.append({j: take_lanes(rest[at][j], pick) for j in todo})
        for s in range(8):
            at, own = (8 * block + s) // inner, (8 * block + s) % inner
            scale = 1.0 / pivots[s][block][s : s + 1]
            scaled = {j: pivots[s][j] * scale for j in todo}
            for later in range(s + 1, 8):
                factor = pivots[later][block][s : s + 1]
                pivots[later] = {j: pivots[later][j] - factor * scaled[j] for j in todo}
            for one in range(outer):
                factor = rest[one][block][s : s + 1]
                for j in todo:
                    value = rest[one][j] - factor * scaled[j]
                    rest[one][j] = jnp.where(within == own, scaled[j], value) if one == at else value
    width = tiles * MODES
    place = lax.rem(lane, width)
    pick = lax.div(place, MODES) * inner + lax.div(lane, width) * MODES + lax.rem(place, MODES)
    for one in range(outer):
        for j in range(TERMS // 8, lines):
            line = take_lanes(rest[one][j], pick)
            for s in range(8):
                part, f = divmod(8 * (j - TERMS // 8) + s, F)
                coef_out[f, part * outer + one : part * outer + one + 1, :] = line[s : s + 1]

    arrive, leave_coef = spread(coef_out, coef_in, coef_sent, coef_got)
    coef_in[pl.ds(me, 1)] = coef_out[pl.ds(me_f, 1)]

    mirror.wait_recv()
    handed = []
    for step in range(1, parts):
        other = lax.rem(me_f + step, F)
        handed.append(
            pltpu.make_async_remote_copy(
                src_ref=vel_first.at[1 - side, own_part],
                dst_ref=vel_first.at[1 - side, own_part],
                send_sem=vel_sem.at[2 * step],
                recv_sem=vel_sem.at[2 * step + 1],
                device_id={"freq": other},
                device_id_type=MESH,
            )
        )
    for copy in handed:
        copy.start()

    pair_lane = iota((chunk, pair), 1)
    sign = jnp.where(pair_lane < span, -1.0, 1.0)
    band_ky = [
        wave_number(seat * band + c * span + lax.rem(pair_lane, span), ny) for c in range(CHUNKS)
    ]

    def band_rows(c, g, kx):
        even, odd = propagator(waves[1][g][1], kx, band_ky[c])
        return (even, band_even), (odd * sign, band_odd)

    def band_tables(at, carry):
        first = pl.multiple_of(lax.rem(at, quarter_x // chunk) * chunk, chunk)
        base = pl.multiple_of(lax.div(at, quarter_x // chunk) * half_x, half_x)
        kx = wave_number(iota((chunk, pair), 0) + (first + base), nx)
        for c in range(CHUNKS):
            for g in range(REFS):
                for one, table in band_rows(c, g, kx):
                    for copy in range(2):
                        table[c, g, pl.ds(base + copy * quarter_x + first, chunk), :] = one
        return carry

    lax.fori_loop(0, half_x // chunk, band_tables, 0)
    for c in range(CHUNKS):
        for g in range(REFS):
            for one, table in band_rows(c, g, jnp.full((chunk, pair), math.pi, jnp.float32)):
                table[c, g, quarter_x : quarter_x + 1, :] = one[:1]

    def split_step(depth_at, velocity):
        cosine = jnp.zeros(velocity.shape, jnp.float32)
        sine = jnp.zeros(velocity.shape, jnp.float32)
        for i in range(nvel):
            shift = slow_ref[depth_at, i] - waves[depth_at][i // per_group][0]
            angle = jnp.full((8, 128), frequency * shift * depth_step, jnp.float32)
            squared = angle * angle
            cosine_i = series(squared, 0, 9)[0:1, 0:1]
            sine_i = (angle * series(squared, 1, 9))[0:1, 0:1]
            cosine = jnp.where(velocity == i, cosine_i, cosine)
            sine = jnp.where(velocity == i, sine_i, sine)
        return cosine, sine

    along_last[...], across_last[...] = split_step(1, vel_last[...])
    for copy in handed:
        copy.wait_recv()
    for one in range(2):
        along_first[one], across_first[one] = split_step(0, vel_first[one])
    arrive()

    def part_of(which):
        return hart[which, 0], hart[which, 1]

    even_k, even_k_t, odd_k, odd_k_t = (part_of(which) for which in range(4))

    def from_modes_of(parts):
        return jnp.concatenate([parts[0], parts[1], parts[0]], 1)

    per_row = (ny // TB) // tiles
    tile_rows = nx // TB
    mode_rows = tile_rows // 2 * MODES
    mode_columns = ny // TB // 2 * MODES
    sums, differences = [], []
    for part in range(2):
        lines = [
            jnp.concatenate(
                [
                    jnp.concatenate(
                        [
                            coef_in[
                                tile_row * per_row + j,
                                part * outer : (part + 1) * outer,
                                a * width : (a + 1) * width,
                            ]
                            for a in range(MODES // outer)
                        ],
                        0,
                    )
                    for j in range(per_row)
                ],
                1,
            )
            for tile_row in range(tile_rows)
        ]
        upper = jnp.concatenate(lines[: tile_rows // 2], 0)
        lower = jnp.concatenate(lines[tile_rows // 2 :], 0)
        for one in (upper + lower, upper - lower):
            left, right = one[:, :mode_columns], one[:, mode_columns:]
            sums.append(left + right)
            differences.append(left - right)
    spread_y = [
        dot(from_modes_of(split2(jnp.concatenate(one, 0))), modes_y[parity])
        for parity, one in enumerate((sums, differences))
    ]
    seat_rows = pl.ds(pl.multiple_of(seat * rows, rows), rows)
    spans = []
    for parity in range(2):
        parts = []
        for p in range(2):
            at = (2 * p + parity) * mode_rows
            line = jnp.concatenate([one[at : at + mode_rows] for one in spread_y], 1)
            parts.append(split2(line))
        spans.append(parts)
    seats = []
    for which in (1, 3):
        own_high, own_low = hart[which, 0, seat_rows, :], hart[which, 1, seat_rows, :]
        seats.append((own_high, jnp.concatenate([own_high, own_low], 0)))
    wide = 128
    for first in range(0, ny, wide):
        lanes = slice(first, first + wide)
        made = [[None, None] for _ in range(REFS)]
        for parity in range(2):
            high = jnp.concatenate([one[0][:, lanes] for one in spans[parity]], 1)
            low = jnp.concatenate([one[1][:, lanes] for one in spans[parity]], 1)
            spectrum = dot(modes_x[parity], jnp.concatenate([high, high, low], 0))
            real, imag = spectrum[:, :wide], spectrum[:, wide:]
            own_high, both = seats[parity]
            part = slice(parity * half_x, (parity + 1) * half_x)
            for g in range(REFS):
                even, odd = wide_even[g, part, lanes], wide_odd[g, part, lanes]
                moved = split2(
                    jnp.concatenate([real * even - imag * odd, real * odd + imag * even], 1)
                )
                back = dot(both, moved[0])
                made[g][parity] = back[:rows] + (back[rows:] + dot(own_high, moved[1]))
        for g in range(REFS):
            for at, slab in enumerate((made[g][0] + made[g][1], made[g][0] - made[g][1])):
                for p in range(2):
                    slabs[at, 2 * g + p, :, lanes] = slab[:, p * wide : (p + 1) * wide]

    def inverse_y(x):
        u = dot3(split2(x[:, :half_y]), even_k)
        v = dot3(split2(x[:, half_y:]), odd_k)
        return jnp.concatenate([u + v, u - v], 1)

    def choose(made, velocity):
        real, imag = made[0]
        for g in range(1, REFS):
            chosen = velocity >= g * per_group
            real = jnp.where(chosen, made[g][0], real)
            imag = jnp.where(chosen, made[g][1], imag)
        return real, imag

    image_piece = ny // F

    def send_image(at, depth_at, first, real):
        part = slice(first, first + real.shape[0])
        for f in range(F):
            image_out[depth_at, f, part, :] = real[:, f * image_piece : (f + 1) * image_piece]
        copies = []
        for step in range(1, F):
            other = lax.rem(me_f + step, F)
            copies.append(
                pltpu.make_async_remote_copy(
                    src_ref=image_out.at[depth_at, other, part],
                    dst_ref=image_in.at[depth_at, me_f, part],
                    send_sem=image_sent.at[at, step],
                    recv_sem=image_got.at[at, step],
                    device_id={"freq": other},
                    device_id_type=MESH,
                )
            )
        for copy in copies:
            copy.start()
        image_in[depth_at, pl.ds(me_f, 1), part, :] = image_out[depth_at, pl.ds(me_f, 1), part, :]
        return copies

    def copies_of(at, c, out, into, sent, landed):
        copies = []
        for step in range(1, group):
            other = lax.rem(seat + step, group)
            copies.append(
                pltpu.make_async_remote_copy(
                    src_ref=out.at[at, c, other],
                    dst_ref=into.at[at, c, seat],
                    send_sem=sent.at[at, c, step],
                    recv_sem=landed.at[at, c, step],
                    device_id={"lat": side * group + other},
                    device_id_type=MESH,
                )
            )
        return copies

    def exchange(at, c, out, into, sent, landed):
        copies = copies_of(at, c, out, into, sent, landed)
        for copy in copies:
            copy.start()
        into[at, c, pl.ds(seat, 1)] = out[at, c, pl.ds(seat, 1)]
        return copies

    def first_rows(at, carry):
        field = inverse_y(slabs[at].reshape(2 * REFS * rows, ny))
        made = [
            (field[2 * g * rows : (2 * g + 1) * rows], field[(2 * g + 1) * rows : (2 * g + 2) * rows])
            for g in range(REFS)
        ]
        real, imag = choose(made, vel_first[at])
        cosine, sine = along_first[at], across_first[at]
        real, imag = real * cosine - imag * sine, real * sine + imag * cosine
        first_real[at] = real
        both = jnp.concatenate([real, imag], 0)
        left, right = both[:, :half_y], both[:, half_y:]
        line = jnp.concatenate(
            [dot3(split2(left + right), even_k_t), dot3(split2(left - right), odd_k_t)], 1
        )
        for c in range(CHUNKS):
            for dst in range(group):
                part = slice(dst * band + c * span, dst * band + (c + 1) * span)
                fwd_out[at, c, dst] = jnp.concatenate([line[:rows, part], line[rows:, part]], 1)
        exchange(at, 0, fwd_out, fwd_in, fwd_sent, fwd_got)
        return carry

    lax.fori_loop(0, 2, first_rows, 0)
    forward = [[copies_of(at, 0, fwd_out, fwd_in, fwd_sent, fwd_got) for at in range(2)]]
    for c in range(1, CHUNKS):
        forward.append([exchange(at, c, fwd_out, fwd_in, fwd_sent, fwd_got) for at in range(2)])
    forward = [sum(copies, []) for copies in forward]
    first_image = send_image(0, 0, 0, first_real[pl.ds(side, 1)].reshape(rows, ny))

    turn = (1 - 2 * side).astype(jnp.float32)
    half = rows // 2

    def apply(table, x):
        high, low = split2(x)
        made = dot(table[0], jnp.concatenate([high, low], 1))
        return made[:, :pair] + (made[:, pair:] + dot(table[1], high))

    backward = []
    for c in range(CHUNKS):
        for copy in forward[c]:
            copy.wait_recv()
        upper, lower = fwd_in[0, c].reshape(half_x, pair), fwd_in[1, c].reshape(half_x, pair)
        spectrum = []
        for one, table in ((upper + lower, even_k), (upper - lower, odd_k)):
            line = apply(table, one)
            spectrum.append((line, jnp.concatenate([line[:, span:], line[:, :span]], 1)))
        lines = []
        for g in range(REFS):
            sides = []
            for parity, table in enumerate((even_k_t, odd_k_t)):
                part = slice(parity * half_x, (parity + 1) * half_x)
                line, swapped = spectrum[parity]
                sides.append(
                    apply(table, line * band_even[c, g, part, :] + swapped * band_odd[c, g, part, :])
                )
            lines.append((sides[0] + turn * sides[1]).reshape(group, rows, pair))
        both = jnp.concatenate(lines, 2)
        for h in range(2):
            back_out[h, c] = both[:, h * half : (h + 1) * half]
            backward.append(exchange(h, c, back_out, back_in, back_sent, back_got))
    last_image = []
    for h in range(2):
        for c in range(CHUNKS):
            for copy in backward[2 * c + h]:
                copy.wait_recv()
        lines = []
        for at in range(2 * REFS):
            part = slice(at * span, (at + 1) * span)
            lines.append(
                jnp.concatenate(
                    [back_in[h, c, src, :, part] for src in range(group) for c in range(CHUNKS)], 1
                )
            )
        field = inverse_y(jnp.concatenate(lines, 0))
        made = [
            (field[2 * g * half : (2 * g + 1) * half], field[(2 * g + 1) * half : (2 * g + 2) * half])
            for g in range(REFS)
        ]
        own = slice(h * half, (h + 1) * half)
        real, imag = choose(made, vel_last[own, :])
        cosine, sine = along_last[own, :], across_last[own, :]
        moved = real * cosine - imag * sine
        last_image += send_image(1 + h, 1, h * half, moved)
        wave_ref[0, own, :] = moved
        wave_ref[1, own, :] = real * sine + imag * cosine

    leave_route()
    leave_coef()
    mirror.wait_send()
    for copy in handed:
        copy.wait_send()
    for copies in forward + backward:
        for copy in copies:
            copy.wait_send()
    for copy in first_image + last_image:
        copy.wait()


def finish(wave_ref, part_ref, wave_hbm, image_hbm, total, sem):
    store = pltpu.make_async_copy(wave_ref, wave_hbm.at[:, 0], sem.at[0])
    store.start()
    image = part_ref[:, 0]
    for f in range(1, part_ref.shape[1]):
        image = image + part_ref[:, f]
    total[...] = image
    last = pltpu.make_async_copy(total, image_hbm, sem.at[1])
    last.start()
    store.wait()
    last.wait()


def stay(x):
    return pltpu.with_memory_space_constraint(x, pltpu.HBM)


def local(spectra, tile_route, bin_in_tile, trace_offset, weights, frequency, slowness, vel_index):
    F = lax.axis_size("freq")
    L = lax.axis_size("lat")
    devices = F * L
    steps, rows, ny = vel_index.shape
    assert steps == 2
    nx = rows * L
    tiles = (nx // TB) * (ny // TB) // devices
    slots = tiles * CAP
    count = spectra.shape[2]
    data_rows = 2 * spectra.shape[1]
    padded = 2 * data_rows
    group = L // 2
    pair = 2 * (ny // group) // CHUNKS
    nvel = slowness.shape[1]
    cfg = (F, L, tiles, nx, ny, rows, data_rows, padded, nvel)

    hart = jnp.asarray(half_tables(nx))
    outer = TERMS * tiles // 128
    modes_x, modes_y = (jnp.asarray(one) for one in mode_tables(nx, MODES // outer))

    f32, bf16, i32 = jnp.float32, jnp.bfloat16, jnp.int32
    dma = pltpu.SemaphoreType.DMA
    wave, images = pl.pallas_call(
        functools.partial(program, cfg),
        out_shape=[
            jax.ShapeDtypeStruct((2, rows, ny), f32),
            jax.ShapeDtypeStruct((2, F, rows, ny // F), f32),
        ],
        in_specs=[HBM] * 5 + [SMEM] + [HBM] * 5,
        out_specs=[VMEM, VMEM],
        scratch_shapes=[
            pltpu.VMEM(spectra.shape, f32),
            pltpu.VMEM((1, count), i32),
            pltpu.VMEM((1, count), i32),
            pltpu.VMEM((2, count), f32),
            pltpu.VMEM((1, count), f32),
            pltpu.SMEM(slowness.shape, f32),
            pltpu.VMEM(hart.shape, bf16),
            pltpu.VMEM(modes_x.shape, bf16),
            pltpu.VMEM(modes_y.shape, bf16),
            pltpu.VMEM((2, rows, ny), i32),
            pltpu.VMEM((rows, ny), i32),
            pltpu.VMEM((devices, (data_rows + 4) // 2, 2 * slots), f32),
            pltpu.VMEM((devices, (data_rows + 4) // 2, 2 * slots), f32),
            pltpu.VMEM((F, 2 * outer, 128), f32),
            pltpu.VMEM((devices, 2 * outer, 128), f32),
            pltpu.VMEM((REFS, nx, ny), f32),
            pltpu.VMEM((REFS, nx, ny), f32),
            pltpu.VMEM((CHUNKS, REFS, nx, pair), f32),
            pltpu.VMEM((CHUNKS, REFS, nx, pair), f32),
            pltpu.VMEM((2, rows, ny), f32),
            pltpu.VMEM((2, rows, ny), f32),
            pltpu.VMEM((rows, ny), f32),
            pltpu.VMEM((rows, ny), f32),
            pltpu.VMEM((2, 2 * REFS, rows, ny), f32),
            pltpu.VMEM((2, rows, ny), f32),
            pltpu.VMEM((2, CHUNKS, group, rows, pair), f32),
            pltpu.VMEM((2, CHUNKS, group, rows, pair), f32),
            pltpu.VMEM((2, CHUNKS, group, rows // 2, REFS * pair), f32),
            pltpu.VMEM((2, CHUNKS, group, rows // 2, REFS * pair), f32),
            pltpu.VMEM((2, F, rows, ny // F), f32),
            dma((5,)),
            dma((6,)),
            dma((devices,)),
            dma((devices,)),
            dma((devices,)),
            dma((devices,)),
            dma((2 * F,)),
            dma((2, CHUNKS, group)),
            dma((2, CHUNKS, group)),
            dma((2, CHUNKS, group)),
            dma((2, CHUNKS, group)),
            dma((3, F)),
            dma((3, F)),
        ],
        compiler_params=pltpu.CompilerParams(
            collective_id=0, has_side_effects=True, vmem_limit_bytes=40 << 20
        ),
    )(
        *map(stay, (spectra, tile_route.reshape(1, count), bin_in_tile.reshape(1, count))),
        *map(stay, (trace_offset, weights.reshape(1, count))),
        frequency,
        stay(slowness),
        *map(stay, (vel_index, hart, modes_x, modes_y)),
    )
    return pl.pallas_call(
        finish,
        out_shape=[
            jax.ShapeDtypeStruct((2, 1, rows, ny), f32),
            jax.ShapeDtypeStruct((2, rows, ny // F), f32),
        ],
        in_specs=[VMEM, VMEM],
        out_specs=[HBM, HBM],
        scratch_shapes=[pltpu.VMEM((2, rows, ny // F), f32), dma((2,))],
        compiler_params=pltpu.CompilerParams(vmem_limit_bytes=8 << 20),
    )(wave, images)


def solution(mesh):
    return jax.shard_map(
        local,
        mesh=mesh,
        in_specs=(
            P(None, None, ("freq", "lat")),
            P(("freq", "lat"), None),
            P(("freq", "lat")),
            P(None, ("freq", "lat")),
            P(("freq", "lat")),
            P("freq"),
            P(),
            P(None, "lat", None),
        ),
        out_specs=(P(None, "freq", "lat", None), P(None, "lat", "freq")),
        check_vma=False,
    )
```

```python
import functools
import math

import jax
import jax.numpy as jnp
import numpy as np
from jax import lax
from jax.experimental import pallas as pl
from jax.experimental.pallas import tpu as pltpu
from jax.sharding import PartitionSpec as P

TB = 32
MODES = 8
CAP = 8
TERMS = MODES * MODES
REFS = 2
CHUNKS = 2

damping = 1.0
depth_step = 1.0

NN = (((1,), (0,)), ((), ()))
NT = (((1,), (1,)), ((), ()))
VMEM = pl.BlockSpec(memory_space=pltpu.VMEM)
SMEM = pl.BlockSpec(memory_space=pltpu.SMEM)
HBM = pl.BlockSpec(memory_space=pltpu.HBM)
MESH = pl.DeviceIdType.MESH


def two_parts(exact):
    high = exact.astype(jnp.bfloat16)
    low = (exact - high.astype(np.float64)).astype(jnp.bfloat16)
    return high, low


def hartley(length):
    at = np.arange(length)
    angle = 2.0 * math.pi / length * (at[:, None] * at[None, :] % length)
    return (np.cos(angle) + np.sin(angle)) / math.sqrt(length)


def orders(length):
    at = np.arange(length // 4)
    even = np.concatenate([2 * at, (length - 2 * at) % length])
    even[length // 4] = length // 2
    return even, np.concatenate([2 * at + 1, length - 1 - 2 * at])


def half_tables(length):
    whole = hartley(length)[:, : length // 2]
    even, odd = (whole[order] for order in orders(length))
    return np.stack([np.stack(two_parts(one), 0) for one in (even, even.T, odd, odd.T)], 0)


def mode_tables(length, inner):
    cosines = np.cos(math.pi * np.arange(MODES)[:, None] * (np.arange(TB)[None, :] + 0.5) / TB)
    count = length // TB // 2
    fold = np.zeros((count, MODES, length))
    for tile in range(count):
        fold[tile, :, tile * TB : (tile + 1) * TB] = cosines
    whole = fold @ hartley(length)
    turned = whole.reshape(count, MODES // inner, inner, length).swapaxes(1, 2)
    left, right = [], []
    for order in orders(length):
        high, low = two_parts(whole.reshape(count * MODES, length)[:, order])
        right.append(np.concatenate([high, high, low], 0))
        high, low = two_parts(turned.reshape(count * MODES, length)[:, order])
        left.append(np.concatenate([high.T, low.T, high.T], 1))
    return np.stack(left, 0), np.stack(right, 0)


def split2(x):
    high = x.astype(jnp.bfloat16)
    return high, (x - high.astype(jnp.float32)).astype(jnp.bfloat16)


def dot(a, b, dims=NN):
    return lax.dot_general(a, b, dims, preferred_element_type=jnp.float32)


def dot3(a, b, dims=NN):
    return dot(a[0], b[0], dims) + (dot(a[0], b[1], dims) + dot(a[1], b[0], dims))


def series(value, first, count):
    total = jnp.full(value.shape, 1.0 / math.factorial(2 * (count - 1) + first), jnp.float32)
    for n in range(count - 2, -1, -1):
        total = 1.0 / math.factorial(2 * n + first) - value * total
    return total


def cosine_of(cell):
    angle = (0.5 * TB - (cell + 0.5)) * (math.pi / TB)
    return angle * series(angle * angle, 1, 9)


def propagator(wave_squared, kx, ky):
    vertical = wave_squared - kx * kx - ky * ky
    root = jnp.sqrt(jnp.abs(vertical)) * depth_step
    squared = root * root
    moving = vertical > 0.0
    even = jnp.where(moving, series(squared, 0, 10), jnp.exp(-root))
    odd = jnp.where(moving, root * series(squared, 1, 10), 0.0)
    return even, odd


def wave_number(place, length):
    half, quarter = length // 2, length // 4
    index = 2 * lax.rem(place, quarter) + lax.div(place, half)
    index = jnp.where(place == quarter, half, index)
    return 2.0 * math.pi / length * index.astype(jnp.float32)


def take_lanes(x, index):
    return jnp.take_along_axis(x, index, axis=1, mode="promise_in_bounds")


def iota(shape, axis):
    return lax.broadcasted_iota(jnp.int32, shape, axis)


def program(
    cfg,
    spectra_hbm,
    tile_hbm,
    bin_hbm,
    offset_hbm,
    weight_hbm,
    freq_ref,
    slow_hbm,
    vel_hbm,
    hart_hbm,
    modes_x_hbm,
    modes_y_hbm,
    wave_ref,
    image_in,
    spectra_ref,
    tile_ref,
    bin_ref,
    offset_ref,
    weight_ref,
    slow_ref,
    hart,
    modes_x,
    modes_y,
    vel_first,
    vel_last,
    route_out,
    route_in,
    coef_out,
    coef_in,
    wide_even,
    wide_odd,
    band_even,
    band_odd,
    along_first,
    across_first,
    along_last,
    across_last,
    slabs,
    first_real,
    fwd_out,
    fwd_in,
    back_out,
    back_in,
    image_out,
    trace_sem,
    table_sem,
    route_sent,
    route_got,
    coef_sent,
    coef_got,
    vel_sem,
    fwd_sent,
    fwd_got,
    back_sent,
    back_got,
    image_sent,
    image_got,
):
    F, L, tiles, nx, ny, rows, data_rows, padded, nvel = cfg
    devices = F * L
    group = L // 2
    half_x, half_y = nx // 2, ny // 2
    band = ny // group
    span = band // CHUNKS
    pair = 2 * span
    slots = tiles * CAP
    per_group = nvel // REFS
    me_f = lax.axis_index("freq")
    me_l = lax.axis_index("lat")
    me = me_l * F + me_f
    side = lax.div(me_l, group)
    seat = lax.rem(me_l, group)

    barrier = pltpu.get_barrier_semaphore()

    def partner_of(at):
        other = lax.rem(me + at, devices)
        return other, {"freq": lax.rem(other, F), "lat": lax.div(other, F)}

    def greet(at, carry):
        _, device = partner_of(at)
        pl.semaphore_signal(barrier, inc=1, device_id=device, device_id_type=MESH)
        return carry

    inputs = [
        pltpu.make_async_copy(src, dst, trace_sem.at[at])
        for at, (src, dst) in enumerate(
            [
                (tile_hbm, tile_ref),
                (bin_hbm, bin_ref),
                (offset_hbm, offset_ref),
                (weight_hbm, weight_ref),
                (spectra_hbm, spectra_ref),
            ]
        )
    ]
    for load in inputs:
        load.start()
    lax.fori_loop(1, devices, greet, 0)
    loads = [
        pltpu.make_async_copy(src, dst, table_sem.at[at])
        for at, (src, dst) in enumerate(
            [
                (vel_hbm.at[0], vel_first.at[side]),
                (vel_hbm.at[1], vel_last),
                (modes_x_hbm, modes_x),
                (modes_y_hbm, modes_y),
                (hart_hbm, hart),
                (slow_hbm, slow_ref),
            ]
        )
    ]
    for load in loads:
        load.start()
    for load in inputs:
        load.wait()

    count = tile_ref.shape[1]
    width = 128
    tile = tile_ref[...]
    columns = [
        jnp.transpose(jnp.broadcast_to(tile[:, at : at + width], (width, width)))
        for at in range(0, count, width)
    ]
    earlier = iota((width, width), 0) < iota((width, width), 1)
    ranks = []
    for at in range(count // width):
        row = jnp.broadcast_to(tile[:, at * width : (at + 1) * width], (width, width))
        same = jnp.where((columns[at] == row) & earlier, 1, 0)
        for before in range(at):
            same = same + jnp.where(columns[before] == row, 1, 0)
        ranks.append(jnp.sum(same, 0, keepdims=True))
    rank = jnp.concatenate(ranks, 1)
    turned = lax.rem(lax.rem(tile, tiles) + me, tiles)
    slot = lax.div(tile, tiles) * slots + turned * CAP + rank

    cell = bin_ref[...]
    root_weight = jnp.sqrt(weight_ref[...])
    cell_x = lax.div(cell, TB).astype(jnp.float32) + offset_ref[0:1, :]
    cell_y = lax.rem(cell, TB).astype(jnp.float32) + offset_ref[1:2, :]
    feats = jnp.concatenate(
        [spectra_ref[0] * root_weight, spectra_ref[1] * root_weight]
        + [root_weight, cosine_of(cell_x), cosine_of(cell_y)]
        + [jnp.zeros((padded - data_rows - 3, count), jnp.float32)],
        0,
    )
    high = feats.astype(jnp.bfloat16)
    rest = feats - high.astype(jnp.float32)
    middle = rest.astype(jnp.bfloat16)
    low = (rest - middle.astype(jnp.float32)).astype(jnp.bfloat16)
    parts = jnp.concatenate([high, middle, low], 0)
    fold = (data_rows + 4) // 2
    wide = 256
    places = iota((wide, count), 0).astype(jnp.float32).astype(jnp.bfloat16)
    one, none = jnp.ones((), jnp.bfloat16), jnp.zeros((), jnp.bfloat16)
    for at in range(0, devices * slots, wide):
        within = jnp.where((slot >= at) & (slot < at + wide), slot - at, wide)
        within = within.astype(jnp.float32).astype(jnp.bfloat16)
        chosen = jnp.where(places == within, one, none)
        got = dot(parts, chosen, NT)
        got = got[:padded] + got[padded : 2 * padded] + got[2 * padded :]
        for piece in range(wide // slots):
            block = got[:, piece * slots : (piece + 1) * slots]
            route_out[at // slots + piece] = jnp.concatenate([block[:fold], block[fold : 2 * fold]], 1)

    pl.semaphore_wait(barrier, devices - 1)

    def spread(out, into, sent, landed):
        def copy_of(at):
            other, device = partner_of(at)
            return pltpu.make_async_remote_copy(
                src_ref=out.at[other] if out.shape[0] == devices else out.at[lax.rem(other, F)],
                dst_ref=into.at[me],
                send_sem=sent.at[at],
                recv_sem=landed.at[at],
                device_id=device,
                device_id_type=MESH,
            )

        def start(at, carry):
            copy_of(at).start()
            return carry

        def arrive(at, carry):
            copy_of(at).wait_recv()
            return carry

        def leave(at, carry):
            copy_of(at).wait_send()
            return carry

        lax.fori_loop(1, devices, start, 0)
        return (
            lambda: lax.fori_loop(1, devices, arrive, 0),
            lambda: lax.fori_loop(1, devices, leave, 0),
        )

    arrive, leave_route = spread(route_out, route_in, route_sent, route_got)
    route_in[pl.ds(me, 1)] = route_out[pl.ds(me, 1)]

    for load in loads:
        load.wait()
    frequency = freq_ref[0]
    waves = []
    for depth_at in range(2):
        squares = []
        for g in range(REFS):
            total = slow_ref[depth_at, g * per_group]
            for i in range(1, per_group):
                total = total + slow_ref[depth_at, g * per_group + i]
            reference = total * (1.0 / per_group)
            squares.append((reference, (frequency * reference) * (frequency * reference)))
        waves.append(squares)

    chunk = 16
    quarter_x, quarter_y = nx // 4, ny // 4
    lane = iota((chunk, quarter_y), 1)
    first_ky = [wave_number(lane + parity * half_y, ny) for parity in range(2)]
    middle_ky = jnp.full((chunk, quarter_y), math.pi, jnp.float32)

    def wide_rows(g, kx):
        made = [propagator(waves[0][g][1], kx, ky) for ky in (*first_ky, middle_ky)]
        return [
            jnp.concatenate([even, jnp.where(lane == 0, middle, even), odd, odd], 1)
            for even, odd, middle in zip(*made)
        ]

    def wide_tables(at, carry):
        first = pl.multiple_of(lax.rem(at, quarter_x // chunk) * chunk, chunk)
        base = pl.multiple_of(lax.div(at, quarter_x // chunk) * half_x, half_x)
        kx = wave_number(iota((chunk, quarter_y), 0) + (first + base), nx)
        for g in range(REFS):
            for one, table in zip(wide_rows(g, kx), (wide_even, wide_odd)):
                for copy in range(2):
                    table[g, pl.ds(base + copy * quarter_x + first, chunk), :] = one
        return carry

    lax.fori_loop(0, half_x // chunk, wide_tables, 0)
    middle_kx = jnp.full((chunk, quarter_y), math.pi, jnp.float32)
    for g in range(REFS):
        for one, table in zip(wide_rows(g, middle_kx), (wide_even, wide_odd)):
            table[g, quarter_x : quarter_x + 1, :] = one[:1]
    arrive()

    parts = F if rows % (8 * F) == 0 else 1
    part_rows = rows // parts
    own_part = pl.ds(pl.multiple_of((me_f if parts > 1 else 0) * part_rows, part_rows), part_rows)
    mirror = pltpu.make_async_remote_copy(
        src_ref=vel_first.at[side, own_part],
        dst_ref=vel_first.at[side, own_part],
        send_sem=vel_sem.at[0],
        recv_sem=vel_sem.at[1],
        device_id={"lat": lax.rem(me_l + group, L)},
        device_id_type=MESH,
    )
    mirror.start()

    group_at = lax.div(lax.rem(iota((fold, 2 * slots), 1), slots), CAP)
    eye = jnp.where(iota((TERMS + data_rows, TERMS), 0) == iota((TERMS + data_rows, TERMS), 1), damping, 0.0)

    def chebyshev(cosine):
        terms = [jnp.ones_like(cosine), cosine]
        for _ in range(MODES - 2):
            terms.append(2.0 * cosine * terms[-1] - terms[-2])
        return terms

    normals = []
    for t in range(tiles):
        pieces = []
        for first in range(0, devices, tiles):
            picked = route_in[first]
            for i in range(1, tiles):
                picked = jnp.where(group_at == (t + i) % tiles, route_in[first + i], picked)
            pieces.append(picked)
        data = jnp.concatenate([piece[:, :slots] for piece in pieces], 1)
        place = jnp.concatenate([piece[:, slots:] for piece in pieces], 1)
        data = jnp.concatenate([data, place[: data_rows - fold]], 0)
        place = place[data_rows - fold :]
        scale = place[0:1]
        along_x = chebyshev(place[1:2])
        along_y = jnp.concatenate(chebyshev(place[2:3]), 0)
        basis = jnp.concatenate([(term * scale) * along_y for term in along_x], 0)
        right = jnp.concatenate([basis, data], 0)
        normals.append(
            eye
            + lax.dot_general(
                right, basis, NT, preferred_element_type=jnp.float32, precision=lax.Precision.HIGHEST
            )
        )
    inner = 128 // tiles
    outer = TERMS // inner
    lines = (TERMS + data_rows) // 8
    rest = []
    for at in range(outer):
        line = jnp.concatenate([one[:, at * inner : (at + 1) * inner] for one in normals], 1)
        rest.append([line[8 * j : 8 * (j + 1)] for j in range(lines)])
    lane = iota((8, 128), 1)
    within = lax.rem(lane, inner)
    for block in range(TERMS // 8):
        todo = range(block, lines)
        pivots = []
        for s in range(8):
            at, own = (8 * block + s) // inner, (8 * block + s) % inner
            pick = lane - within + own
            pivots.append({j: take_lanes(rest[at][j], pick) for j in todo})
        for s in range(8):
            at, own = (8 * block + s) // inner, (8 * block + s) % inner
            scale = 1.0 / pivots[s][block][s : s + 1]
            scaled = {j: pivots[s][j] * scale for j in todo}
            for later in range(s + 1, 8):
                factor = pivots[later][block][s : s + 1]
                pivots[later] = {j: pivots[later][j] - factor * scaled[j] for j in todo}
            for one in range(outer):
                factor = rest[one][block][s : s + 1]
                for j in todo:
                    value = rest[one][j] - factor * scaled[j]
                    rest[one][j] = jnp.where(within == own, scaled[j], value) if one == at else value
    width = tiles * MODES
    place = lax.rem(lane, width)
    pick = lax.div(place, MODES) * inner + lax.div(lane, width) * MODES + lax.rem(place, MODES)
    for one in range(outer):
        for j in range(TERMS // 8, lines):
            line = take_lanes(rest[one][j], pick)
            for s in range(8):
                part, f = divmod(8 * (j - TERMS // 8) + s, F)
                coef_out[f, part * outer + one : part * outer + one + 1, :] = line[s : s + 1]

    arrive, leave_coef = spread(coef_out, coef_in, coef_sent, coef_got)
    coef_in[pl.ds(me, 1)] = coef_out[pl.ds(me_f, 1)]

    mirror.wait_recv()
    handed = []
    for step in range(1, parts):
        other = lax.rem(me_f + step, F)
        handed.append(
            pltpu.make_async_remote_copy(
                src_ref=vel_first.at[1 - side, own_part],
                dst_ref=vel_first.at[1 - side, own_part],
                send_sem=vel_sem.at[2 * step],
                recv_sem=vel_sem.at[2 * step + 1],
                device_id={"freq": other},
                device_id_type=MESH,
            )
        )
    for copy in handed:
        copy.start()

    pair_lane = iota((chunk, pair), 1)
    sign = jnp.where(pair_lane < span, -1.0, 1.0)
    band_ky = [
        wave_number(seat * band + c * span + lax.rem(pair_lane, span), ny) for c in range(CHUNKS)
    ]

    def band_rows(c, g, kx):
        even, odd = propagator(waves[1][g][1], kx, band_ky[c])
        return (even, band_even), (odd * sign, band_odd)

    def band_tables(at, carry):
        first = pl.multiple_of(lax.rem(at, quarter_x // chunk) * chunk, chunk)
        base = pl.multiple_of(lax.div(at, quarter_x // chunk) * half_x, half_x)
        kx = wave_number(iota((chunk, pair), 0) + (first + base), nx)
        for c in range(CHUNKS):
            for g in range(REFS):
                for one, table in band_rows(c, g, kx):
                    for copy in range(2):
                        table[c, g, pl.ds(base + copy * quarter_x + first, chunk), :] = one
        return carry

    lax.fori_loop(0, half_x // chunk, band_tables, 0)
    for c in range(CHUNKS):
        for g in range(REFS):
            for one, table in band_rows(c, g, jnp.full((chunk, pair), math.pi, jnp.float32)):
                table[c, g, quarter_x : quarter_x + 1, :] = one[:1]

    def split_step(depth_at, velocity):
        cosine = jnp.zeros(velocity.shape, jnp.float32)
        sine = jnp.zeros(velocity.shape, jnp.float32)
        for i in range(nvel):
            shift = slow_ref[depth_at, i] - waves[depth_at][i // per_group][0]
            angle = jnp.full((8, 128), frequency * shift * depth_step, jnp.float32)
            squared = angle * angle
            cosine_i = series(squared, 0, 9)[0:1, 0:1]
            sine_i = (angle * series(squared, 1, 9))[0:1, 0:1]
            cosine = jnp.where(velocity == i, cosine_i, cosine)
            sine = jnp.where(velocity == i, sine_i, sine)
        return cosine, sine

    along_last[...], across_last[...] = split_step(1, vel_last[...])
    for copy in handed:
        copy.wait_recv()
    for one in range(2):
        along_first[one], across_first[one] = split_step(0, vel_first[one])
    arrive()

    def part_of(which):
        return hart[which, 0], hart[which, 1]

    even_k, even_k_t, odd_k, odd_k_t = (part_of(which) for which in range(4))

    def from_modes_of(parts):
        return jnp.concatenate([parts[0], parts[1], parts[0]], 1)

    per_row = (ny // TB) // tiles
    tile_rows = nx // TB
    mode_rows = tile_rows // 2 * MODES
    mode_columns = ny // TB // 2 * MODES
    sums, differences = [], []
    for part in range(2):
        lines = [
            jnp.concatenate(
                [
                    jnp.concatenate(
                        [
                            coef_in[
                                tile_row * per_row + j,
                                part * outer : (part + 1) * outer,
                                a * width : (a + 1) * width,
                            ]
                            for a in range(MODES // outer)
                        ],
                        0,
                    )
                    for j in range(per_row)
                ],
                1,
            )
            for tile_row in range(tile_rows)
        ]
        upper = jnp.concatenate(lines[: tile_rows // 2], 0)
        lower = jnp.concatenate(lines[tile_rows // 2 :], 0)
        for one in (upper + lower, upper - lower):
            left, right = one[:, :mode_columns], one[:, mode_columns:]
            sums.append(left + right)
            differences.append(left - right)
    spread_y = [
        dot(from_modes_of(split2(jnp.concatenate(one, 0))), modes_y[parity])
        for parity, one in enumerate((sums, differences))
    ]
    seat_rows = pl.ds(pl.multiple_of(seat * rows, rows), rows)
    spans = []
    for parity in range(2):
        parts = []
        for p in range(2):
            at = (2 * p + parity) * mode_rows
            line = jnp.concatenate([one[at : at + mode_rows] for one in spread_y], 1)
            parts.append(split2(line))
        spans.append(parts)
    seats = []
    for which in (1, 3):
        own_high, own_low = hart[which, 0, seat_rows, :], hart[which, 1, seat_rows, :]
        seats.append((own_high, jnp.concatenate([own_high, own_low], 0)))
    wide = 256
    for first in range(0, ny, wide):
        lanes = slice(first, first + wide)
        made = [[None, None] for _ in range(REFS)]
        for parity in range(2):
            high = jnp.concatenate([one[0][:, lanes] for one in spans[parity]], 1)
            low = jnp.concatenate([one[1][:, lanes] for one in spans[parity]], 1)
            spectrum = dot(modes_x[parity], jnp.concatenate([high, high, low], 0))
            real, imag = spectrum[:, :wide], spectrum[:, wide:]
            own_high, both = seats[parity]
            part = slice(parity * half_x, (parity + 1) * half_x)
            for g in range(REFS):
                even, odd = wide_even[g, part, lanes], wide_odd[g, part, lanes]
                moved = split2(
                    jnp.concatenate([real * even - imag * odd, real * odd + imag * even], 1)
                )
                back = dot(both, moved[0])
                made[g][parity] = back[:rows] + (back[rows:] + dot(own_high, moved[1]))
        for g in range(REFS):
            for at, slab in enumerate((made[g][0] + made[g][1], made[g][0] - made[g][1])):
                for p in range(2):
                    slabs[at, 2 * g + p, :, lanes] = slab[:, p * wide : (p + 1) * wide]

    def inverse_y(x):
        u = dot3(split2(x[:, :half_y]), even_k)
        v = dot3(split2(x[:, half_y:]), odd_k)
        return jnp.concatenate([u + v, u - v], 1)

    def choose(made, velocity):
        real, imag = made[0]
        for g in range(1, REFS):
            chosen = velocity >= g * per_group
            real = jnp.where(chosen, made[g][0], real)
            imag = jnp.where(chosen, made[g][1], imag)
        return real, imag

    image_piece = ny // F

    def send_image(at, depth_at, first, real):
        part = slice(first, first + real.shape[0])
        for f in range(F):
            image_out[depth_at, f, part, :] = real[:, f * image_piece : (f + 1) * image_piece]
        copies = []
        for step in range(1, F):
            other = lax.rem(me_f + step, F)
            copies.append(
                pltpu.make_async_remote_copy(
                    src_ref=image_out.at[depth_at, other, part],
                    dst_ref=image_in.at[depth_at, me_f, part],
                    send_sem=image_sent.at[at, step],
                    recv_sem=image_got.at[at, step],
                    device_id={"freq": other},
                    device_id_type=MESH,
                )
            )
        for copy in copies:
            copy.start()
        image_in[depth_at, pl.ds(me_f, 1), part, :] = image_out[depth_at, pl.ds(me_f, 1), part, :]
        return copies

    def copies_of(at, c, out, into, sent, landed):
        copies = []
        for step in range(1, group):
            other = lax.rem(seat + step, group)
            copies.append(
                pltpu.make_async_remote_copy(
                    src_ref=out.at[at, c, other],
                    dst_ref=into.at[at, c, seat],
                    send_sem=sent.at[at, c, step],
                    recv_sem=landed.at[at, c, step],
                    device_id={"lat": side * group + other},
                    device_id_type=MESH,
                )
            )
        return copies

    def exchange(at, c, out, into, sent, landed):
        copies = copies_of(at, c, out, into, sent, landed)
        for copy in copies:
            copy.start()
        into[at, c, pl.ds(seat, 1)] = out[at, c, pl.ds(seat, 1)]
        return copies

    def first_rows(at, carry):
        field = inverse_y(slabs[at].reshape(2 * REFS * rows, ny))
        made = [
            (field[2 * g * rows : (2 * g + 1) * rows], field[(2 * g + 1) * rows : (2 * g + 2) * rows])
            for g in range(REFS)
        ]
        real, imag = choose(made, vel_first[at])
        cosine, sine = along_first[at], across_first[at]
        real, imag = real * cosine - imag * sine, real * sine + imag * cosine
        first_real[at] = real
        both = jnp.concatenate([real, imag], 0)
        left, right = both[:, :half_y], both[:, half_y:]
        line = jnp.concatenate(
            [dot3(split2(left + right), even_k_t), dot3(split2(left - right), odd_k_t)], 1
        )
        for c in range(CHUNKS):
            for dst in range(group):
                part = slice(dst * band + c * span, dst * band + (c + 1) * span)
                fwd_out[at, c, dst] = jnp.concatenate([line[:rows, part], line[rows:, part]], 1)
        exchange(at, 0, fwd_out, fwd_in, fwd_sent, fwd_got)
        return carry

    lax.fori_loop(0, 2, first_rows, 0)
    forward = [[copies_of(at, 0, fwd_out, fwd_in, fwd_sent, fwd_got) for at in range(2)]]
    for c in range(1, CHUNKS):
        forward.append([exchange(at, c, fwd_out, fwd_in, fwd_sent, fwd_got) for at in range(2)])
    forward = [sum(copies, []) for copies in forward]
    first_image = send_image(0, 0, 0, first_real[pl.ds(side, 1)].reshape(rows, ny))

    turn = (1 - 2 * side).astype(jnp.float32)
    half = rows // 2

    def apply(table, x):
        high, low = split2(x)
        made = dot(table[0], jnp.concatenate([high, low], 1))
        return made[:, :pair] + (made[:, pair:] + dot(table[1], high))

    backward = []
    for c in range(CHUNKS):
        for copy in forward[c]:
            copy.wait_recv()
        upper, lower = fwd_in[0, c].reshape(half_x, pair), fwd_in[1, c].reshape(half_x, pair)
        spectrum = []
        for one, table in ((upper + lower, even_k), (upper - lower, odd_k)):
            line = apply(table, one)
            spectrum.append((line, jnp.concatenate([line[:, span:], line[:, :span]], 1)))
        lines = []
        for g in range(REFS):
            sides = []
            for parity, table in enumerate((even_k_t, odd_k_t)):
                part = slice(parity * half_x, (parity + 1) * half_x)
                line, swapped = spectrum[parity]
                sides.append(
                    apply(table, line * band_even[c, g, part, :] + swapped * band_odd[c, g, part, :])
                )
            lines.append((sides[0] + turn * sides[1]).reshape(group, rows, pair))
        both = jnp.concatenate(lines, 2)
        for h in range(2):
            back_out[h, c] = both[:, h * half : (h + 1) * half]
            backward.append(exchange(h, c, back_out, back_in, back_sent, back_got))
    last_image = []
    for h in range(2):
        for c in range(CHUNKS):
            for copy in backward[2 * c + h]:
                copy.wait_recv()
        lines = []
        for at in range(2 * REFS):
            part = slice(at * span, (at + 1) * span)
            lines.append(
                jnp.concatenate(
                    [back_in[h, c, src, :, part] for src in range(group) for c in range(CHUNKS)], 1
                )
            )
        field = inverse_y(jnp.concatenate(lines, 0))
        made = [
            (field[2 * g * half : (2 * g + 1) * half], field[(2 * g + 1) * half : (2 * g + 2) * half])
            for g in range(REFS)
        ]
        own = slice(h * half, (h + 1) * half)
        real, imag = choose(made, vel_last[own, :])
        cosine, sine = along_last[own, :], across_last[own, :]
        moved = real * cosine - imag * sine
        last_image += send_image(1 + h, 1, h * half, moved)
        wave_ref[0, own, :] = moved
        wave_ref[1, own, :] = real * sine + imag * cosine

    leave_route()
    leave_coef()
    mirror.wait_send()
    for copy in handed:
        copy.wait_send()
    for copies in forward + backward:
        for copy in copies:
            copy.wait_send()
    for copy in first_image + last_image:
        copy.wait()


def finish(wave_ref, part_ref, wave_hbm, image_hbm, total, sem):
    store = pltpu.make_async_copy(wave_ref, wave_hbm.at[:, 0], sem.at[0])
    store.start()
    image = part_ref[:, 0]
    for f in range(1, part_ref.shape[1]):
        image = image + part_ref[:, f]
    total[...] = image
    last = pltpu.make_async_copy(total, image_hbm, sem.at[1])
    last.start()
    store.wait()
    last.wait()


def stay(x):
    return pltpu.with_memory_space_constraint(x, pltpu.HBM)


def local(spectra, tile_route, bin_in_tile, trace_offset, weights, frequency, slowness, vel_index):
    F = lax.axis_size("freq")
    L = lax.axis_size("lat")
    devices = F * L
    steps, rows, ny = vel_index.shape
    assert steps == 2
    nx = rows * L
    tiles = (nx // TB) * (ny // TB) // devices
    slots = tiles * CAP
    count = spectra.shape[2]
    data_rows = 2 * spectra.shape[1]
    padded = 2 * data_rows
    group = L // 2
    pair = 2 * (ny // group) // CHUNKS
    nvel = slowness.shape[1]
    cfg = (F, L, tiles, nx, ny, rows, data_rows, padded, nvel)

    hart = jnp.asarray(half_tables(nx))
    outer = TERMS * tiles // 128
    modes_x, modes_y = (jnp.asarray(one) for one in mode_tables(nx, MODES // outer))

    f32, bf16, i32 = jnp.float32, jnp.bfloat16, jnp.int32
    dma = pltpu.SemaphoreType.DMA
    wave, images = pl.pallas_call(
        functools.partial(program, cfg),
        out_shape=[
            jax.ShapeDtypeStruct((2, rows, ny), f32),
            jax.ShapeDtypeStruct((2, F, rows, ny // F), f32),
        ],
        in_specs=[HBM] * 5 + [SMEM] + [HBM] * 5,
        out_specs=[VMEM, VMEM],
        scratch_shapes=[
            pltpu.VMEM(spectra.shape, f32),
            pltpu.VMEM((1, count), i32),
            pltpu.VMEM((1, count), i32),
            pltpu.VMEM((2, count), f32),
            pltpu.VMEM((1, count), f32),
            pltpu.SMEM(slowness.shape, f32),
            pltpu.VMEM(hart.shape, bf16),
            pltpu.VMEM(modes_x.shape, bf16),
            pltpu.VMEM(modes_y.shape, bf16),
            pltpu.VMEM((2, rows, ny), i32),
            pltpu.VMEM((rows, ny), i32),
            pltpu.VMEM((devices, (data_rows + 4) // 2, 2 * slots), f32),
            pltpu.VMEM((devices, (data_rows + 4) // 2, 2 * slots), f32),
            pltpu.VMEM((F, 2 * outer, 128), f32),
            pltpu.VMEM((devices, 2 * outer, 128), f32),
            pltpu.VMEM((REFS, nx, ny), f32),
            pltpu.VMEM((REFS, nx, ny), f32),
            pltpu.VMEM((CHUNKS, REFS, nx, pair), f32),
            pltpu.VMEM((CHUNKS, REFS, nx, pair), f32),
            pltpu.VMEM((2, rows, ny), f32),
            pltpu.VMEM((2, rows, ny), f32),
            pltpu.VMEM((rows, ny), f32),
            pltpu.VMEM((rows, ny), f32),
            pltpu.VMEM((2, 2 * REFS, rows, ny), f32),
            pltpu.VMEM((2, rows, ny), f32),
            pltpu.VMEM((2, CHUNKS, group, rows, pair), f32),
            pltpu.VMEM((2, CHUNKS, group, rows, pair), f32),
            pltpu.VMEM((2, CHUNKS, group, rows // 2, REFS * pair), f32),
            pltpu.VMEM((2, CHUNKS, group, rows // 2, REFS * pair), f32),
            pltpu.VMEM((2, F, rows, ny // F), f32),
            dma((5,)),
            dma((6,)),
            dma((devices,)),
            dma((devices,)),
            dma((devices,)),
            dma((devices,)),
            dma((2 * F,)),
            dma((2, CHUNKS, group)),
            dma((2, CHUNKS, group)),
            dma((2, CHUNKS, group)),
            dma((2, CHUNKS, group)),
            dma((3, F)),
            dma((3, F)),
        ],
        compiler_params=pltpu.CompilerParams(
            collective_id=0, has_side_effects=True, vmem_limit_bytes=40 << 20
        ),
    )(
        *map(stay, (spectra, tile_route.reshape(1, count), bin_in_tile.reshape(1, count))),
        *map(stay, (trace_offset, weights.reshape(1, count))),
        frequency,
        stay(slowness),
        *map(stay, (vel_index, hart, modes_x, modes_y)),
    )
    return pl.pallas_call(
        finish,
        out_shape=[
            jax.ShapeDtypeStruct((2, 1, rows, ny), f32),
            jax.ShapeDtypeStruct((2, rows, ny // F), f32),
        ],
        in_specs=[VMEM, VMEM],
        out_specs=[HBM, HBM],
        scratch_shapes=[pltpu.VMEM((2, rows, ny // F), f32), dma((2,))],
        compiler_params=pltpu.CompilerParams(vmem_limit_bytes=8 << 20),
    )(wave, images)


def solution(mesh):
    return jax.shard_map(
        local,
        mesh=mesh,
        in_specs=(
            P(None, None, ("freq", "lat")),
            P(("freq", "lat"), None),
            P(("freq", "lat")),
            P(None, ("freq", "lat")),
            P(("freq", "lat")),
            P("freq"),
            P(),
            P(None, "lat", None),
        ),
        out_specs=(P(None, "freq", "lat", None), P(None, "lat", "freq")),
        check_vma=False,
    )
```

```python
import functools
import math

import jax
import jax.numpy as jnp
import numpy as np
from jax import lax
from jax.experimental import pallas as pl
from jax.experimental.pallas import tpu as pltpu
from jax.sharding import PartitionSpec as P

TB = 32
MODES = 8
CAP = 8
TERMS = MODES * MODES
REFS = 2
CHUNKS = 2

damping = 1.0
depth_step = 1.0

NN = (((1,), (0,)), ((), ()))
NT = (((1,), (1,)), ((), ()))
VMEM = pl.BlockSpec(memory_space=pltpu.VMEM)
SMEM = pl.BlockSpec(memory_space=pltpu.SMEM)
HBM = pl.BlockSpec(memory_space=pltpu.HBM)
MESH = pl.DeviceIdType.MESH


def two_parts(exact):
    high = exact.astype(jnp.bfloat16)
    low = (exact - high.astype(np.float64)).astype(jnp.bfloat16)
    return high, low


def hartley(length):
    at = np.arange(length)
    angle = 2.0 * math.pi / length * (at[:, None] * at[None, :] % length)
    return (np.cos(angle) + np.sin(angle)) / math.sqrt(length)


def orders(length):
    at = np.arange(length // 4)
    even = np.concatenate([2 * at, (length - 2 * at) % length])
    even[length // 4] = length // 2
    return even, np.concatenate([2 * at + 1, length - 1 - 2 * at])


def half_tables(length):
    whole = hartley(length)[:, : length // 2]
    even, odd = (whole[order] for order in orders(length))
    return np.stack([np.stack(two_parts(one), 0) for one in (even, even.T, odd, odd.T)], 0)


def mode_tables(length, inner):
    cosines = np.cos(math.pi * np.arange(MODES)[:, None] * (np.arange(TB)[None, :] + 0.5) / TB)
    count = length // TB // 2
    fold = np.zeros((count, MODES, length))
    for tile in range(count):
        fold[tile, :, tile * TB : (tile + 1) * TB] = cosines
    whole = fold @ hartley(length)
    turned = whole.reshape(count, MODES // inner, inner, length).swapaxes(1, 2)
    left, right = [], []
    for order in orders(length):
        high, low = two_parts(whole.reshape(count * MODES, length)[:, order])
        right.append(np.concatenate([high, high, low], 0))
        high, low = two_parts(turned.reshape(count * MODES, length)[:, order])
        left.append(np.concatenate([high.T, low.T, high.T], 1))
    return np.stack(left, 0), np.stack(right, 0)


def split2(x):
    high = x.astype(jnp.bfloat16)
    return high, (x - high.astype(jnp.float32)).astype(jnp.bfloat16)


def dot(a, b, dims=NN):
    return lax.dot_general(a, b, dims, preferred_element_type=jnp.float32)


def dot3(a, b, dims=NN):
    return dot(a[0], b[0], dims) + (dot(a[0], b[1], dims) + dot(a[1], b[0], dims))


def series(value, first, count):
    total = jnp.full(value.shape, 1.0 / math.factorial(2 * (count - 1) + first), jnp.float32)
    for n in range(count - 2, -1, -1):
        total = 1.0 / math.factorial(2 * n + first) - value * total
    return total


def cosine_of(cell):
    angle = (0.5 * TB - (cell + 0.5)) * (math.pi / TB)
    return angle * series(angle * angle, 1, 9)


def propagator(wave_squared, kx, ky):
    vertical = wave_squared - kx * kx - ky * ky
    root = jnp.sqrt(jnp.abs(vertical)) * depth_step
    squared = root * root
    moving = vertical > 0.0
    even = jnp.where(moving, series(squared, 0, 10), jnp.exp(-root))
    odd = jnp.where(moving, root * series(squared, 1, 10), 0.0)
    return even, odd


def wave_number(place, length):
    half, quarter = length // 2, length // 4
    index = 2 * lax.rem(place, quarter) + lax.div(place, half)
    index = jnp.where(place == quarter, half, index)
    return 2.0 * math.pi / length * index.astype(jnp.float32)


def take_lanes(x, index):
    return jnp.take_along_axis(x, index, axis=1, mode="promise_in_bounds")


def iota(shape, axis):
    return lax.broadcasted_iota(jnp.int32, shape, axis)


def program(
    cfg,
    spectra_hbm,
    tile_hbm,
    bin_hbm,
    offset_hbm,
    weight_hbm,
    freq_ref,
    slow_hbm,
    vel_hbm,
    hart_hbm,
    modes_x_hbm,
    modes_y_hbm,
    wave_ref,
    image_in,
    spectra_ref,
    tile_ref,
    bin_ref,
    offset_ref,
    weight_ref,
    slow_ref,
    hart,
    modes_x,
    modes_y,
    vel_first,
    vel_last,
    route_out,
    route_in,
    coef_out,
    coef_in,
    wide_even,
    wide_odd,
    band_even,
    band_odd,
    along_first,
    across_first,
    along_last,
    across_last,
    slabs,
    first_real,
    fwd_out,
    fwd_in,
    back_out,
    back_in,
    image_out,
    trace_sem,
    table_sem,
    route_sent,
    route_got,
    coef_sent,
    coef_got,
    vel_sem,
    fwd_sent,
    fwd_got,
    back_sent,
    back_got,
    image_sent,
    image_got,
):
    F, L, tiles, nx, ny, rows, data_rows, padded, nvel = cfg
    devices = F * L
    group = L // 2
    half_x, half_y = nx // 2, ny // 2
    band = ny // group
    span = band // CHUNKS
    pair = 2 * span
    slots = tiles * CAP
    per_group = nvel // REFS
    me_f = lax.axis_index("freq")
    me_l = lax.axis_index("lat")
    me = me_l * F + me_f
    side = lax.div(me_l, group)
    seat = lax.rem(me_l, group)

    barrier = pltpu.get_barrier_semaphore()

    def partner_of(at):
        other = lax.rem(me + at, devices)
        return other, {"freq": lax.rem(other, F), "lat": lax.div(other, F)}

    def greet(at, carry):
        _, device = partner_of(at)
        pl.semaphore_signal(barrier, inc=1, device_id=device, device_id_type=MESH)
        return carry

    inputs = [
        pltpu.make_async_copy(src, dst, trace_sem.at[at])
        for at, (src, dst) in enumerate(
            [
                (tile_hbm, tile_ref),
                (bin_hbm, bin_ref),
                (offset_hbm, offset_ref),
                (weight_hbm, weight_ref),
                (spectra_hbm, spectra_ref),
            ]
        )
    ]
    for load in inputs:
        load.start()
    lax.fori_loop(1, devices, greet, 0)
    loads = [
        pltpu.make_async_copy(src, dst, table_sem.at[at])
        for at, (src, dst) in enumerate(
            [
                (vel_hbm.at[0], vel_first.at[side]),
                (vel_hbm.at[1], vel_last),
                (modes_x_hbm, modes_x),
                (modes_y_hbm, modes_y),
                (hart_hbm, hart),
                (slow_hbm, slow_ref),
            ]
        )
    ]
    for load in inputs:
        load.wait()
    for load in loads:
        load.start()

    count = tile_ref.shape[1]
    width = 128
    tile = tile_ref[...]
    columns = [
        jnp.transpose(jnp.broadcast_to(tile[:, at : at + width], (width, width)))
        for at in range(0, count, width)
    ]
    earlier = iota((width, width), 0) < iota((width, width), 1)
    ranks = []
    for at in range(count // width):
        row = jnp.broadcast_to(tile[:, at * width : (at + 1) * width], (width, width))
        same = jnp.where((columns[at] == row) & earlier, 1, 0)
        for before in range(at):
            same = same + jnp.where(columns[before] == row, 1, 0)
        ranks.append(jnp.sum(same, 0, keepdims=True))
    rank = jnp.concatenate(ranks, 1)
    turned = lax.rem(lax.rem(tile, tiles) + me, tiles)
    slot = lax.div(tile, tiles) * slots + turned * CAP + rank

    cell = bin_ref[...]
    root_weight = jnp.sqrt(weight_ref[...])
    cell_x = lax.div(cell, TB).astype(jnp.float32) + offset_ref[0:1, :]
    cell_y = lax.rem(cell, TB).astype(jnp.float32) + offset_ref[1:2, :]
    feats = jnp.concatenate(
        [spectra_ref[0] * root_weight, spectra_ref[1] * root_weight]
        + [root_weight, cosine_of(cell_x), cosine_of(cell_y)]
        + [jnp.zeros((padded - data_rows - 3, count), jnp.float32)],
        0,
    )
    high = feats.astype(jnp.bfloat16)
    rest = feats - high.astype(jnp.float32)
    middle = rest.astype(jnp.bfloat16)
    low = (rest - middle.astype(jnp.float32)).astype(jnp.bfloat16)
    parts = jnp.concatenate([high, middle, low], 0)
    fold = (data_rows + 4) // 2
    wide = 256
    places = iota((wide, count), 0).astype(jnp.float32).astype(jnp.bfloat16)
    one, none = jnp.ones((), jnp.bfloat16), jnp.zeros((), jnp.bfloat16)
    for at in range(0, devices * slots, wide):
        within = jnp.where((slot >= at) & (slot < at + wide), slot - at, wide)
        within = within.astype(jnp.float32).astype(jnp.bfloat16)
        chosen = jnp.where(places == within, one, none)
        got = dot(parts, chosen, NT)
        got = got[:padded] + got[padded : 2 * padded] + got[2 * padded :]
        for piece in range(wide // slots):
            block = got[:, piece * slots : (piece + 1) * slots]
            route_out[at // slots + piece] = jnp.concatenate([block[:fold], block[fold : 2 * fold]], 1)

    pl.semaphore_wait(barrier, devices - 1)

    def spread(out, into, sent, landed):
        def copy_of(at):
            other, device = partner_of(at)
            return pltpu.make_async_remote_copy(
                src_ref=out.at[other] if out.shape[0] == devices else out.at[lax.rem(other, F)],
                dst_ref=into.at[me],
                send_sem=sent.at[at],
                recv_sem=landed.at[at],
                device_id=device,
                device_id_type=MESH,
            )

        def start(at, carry):
            copy_of(at).start()
            return carry

        def arrive(at, carry):
            copy_of(at).wait_recv()
            return carry

        def leave(at, carry):
            copy_of(at).wait_send()
            return carry

        lax.fori_loop(1, devices, start, 0)
        return (
            lambda: lax.fori_loop(1, devices, arrive, 0),
            lambda: lax.fori_loop(1, devices, leave, 0),
        )

    arrive, leave_route = spread(route_out, route_in, route_sent, route_got)
    route_in[pl.ds(me, 1)] = route_out[pl.ds(me, 1)]

    for load in loads:
        load.wait()
    frequency = freq_ref[0]
    waves = []
    for depth_at in range(2):
        squares = []
        for g in range(REFS):
            total = slow_ref[depth_at, g * per_group]
            for i in range(1, per_group):
                total = total + slow_ref[depth_at, g * per_group + i]
            reference = total * (1.0 / per_group)
            squares.append((reference, (frequency * reference) * (frequency * reference)))
        waves.append(squares)

    chunk = 16
    quarter_x, quarter_y = nx // 4, ny // 4
    lane = iota((chunk, quarter_y), 1)
    first_ky = [wave_number(lane + parity * half_y, ny) for parity in range(2)]
    middle_ky = jnp.full((chunk, quarter_y), math.pi, jnp.float32)

    def wide_rows(g, kx):
        made = [propagator(waves[0][g][1], kx, ky) for ky in (*first_ky, middle_ky)]
        return [
            jnp.concatenate([even, jnp.where(lane == 0, middle, even), odd, odd], 1)
            for even, odd, middle in zip(*made)
        ]

    def wide_tables(at, carry):
        first = pl.multiple_of(lax.rem(at, quarter_x // chunk) * chunk, chunk)
        base = pl.multiple_of(lax.div(at, quarter_x // chunk) * half_x, half_x)
        kx = wave_number(iota((chunk, quarter_y), 0) + (first + base), nx)
        for g in range(REFS):
            for one, table in zip(wide_rows(g, kx), (wide_even, wide_odd)):
                for copy in range(2):
                    table[g, pl.ds(base + copy * quarter_x + first, chunk), :] = one
        return carry

    lax.fori_loop(0, half_x // chunk, wide_tables, 0)
    middle_kx = jnp.full((chunk, quarter_y), math.pi, jnp.float32)
    for g in range(REFS):
        for one, table in zip(wide_rows(g, middle_kx), (wide_even, wide_odd)):
            table[g, quarter_x : quarter_x + 1, :] = one[:1]
    arrive()

    parts = F if rows % (8 * F) == 0 else 1
    part_rows = rows // parts
    own_part = pl.ds(pl.multiple_of((me_f if parts > 1 else 0) * part_rows, part_rows), part_rows)
    mirror = pltpu.make_async_remote_copy(
        src_ref=vel_first.at[side, own_part],
        dst_ref=vel_first.at[side, own_part],
        send_sem=vel_sem.at[0],
        recv_sem=vel_sem.at[1],
        device_id={"lat": lax.rem(me_l + group, L)},
        device_id_type=MESH,
    )
    mirror.start()

    group_at = lax.div(lax.rem(iota((fold, 2 * slots), 1), slots), CAP)
    eye = jnp.where(iota((TERMS + data_rows, TERMS), 0) == iota((TERMS + data_rows, TERMS), 1), damping, 0.0)

    def chebyshev(cosine):
        terms = [jnp.ones_like(cosine), cosine]
        for _ in range(MODES - 2):
            terms.append(2.0 * cosine * terms[-1] - terms[-2])
        return terms

    normals = []
    for t in range(tiles):
        pieces = []
        for first in range(0, devices, tiles):
            picked = route_in[first]
            for i in range(1, tiles):
                picked = jnp.where(group_at == (t + i) % tiles, route_in[first + i], picked)
            pieces.append(picked)
        data = jnp.concatenate([piece[:, :slots] for piece in pieces], 1)
        place = jnp.concatenate([piece[:, slots:] for piece in pieces], 1)
        data = jnp.concatenate([data, place[: data_rows - fold]], 0)
        place = place[data_rows - fold :]
        scale = place[0:1]
        along_x = chebyshev(place[1:2])
        along_y = jnp.concatenate(chebyshev(place[2:3]), 0)
        basis = jnp.concatenate([(term * scale) * along_y for term in along_x], 0)
        right = jnp.concatenate([basis, data], 0)
        normals.append(
            eye
            + lax.dot_general(
                right, basis, NT, preferred_element_type=jnp.float32, precision=lax.Precision.HIGHEST
            )
        )
    inner = 128 // tiles
    outer = TERMS // inner
    lines = (TERMS + data_rows) // 8
    rest = []
    for at in range(outer):
        line = jnp.concatenate([one[:, at * inner : (at + 1) * inner] for one in normals], 1)
        rest.append([line[8 * j : 8 * (j + 1)] for j in range(lines)])
    lane = iota((8, 128), 1)
    within = lax.rem(lane, inner)
    for block in range(TERMS // 8):
        todo = range(block, lines)
        pivots = []
        for s in range(8):
            at, own = (8 * block + s) // inner, (8 * block + s) % inner
            pick = lane - within + own
            pivots.append({j: take_lanes(rest[at][j], pick) for j in todo})
        for s in range(8):
            at, own = (8 * block + s) // inner, (8 * block + s) % inner
            scale = 1.0 / pivots[s][block][s : s + 1]
            scaled = {j: pivots[s][j] * scale for j in todo}
            for later in range(s + 1, 8):
                factor = pivots[later][block][s : s + 1]
                pivots[later] = {j: pivots[later][j] - factor * scaled[j] for j in todo}
            for one in range(outer):
                factor = rest[one][block][s : s + 1]
                for j in todo:
                    value = rest[one][j] - factor * scaled[j]
                    rest[one][j] = jnp.where(within == own, scaled[j], value) if one == at else value
    width = tiles * MODES
    place = lax.rem(lane, width)
    pick = lax.div(place, MODES) * inner + lax.div(lane, width) * MODES + lax.rem(place, MODES)
    for one in range(outer):
        for j in range(TERMS // 8, lines):
            line = take_lanes(rest[one][j], pick)
            for s in range(8):
                part, f = divmod(8 * (j - TERMS // 8) + s, F)
                coef_out[f, part * outer + one : part * outer + one + 1, :] = line[s : s + 1]

    arrive, leave_coef = spread(coef_out, coef_in, coef_sent, coef_got)
    coef_in[pl.ds(me, 1)] = coef_out[pl.ds(me_f, 1)]

    mirror.wait_recv()
    handed = []
    for step in range(1, parts):
        other = lax.rem(me_f + step, F)
        handed.append(
            pltpu.make_async_remote_copy(
                src_ref=vel_first.at[1 - side, own_part],
                dst_ref=vel_first.at[1 - side, own_part],
                send_sem=vel_sem.at[2 * step],
                recv_sem=vel_sem.at[2 * step + 1],
                device_id={"freq": other},
                device_id_type=MESH,
            )
        )
    for copy in handed:
        copy.start()

    pair_lane = iota((chunk, pair), 1)
    sign = jnp.where(pair_lane < span, -1.0, 1.0)
    band_ky = [
        wave_number(seat * band + c * span + lax.rem(pair_lane, span), ny) for c in range(CHUNKS)
    ]

    def band_rows(c, g, kx):
        even, odd = propagator(waves[1][g][1], kx, band_ky[c])
        return (even, band_even), (odd * sign, band_odd)

    def band_tables(at, carry):
        first = pl.multiple_of(lax.rem(at, quarter_x // chunk) * chunk, chunk)
        base = pl.multiple_of(lax.div(at, quarter_x // chunk) * half_x, half_x)
        kx = wave_number(iota((chunk, pair), 0) + (first + base), nx)
        for c in range(CHUNKS):
            for g in range(REFS):
                for one, table in band_rows(c, g, kx):
                    for copy in range(2):
                        table[c, g, pl.ds(base + copy * quarter_x + first, chunk), :] = one
        return carry

    lax.fori_loop(0, half_x // chunk, band_tables, 0)
    for c in range(CHUNKS):
        for g in range(REFS):
            for one, table in band_rows(c, g, jnp.full((chunk, pair), math.pi, jnp.float32)):
                table[c, g, quarter_x : quarter_x + 1, :] = one[:1]

    def split_step(depth_at, velocity):
        cosine = jnp.zeros(velocity.shape, jnp.float32)
        sine = jnp.zeros(velocity.shape, jnp.float32)
        for i in range(nvel):
            shift = slow_ref[depth_at, i] - waves[depth_at][i // per_group][0]
            angle = jnp.full((8, 128), frequency * shift * depth_step, jnp.float32)
            squared = angle * angle
            cosine_i = series(squared, 0, 9)[0:1, 0:1]
            sine_i = (angle * series(squared, 1, 9))[0:1, 0:1]
            cosine = jnp.where(velocity == i, cosine_i, cosine)
            sine = jnp.where(velocity == i, sine_i, sine)
        return cosine, sine

    along_last[...], across_last[...] = split_step(1, vel_last[...])
    for copy in handed:
        copy.wait_recv()
    for one in range(2):
        along_first[one], across_first[one] = split_step(0, vel_first[one])
    arrive()

    def part_of(which):
        return hart[which, 0], hart[which, 1]

    even_k, even_k_t, odd_k, odd_k_t = (part_of(which) for which in range(4))

    def from_modes_of(parts):
        return jnp.concatenate([parts[0], parts[1], parts[0]], 1)

    per_row = (ny // TB) // tiles
    tile_rows = nx // TB
    mode_rows = tile_rows // 2 * MODES
    mode_columns = ny // TB // 2 * MODES
    sums, differences = [], []
    for part in range(2):
        lines = [
            jnp.concatenate(
                [
                    jnp.concatenate(
                        [
                            coef_in[
                                tile_row * per_row + j,
                                part * outer : (part + 1) * outer,
                                a * width : (a + 1) * width,
                            ]
                            for a in range(MODES // outer)
                        ],
                        0,
                    )
                    for j in range(per_row)
                ],
                1,
            )
            for tile_row in range(tile_rows)
        ]
        upper = jnp.concatenate(lines[: tile_rows // 2], 0)
        lower = jnp.concatenate(lines[tile_rows // 2 :], 0)
        for one in (upper + lower, upper - lower):
            left, right = one[:, :mode_columns], one[:, mode_columns:]
            sums.append(left + right)
            differences.append(left - right)
    spread_y = [
        dot(from_modes_of(split2(jnp.concatenate(one, 0))), modes_y[parity])
        for parity, one in enumerate((sums, differences))
    ]
    seat_rows = pl.ds(pl.multiple_of(seat * rows, rows), rows)
    spans = []
    for parity in range(2):
        parts = []
        for p in range(2):
            at = (2 * p + parity) * mode_rows
            line = jnp.concatenate([one[at : at + mode_rows] for one in spread_y], 1)
            parts.append(split2(line))
        spans.append(parts)
    seats = []
    for which in (1, 3):
        own_high, own_low = hart[which, 0, seat_rows, :], hart[which, 1, seat_rows, :]
        seats.append((own_high, jnp.concatenate([own_high, own_low], 0)))
    wide = 256
    for first in range(0, ny, wide):
        lanes = slice(first, first + wide)
        made = [[None, None] for _ in range(REFS)]
        for parity in range(2):
            high = jnp.concatenate([one[0][:, lanes] for one in spans[parity]], 1)
            low = jnp.concatenate([one[1][:, lanes] for one in spans[parity]], 1)
            spectrum = dot(modes_x[parity], jnp.concatenate([high, high, low], 0))
            real, imag = spectrum[:, :wide], spectrum[:, wide:]
            own_high, both = seats[parity]
            part = slice(parity * half_x, (parity + 1) * half_x)
            for g in range(REFS):
                even, odd = wide_even[g, part, lanes], wide_odd[g, part, lanes]
                moved = split2(
                    jnp.concatenate([real * even - imag * odd, real * odd + imag * even], 1)
                )
                back = dot(both, moved[0])
                made[g][parity] = back[:rows] + (back[rows:] + dot(own_high, moved[1]))
        for g in range(REFS):
            for at, slab in enumerate((made[g][0] + made[g][1], made[g][0] - made[g][1])):
                for p in range(2):
                    slabs[at, 2 * g + p, :, lanes] = slab[:, p * wide : (p + 1) * wide]

    def inverse_y(x):
        u = dot3(split2(x[:, :half_y]), even_k)
        v = dot3(split2(x[:, half_y:]), odd_k)
        return jnp.concatenate([u + v, u - v], 1)

    def choose(made, velocity):
        real, imag = made[0]
        for g in range(1, REFS):
            chosen = velocity >= g * per_group
            real = jnp.where(chosen, made[g][0], real)
            imag = jnp.where(chosen, made[g][1], imag)
        return real, imag

    image_piece = ny // F

    def send_image(at, depth_at, first, real):
        part = slice(first, first + real.shape[0])
        for f in range(F):
            image_out[depth_at, f, part, :] = real[:, f * image_piece : (f + 1) * image_piece]
        copies = []
        for step in range(1, F):
            other = lax.rem(me_f + step, F)
            copies.append(
                pltpu.make_async_remote_copy(
                    src_ref=image_out.at[depth_at, other, part],
                    dst_ref=image_in.at[depth_at, me_f, part],
                    send_sem=image_sent.at[at, step],
                    recv_sem=image_got.at[at, step],
                    device_id={"freq": other},
                    device_id_type=MESH,
                )
            )
        for copy in copies:
            copy.start()
        image_in[depth_at, pl.ds(me_f, 1), part, :] = image_out[depth_at, pl.ds(me_f, 1), part, :]
        return copies

    def copies_of(at, c, out, into, sent, landed):
        copies = []
        for step in range(1, group):
            other = lax.rem(seat + step, group)
            copies.append(
                pltpu.make_async_remote_copy(
                    src_ref=out.at[at, c, other],
                    dst_ref=into.at[at, c, seat],
                    send_sem=sent.at[at, c, step],
                    recv_sem=landed.at[at, c, step],
                    device_id={"lat": side * group + other},
                    device_id_type=MESH,
                )
            )
        return copies

    def exchange(at, c, out, into, sent, landed):
        copies = copies_of(at, c, out, into, sent, landed)
        for copy in copies:
            copy.start()
        into[at, c, pl.ds(seat, 1)] = out[at, c, pl.ds(seat, 1)]
        return copies

    def first_rows(at, carry):
        field = inverse_y(slabs[at].reshape(2 * REFS * rows, ny))
        made = [
            (field[2 * g * rows : (2 * g + 1) * rows], field[(2 * g + 1) * rows : (2 * g + 2) * rows])
            for g in range(REFS)
        ]
        real, imag = choose(made, vel_first[at])
        cosine, sine = along_first[at], across_first[at]
        real, imag = real * cosine - imag * sine, real * sine + imag * cosine
        first_real[at] = real
        both = jnp.concatenate([real, imag], 0)
        left, right = both[:, :half_y], both[:, half_y:]
        line = jnp.concatenate(
            [dot3(split2(left + right), even_k_t), dot3(split2(left - right), odd_k_t)], 1
        )
        for c in range(CHUNKS):
            for dst in range(group):
                part = slice(dst * band + c * span, dst * band + (c + 1) * span)
                fwd_out[at, c, dst] = jnp.concatenate([line[:rows, part], line[rows:, part]], 1)
        exchange(at, 0, fwd_out, fwd_in, fwd_sent, fwd_got)
        return carry

    lax.fori_loop(0, 2, first_rows, 0)
    forward = [[copies_of(at, 0, fwd_out, fwd_in, fwd_sent, fwd_got) for at in range(2)]]
    for c in range(1, CHUNKS):
        forward.append([exchange(at, c, fwd_out, fwd_in, fwd_sent, fwd_got) for at in range(2)])
    forward = [sum(copies, []) for copies in forward]
    first_image = send_image(0, 0, 0, first_real[pl.ds(side, 1)].reshape(rows, ny))

    turn = (1 - 2 * side).astype(jnp.float32)
    half = rows // 2

    def apply(table, x):
        high, low = split2(x)
        made = dot(table[0], jnp.concatenate([high, low], 1))
        return made[:, :pair] + (made[:, pair:] + dot(table[1], high))

    backward = []
    for c in range(CHUNKS):
        for copy in forward[c]:
            copy.wait_recv()
        upper, lower = fwd_in[0, c].reshape(half_x, pair), fwd_in[1, c].reshape(half_x, pair)
        spectrum = []
        for one, table in ((upper + lower, even_k), (upper - lower, odd_k)):
            line = apply(table, one)
            spectrum.append((line, jnp.concatenate([line[:, span:], line[:, :span]], 1)))
        lines = []
        for g in range(REFS):
            sides = []
            for parity, table in enumerate((even_k_t, odd_k_t)):
                part = slice(parity * half_x, (parity + 1) * half_x)
                line, swapped = spectrum[parity]
                sides.append(
                    apply(table, line * band_even[c, g, part, :] + swapped * band_odd[c, g, part, :])
                )
            lines.append((sides[0] + turn * sides[1]).reshape(group, rows, pair))
        both = jnp.concatenate(lines, 2)
        for h in range(2):
            back_out[h, c] = both[:, h * half : (h + 1) * half]
            backward.append(exchange(h, c, back_out, back_in, back_sent, back_got))
    last_image = []
    for h in range(2):
        for c in range(CHUNKS):
            for copy in backward[2 * c + h]:
                copy.wait_recv()
        lines = []
        for at in range(2 * REFS):
            part = slice(at * span, (at + 1) * span)
            lines.append(
                jnp.concatenate(
                    [back_in[h, c, src, :, part] for src in range(group) for c in range(CHUNKS)], 1
                )
            )
        field = inverse_y(jnp.concatenate(lines, 0))
        made = [
            (field[2 * g * half : (2 * g + 1) * half], field[(2 * g + 1) * half : (2 * g + 2) * half])
            for g in range(REFS)
        ]
        own = slice(h * half, (h + 1) * half)
        real, imag = choose(made, vel_last[own, :])
        cosine, sine = along_last[own, :], across_last[own, :]
        moved = real * cosine - imag * sine
        last_image += send_image(1 + h, 1, h * half, moved)
        wave_ref[0, own, :] = moved
        wave_ref[1, own, :] = real * sine + imag * cosine

    leave_route()
    leave_coef()
    mirror.wait_send()
    for copy in handed:
        copy.wait_send()
    for copies in forward + backward:
        for copy in copies:
            copy.wait_send()
    for copy in first_image + last_image:
        copy.wait()


def finish(wave_ref, part_ref, wave_hbm, image_hbm, total, sem):
    store = pltpu.make_async_copy(wave_ref, wave_hbm.at[:, 0], sem.at[0])
    store.start()
    image = part_ref[:, 0]
    for f in range(1, part_ref.shape[1]):
        image = image + part_ref[:, f]
    total[...] = image
    last = pltpu.make_async_copy(total, image_hbm, sem.at[1])
    last.start()
    store.wait()
    last.wait()


def stay(x):
    return pltpu.with_memory_space_constraint(x, pltpu.HBM)


def local(spectra, tile_route, bin_in_tile, trace_offset, weights, frequency, slowness, vel_index):
    F = lax.axis_size("freq")
    L = lax.axis_size("lat")
    devices = F * L
    steps, rows, ny = vel_index.shape
    assert steps == 2
    nx = rows * L
    tiles = (nx // TB) * (ny // TB) // devices
    slots = tiles * CAP
    count = spectra.shape[2]
    data_rows = 2 * spectra.shape[1]
    padded = 2 * data_rows
    group = L // 2
    pair = 2 * (ny // group) // CHUNKS
    nvel = slowness.shape[1]
    cfg = (F, L, tiles, nx, ny, rows, data_rows, padded, nvel)

    hart = jnp.asarray(half_tables(nx))
    outer = TERMS * tiles // 128
    modes_x, modes_y = (jnp.asarray(one) for one in mode_tables(nx, MODES // outer))

    f32, bf16, i32 = jnp.float32, jnp.bfloat16, jnp.int32
    dma = pltpu.SemaphoreType.DMA
    wave, images = pl.pallas_call(
        functools.partial(program, cfg),
        out_shape=[
            jax.ShapeDtypeStruct((2, rows, ny), f32),
            jax.ShapeDtypeStruct((2, F, rows, ny // F), f32),
        ],
        in_specs=[HBM] * 5 + [SMEM] + [HBM] * 5,
        out_specs=[VMEM, VMEM],
        scratch_shapes=[
            pltpu.VMEM(spectra.shape, f32),
            pltpu.VMEM((1, count), i32),
            pltpu.VMEM((1, count), i32),
            pltpu.VMEM((2, count), f32),
            pltpu.VMEM((1, count), f32),
            pltpu.SMEM(slowness.shape, f32),
            pltpu.VMEM(hart.shape, bf16),
            pltpu.VMEM(modes_x.shape, bf16),
            pltpu.VMEM(modes_y.shape, bf16),
            pltpu.VMEM((2, rows, ny), i32),
            pltpu.VMEM((rows, ny), i32),
            pltpu.VMEM((devices, (data_rows + 4) // 2, 2 * slots), f32),
            pltpu.VMEM((devices, (data_rows + 4) // 2, 2 * slots), f32),
            pltpu.VMEM((F, 2 * outer, 128), f32),
            pltpu.VMEM((devices, 2 * outer, 128), f32),
            pltpu.VMEM((REFS, nx, ny), f32),
            pltpu.VMEM((REFS, nx, ny), f32),
            pltpu.VMEM((CHUNKS, REFS, nx, pair), f32),
            pltpu.VMEM((CHUNKS, REFS, nx, pair), f32),
            pltpu.VMEM((2, rows, ny), f32),
            pltpu.VMEM((2, rows, ny), f32),
            pltpu.VMEM((rows, ny), f32),
            pltpu.VMEM((rows, ny), f32),
            pltpu.VMEM((2, 2 * REFS, rows, ny), f32),
            pltpu.VMEM((2, rows, ny), f32),
            pltpu.VMEM((2, CHUNKS, group, rows, pair), f32),
            pltpu.VMEM((2, CHUNKS, group, rows, pair), f32),
            pltpu.VMEM((2, CHUNKS, group, rows // 2, REFS * pair), f32),
            pltpu.VMEM((2, CHUNKS, group, rows // 2, REFS * pair), f32),
            pltpu.VMEM((2, F, rows, ny // F), f32),
            dma((5,)),
            dma((6,)),
            dma((devices,)),
            dma((devices,)),
            dma((devices,)),
            dma((devices,)),
            dma((2 * F,)),
            dma((2, CHUNKS, group)),
            dma((2, CHUNKS, group)),
            dma((2, CHUNKS, group)),
            dma((2, CHUNKS, group)),
            dma((3, F)),
            dma((3, F)),
        ],
        compiler_params=pltpu.CompilerParams(
            collective_id=0, has_side_effects=True, vmem_limit_bytes=40 << 20
        ),
    )(
        *map(stay, (spectra, tile_route.reshape(1, count), bin_in_tile.reshape(1, count))),
        *map(stay, (trace_offset, weights.reshape(1, count))),
        frequency,
        stay(slowness),
        *map(stay, (vel_index, hart, modes_x, modes_y)),
    )
    return pl.pallas_call(
        finish,
        out_shape=[
            jax.ShapeDtypeStruct((2, 1, rows, ny), f32),
            jax.ShapeDtypeStruct((2, rows, ny // F), f32),
        ],
        in_specs=[VMEM, VMEM],
        out_specs=[HBM, HBM],
        scratch_shapes=[pltpu.VMEM((2, rows, ny // F), f32), dma((2,))],
        compiler_params=pltpu.CompilerParams(vmem_limit_bytes=8 << 20),
    )(wave, images)


def solution(mesh):
    return jax.shard_map(
        local,
        mesh=mesh,
        in_specs=(
            P(None, None, ("freq", "lat")),
            P(("freq", "lat"), None),
            P(("freq", "lat")),
            P(None, ("freq", "lat")),
            P(("freq", "lat")),
            P("freq"),
            P(),
            P(None, "lat", None),
        ),
        out_specs=(P(None, "freq", "lat", None), P(None, "lat", "freq")),
        check_vma=False,
    )
```
